32 devices in a mesh: dom: 8 (over z, y), cls: 4 (over x, core).
Axes of the slice: x: 2, y: 2, z: 4, core: 2. Of those that a mesh axis runs over, the one named last changes fastest.
Arguments:
- images: bfloat16 [4096, 2, 16384], P(('dom', 'cls')), may hold values from -6 to 6
- slices: bfloat16 [32, 4, 2, 16384], P(('dom', 'cls')), may hold values from -6 to 6
- classes: int32 [4096], P(('dom', 'cls')), may hold values from 0 to 31, as said below
- rotations: int32 [4096], P(('dom', 'cls')), may hold values from 0 to 3
- defocus: int32 [4096], P(('dom', 'cls')), may hold values from 8000 to 29999
- groups: int32 [4096], P(('dom', 'cls')), may hold values from 0 to 255, as said below
Outputs:
- sigma: float32 [256, 64], P(('dom', 'cls'))
The draws below stay inside these ranges and needn't reach their ends.
Inputs may be any that keep to these rules, and one draw needn't show every extreme that they name: Class c is owned by device c // 1 of dom+cls. In the rows of one device, at most 8 particles have classes of one owner; in every draw one owner gets exactly 8 from the rows of every device. `groups`: group g is owned by device g // 8 of dom+cls. Every group holds at least 8 particles.
All inputs are finite; a program needn't handle non-finite values.
Results may differ from the reference program's by a relative error of at most 0.0003.
Values may be sent and summed in bfloat16 or wider, within the bound.
A program may use at most 192 MiB of HBM per device.

```python
import math
import jax
import jax.numpy as jnp
from jax import lax

SIDE = 128
PIX = 16384
SHELLS = 64
ROT = 4
CLS_DEV = 1
CLASSES = 32
P_DEV = 128
PARTICLES = 4096
CAP = 8
GROUPS_DEV = 8
GROUPS = 256


def draw_classes(key, part):
    owner_count = CLASSES // CLS_DEV
    block_count = PARTICLES // P_DEV
    slot_count = owner_count * CAP
    key_popular, key_bias, key_blocks = jax.random.split(jax.random.fold_in(key, 11), 3)
    popular = jax.random.randint(key_popular, (), 0, owner_count)
    owner_bias = jax.random.randint(key_bias, (owner_count,), 0, 4096)

    def one_block(block_index):
        block_key = jax.random.fold_in(key_blocks, block_index)
        key_noise, key_order, key_within = jax.random.split(block_key, 3)
        noise = jax.random.randint(key_noise, (owner_count, CAP), 0, 4096)
        owner_ids = jnp.broadcast_to(jnp.arange(owner_count, dtype=jnp.int32)[:, None], (owner_count, CAP))
        scores = owner_bias[:, None] + noise + jnp.where(owner_ids == popular, 16384, 0)
        distinct = scores.reshape(-1) * slot_count + jnp.arange(slot_count, dtype=jnp.int32)
        chosen_values, picked = lax.top_k(distinct, P_DEV)
        owner_of = picked.astype(jnp.int32) // CAP
        shuffle = jax.random.permutation(key_order, P_DEV)
        owner_of = owner_of[shuffle]
        within = jax.random.randint(key_within, (P_DEV,), 0, CLS_DEV)
        return owner_of * CLS_DEV + within
    return jax.vmap(one_block)(jnp.arange(block_count, dtype=jnp.int32)).reshape(-1).astype(jnp.int32)


def draw_groups(key, part):
    block_count = PARTICLES // P_DEV
    half_rows = P_DEV // 2
    key_random, key_order = jax.random.split(jax.random.fold_in(key, 23), 2)
    device_ids = jnp.arange(block_count, dtype=jnp.int32)[:, None]
    row_ids = jnp.arange(P_DEV, dtype=jnp.int32)[None, :]
    far_owner = (device_ids + block_count // 2) % block_count
    far_group = far_owner * GROUPS_DEV + row_ids % GROUPS_DEV
    random_group = jax.random.randint(key_random, (block_count, P_DEV), 0, GROUPS)
    base = jnp.where(row_ids < half_rows, far_group, random_group)
    order_keys = jax.random.split(key_order, block_count)
    orders = jax.vmap(lambda one_key: jax.random.permutation(one_key, P_DEV))(order_keys)
    mixed = jnp.take_along_axis(base, orders.astype(jnp.int32), axis=1)
    return mixed.reshape(-1).astype(jnp.int32)


def set_ends(array, key, least, high):
    index_at = [jax.random.randint(jax.random.fold_in(key, axis), (), 0, length) for axis, length in enumerate(array.shape)]
    main_axis = array.shape.index(max(array.shape))
    neighbour = index_at[:main_axis] + [(index_at[main_axis] + 1) % array.shape[main_axis]] + index_at[main_axis + 1:]
    return array.at[tuple(index_at)].set(least).at[tuple(neighbour)].set(high)


def shard_levels(rng, extent, pieces, low, top_value):
    loudness, own = 1.0, jax.random.fold_in(rng, 6)
    for dim, shards_of in pieces:
        heights = jnp.exp(jax.random.uniform(jax.random.fold_in(own, dim), (shards_of,), jnp.float32, low / len(pieces), top_value / len(pieces)))
        loudness = loudness * jnp.repeat(heights, extent[dim] // shards_of).reshape([-1 if axis == dim else 1 for axis in range(len(extent))])
    return loudness


def gaussian(stream_key, dims, scale, bound, shards=(), kind=jnp.bfloat16):
    drawn = scale * jax.random.normal(stream_key, dims, jnp.float32)
    if shards:
        drawn = drawn * shard_levels(stream_key, dims, shards, -0.22, 0.18)
    return jnp.clip(drawn, -bound, bound).astype(kind)


def setup_inputs(seed: int = 0) -> dict:
    key_list = jax.random.split(jax.random.key(seed), 7)
    return {
        "images": gaussian(key_list[0], (PARTICLES, 2, PIX), 1.0, 6.0, ((0, 32),)),
        "slices": gaussian(key_list[1], (CLASSES, ROT, 2, PIX), 1.0, 6.0, ((0, 32),)),
        "classes": draw_classes(jax.random.fold_in(key_list[6], 71), 0),
        "rotations": set_ends(jax.random.randint(key_list[3], (PARTICLES,), 0, ROT), jax.random.fold_in(key_list[3], 1), 0, ROT - 1).astype(jnp.int32),
        "defocus": set_ends(jax.random.randint(key_list[4], (PARTICLES,), 8000, 30000), jax.random.fold_in(key_list[4], 1), 8000, 29999).astype(jnp.int32),
        "groups": draw_groups(jax.random.fold_in(key_list[6], 71), 0),
    }


PIXEL_SIZE = 1.5
WAVELENGTH = 0.0197
SPHERICAL = 27000000.0
AMPLITUDE = 0.1

def frequency_grid(side_cells):
    offsets = jnp.arange(side_cells, dtype=jnp.int32)
    signed = jnp.where(offsets < side_cells // 2, offsets, offsets - side_cells)
    return (signed[:, None] * signed[:, None] + signed[None, :] * signed[None, :]).reshape(-1).astype(jnp.int32)

def shell_matrix(radius_sq, shell_count):
    shell_ids = jnp.arange(shell_count, dtype=jnp.int32)
    lower = shell_ids * shell_ids
    upper = (shell_ids + 1) * (shell_ids + 1)
    in_shell = (lower[None, :] <= radius_sq[:, None]) & (radius_sq[:, None] < upper[None, :])
    return in_shell.astype(jnp.float32)

def contrast(defocus, radius_sq, side_cells):
    spatial = radius_sq.astype(jnp.float32) / jnp.float32((side_cells * PIXEL_SIZE) ** 2)
    depth = defocus.astype(jnp.float32)[:, None]
    phase_shift = math.pi * WAVELENGTH * depth * spatial[None, :] - 0.5 * math.pi * SPHERICAL * WAVELENGTH ** 3 * spatial[None, :] * spatial[None, :]
    return -(math.sqrt(1.0 - AMPLITUDE * AMPLITUDE) * jnp.sin(phase_shift) + AMPLITUDE * jnp.cos(phase_shift))

def power_in_shells(images, fetched, ctf, shell_table):
    difference = images.astype(jnp.float32) - ctf[:, None, :] * fetched.astype(jnp.float32)
    pixel_power = lax.optimization_barrier(jnp.sum(difference * difference, axis=1))
    return jnp.dot(pixel_power, shell_table, precision=lax.Precision.HIGHEST, preferred_element_type=jnp.float32)

def reference(images, slices, classes, rotations, defocus, groups):
    radius_sq = frequency_grid(SIDE)
    shell_table = shell_matrix(radius_sq, SHELLS)
    block_rows = math.gcd(PARTICLES, 512)
    block_count = PARTICLES // block_rows

    def per_block(operands):
        image_rows, class_rows, rotation_rows, defocus_rows = operands
        fetched = slices[class_rows, rotation_rows]
        ctf = contrast(defocus_rows, radius_sq, SIDE)
        return power_in_shells(image_rows, fetched, ctf, shell_table)
    shell_power = lax.map(per_block, (images.reshape(block_count, block_rows, 2, PIX), classes.reshape(block_count, block_rows), rotations.reshape(block_count, block_rows), defocus.reshape(block_count, block_rows))).reshape(PARTICLES, SHELLS)
    group_sums = jax.ops.segment_sum(shell_power, groups, num_segments=GROUPS)
    group_counts = jax.ops.segment_sum(jnp.ones((PARTICLES,), jnp.float32), groups, num_segments=GROUPS)
    pixel_counts = lax.optimization_barrier(jnp.sum(shell_table, axis=0))
    return group_sums / (2.0 * group_counts[:, None] * pixel_counts[None, :])
```

```python
import functools
import math

import jax
import jax.numpy as jnp
import numpy as np
from jax import lax
from jax.experimental import pallas as pl
from jax.experimental.pallas import tpu as pltpu
from jax.sharding import PartitionSpec as P

GROUPS_DEV = 8
PIXEL_SIZE = 1.5
WAVELENGTH = 0.0197
SPHERICAL = 27000000.0
AMPLITUDE = 0.1
ROUND = 12582912.0
MESH = pl.DeviceIdType.MESH
AXES = ("dom", "cls")
ROUTES = (("x", "y", "z"), ("z", "y", "x"), ("z", "x", "y"))
SHARE = (8, 12, 12)


def sine_coefficients(terms):
    nodes = 0.5 * np.cos((np.arange(400) + 0.5) * math.pi / 400)
    nodes = nodes[np.abs(nodes) > 1e-3]
    basis = np.stack([nodes ** (2 * k + 1) for k in range(terms)], 1)
    return np.linalg.lstsq(basis, np.sin(2 * math.pi * nodes), rcond=None)[0]


SINE = [float(v) for v in sine_coefficients(5)]


def gather_kernel(shape, own_ref, out_ref, local_sem, send_sem, recv_sem, pair_send, pair_recv):
    size = dict(x=shape[0], y=shape[1], z=shape[2])
    dom, cls = lax.axis_index("dom"), lax.axis_index("cls")
    here = dict(x=cls // 2, y=dom % size["y"], z=dom // size["y"])
    core = cls % 2
    rows = out_ref.shape[2]
    starts = [0]
    for share in SHARE:
        starts.append(starts[-1] + rows * share // 32)

    def device(at, which):
        return (at["z"] * size["y"] + at["y"], at["x"] * 2 + which)

    def slot(at, which):
        d = device(at, which)
        return d[0] * (size["x"] * 2) + d[1]

    def moved(at, dim, step):
        new = dict(at)
        new[dim] = at[dim] + step
        return new

    ways = []
    for dim in "xyz":
        if size[dim] == 1:
            continue
        if size[dim] == 2:
            other = dict(here)
            other[dim] = 1 - here[dim]
            ways.append((dim, 0, other, None))
        else:
            ways.append((dim, 1, moved(here, dim, 1), here[dim] < size[dim] - 1))
            ways.append((dim, -1, moved(here, dim, -1), here[dim] > 0))

    def when(conds, fn):
        conds = [c for c in conds if c is not None]
        if not conds:
            fn()
        else:
            pl.when(functools.reduce(jnp.logical_and, conds))(fn)

    barrier = pltpu.get_barrier_semaphore()
    partner = device(here, 1 - core)
    pl.semaphore_signal(barrier, inc=1, device_id=partner, device_id_type=MESH)
    for dim, sign, other, ok in ways:

        def greet(other=other):
            pl.semaphore_signal(barrier, inc=1, device_id=device(other, core), device_id_type=MESH)

        when([ok], greet)
    peers = 1
    for dim, sign, other, ok in ways:
        peers = peers + (1 if ok is None else ok.astype(jnp.int32))
    pl.semaphore_wait(barrier, peers)

    mine = slot(here, core)
    local = pltpu.make_async_copy(own_ref, out_ref.at[mine], local_sem)
    local.start()

    def part(ref, index):
        return ref.at[:, pl.ds(starts[index], starts[index + 1] - starts[index]), :]

    def copy(index, source, src_slot, to, way, own):
        src = part(own_ref, index) if own else part(out_ref.at[src_slot], index)
        return pltpu.make_async_remote_copy(
            src_ref=src,
            dst_ref=part(out_ref.at[src_slot], index),
            send_sem=send_sem.at[index, source, way],
            recv_sem=recv_sem.at[index, src_slot],
            device_id=to,
            device_id_type=MESH,
        )

    def pair_copy(index, source, src_slot, own):
        src = part(own_ref, index) if own else part(out_ref.at[src_slot], index)
        return pltpu.make_async_remote_copy(
            src_ref=src,
            dst_ref=part(out_ref.at[src_slot], index),
            send_sem=pair_send.at[index, source],
            recv_sem=pair_recv.at[index, src_slot],
            device_id=partner,
            device_id_type=MESH,
        )

    choices = {}
    for dim in "xyz":
        n = size[dim]
        if n == 1:
            choices[dim] = [(0, here[dim], None, 0)]
        elif n == 2:
            choices[dim] = [(0, here[dim], None, 0), (0, 1 - here[dim], None, 1)]
        else:
            listed = [(0, here[dim], None, 0)]
            for t in range(1, n):
                listed.append((1, here[dim] - t, here[dim] >= t, t))
                listed.append((-1, here[dim] + t, here[dim] + t < n, t))
            choices[dim] = listed
    events = []
    for ix, cx in enumerate(choices["x"]):
        for iy, cy in enumerate(choices["y"]):
            for iz, cz in enumerate(choices["z"]):
                pick = dict(x=cx, y=cy, z=cz)
                depth = cx[3] + cy[3] + cz[3]
                number = (ix * len(choices["y"]) + iy) * len(choices["z"]) + iz
                for index in range(3):
                    events.append((depth, index, number, pick))
    events.sort(key=lambda e: e[:3])
    finish = []
    for depth, index, number, pick in events:
        at = {dim: pick[dim][1] for dim in "xyz"}
        exists = [pick[dim][2] for dim in "xyz"]
        src_slot = slot(at, core)
        order = ROUTES[index]
        last = max([k for k, dim in enumerate(order) if pick[dim][3] > 0], default=-1)
        sends = []
        for number_way, (dim, sign, other, ok) in enumerate(ways):
            k = order.index(dim)
            if k < last:
                continue
            if k == last and (size[dim] == 2 or sign != pick[dim][0]):
                continue
            sends.append((number_way, device(other, core), ok))

        def arrive(index=index, number=number, src_slot=src_slot, depth=depth, sends=sends):
            own = depth == 0
            if not own:
                copy(index, number, src_slot, partner, 0, False).wait_recv()
            for way, to, ok in sends:
                when([ok], copy(index, number, src_slot, to, way, own).start)
            pair_copy(index, number, src_slot, own).start()

        def done(index=index, number=number, src_slot=src_slot, depth=depth, sends=sends, at=at):
            own = depth == 0
            for way, to, ok in sends:
                when([ok], copy(index, number, src_slot, to, way, own).wait_send)
            pair_copy(index, number, src_slot, own).wait_send()
            pair_copy(index, number, slot(at, 1 - core), False).wait_recv()

        when(exists, arrive)
        finish.append((exists, done))
    for exists, done in finish:
        when(exists, done)
    local.wait()


def gather(shape, own):
    devices = 2 * shape[0] * shape[1] * shape[2]
    total = 1
    for n in shape:
        total *= n if n <= 2 else 2 * n - 1
    return pl.pallas_call(
        functools.partial(gather_kernel, shape),
        out_shape=jax.ShapeDtypeStruct((devices,) + own.shape, own.dtype),
        in_specs=[pl.BlockSpec(memory_space=pltpu.VMEM)],
        out_specs=pl.BlockSpec(memory_space=pltpu.VMEM),
        scratch_shapes=[
            pltpu.SemaphoreType.DMA,
            pltpu.SemaphoreType.DMA((3, total, 4)),
            pltpu.SemaphoreType.DMA((3, devices)),
            pltpu.SemaphoreType.DMA((3, total)),
            pltpu.SemaphoreType.DMA((3, devices)),
        ],
        compiler_params=pltpu.CompilerParams(
            collective_id=0, has_side_effects=True, vmem_limit_bytes=12 * 1024 * 1024
        ),
        name="gather_slices",
    )(own)


def power_kernel(
    side, rot_count, classes_ref, rotations_ref, defocus_ref, images_ref, slices_ref, slope_ref, offset_ref, groups_ref, out_ref, power, acc
):
    step = pl.program_id(0)
    count, chunk, lanes = images_ref.shape
    shells = side // 2
    pitch = power.shape[0] // count

    @pl.when(step == 0)
    def _():
        acc[...] = jnp.zeros_like(acc)

    slope = slope_ref[...]
    offset = offset_ref[...]

    def one(i, carry):
        turns = defocus_ref[i].astype(jnp.float32) * slope + offset
        x = turns - ((turns + ROUND) - ROUND)
        y = x * x
        s = jnp.full_like(y, SINE[-1])
        for value in SINE[-2::-1]:
            s = s * y + value
        s = s * x
        d = images_ref[i].astype(jnp.float32) + s * slices_ref[classes_ref[i] * rot_count + rotations_ref[i]].astype(jnp.float32)
        power[pl.ds(pl.multiple_of(i * pitch, 8), chunk), :] = d * d
        return carry

    lax.fori_loop(0, count, one, 0, unroll=8)

    b = lax.broadcasted_iota(jnp.int32, (lanes, shells), 0)
    s = lax.broadcasted_iota(jnp.int32, (lanes, shells), 1)
    fb = jnp.where(b < side // 2, b, b - side)
    total = acc[...]
    for k in range(chunk // 2):
        a = step * (chunk // 2) + k
        fa = jnp.where(a < side // 2, a, a - side)
        r = fa * fa + fb * fb
        table = jnp.where((s * s <= r) & (r < (s + 1) * (s + 1)), 1.0, 0.0).astype(jnp.bfloat16)
        p = power[pl.ds(2 * k, count, stride=pitch), :] + power[pl.ds(2 * k + 1, count, stride=pitch), :]
        high = p.astype(jnp.bfloat16)
        low = (p - high.astype(jnp.float32)).astype(jnp.bfloat16)
        total = total + jnp.dot(
            jnp.concatenate([high, low], axis=1),
            jnp.concatenate([table, table], axis=0),
            preferred_element_type=jnp.float32,
        )
    acc[...] = total

    @pl.when(step == pl.num_programs(0) - 1)
    def _():
        groups = out_ref.shape[0]
        ids = lax.broadcasted_iota(jnp.int32, (groups, count), 0)
        member = jnp.where(ids == groups_ref[...], 1.0, 0.0)
        both = jnp.concatenate([acc[...], jnp.ones((count, out_ref.shape[1] - shells), jnp.float32)], axis=1)
        out_ref[...] = jnp.dot(
            member, both, precision=lax.Precision.HIGHEST, preferred_element_type=jnp.float32
        )


def shell_power(images, slices, classes, rotations, rot_count, defocus, groups, group_total):
    count, rows, side = images.shape
    chunk = 32
    offsets = np.arange(side)
    signed = np.where(offsets < side // 2, offsets, offsets - side)
    radius = (signed[:, None] ** 2 + signed[None, :] ** 2).astype(np.float64)
    spatial = np.repeat(radius / (side * PIXEL_SIZE) ** 2, 2, axis=0)
    slope = (0.5 * WAVELENGTH * spatial).astype(np.float32)
    offset = -0.25 * SPHERICAL * WAVELENGTH**3 * spatial**2 + math.asin(AMPLITUDE) / (2 * math.pi)
    offset = (offset - np.round(offset)).astype(np.float32)
    smem = pl.BlockSpec(memory_space=pltpu.SMEM)
    return pl.pallas_call(
        functools.partial(power_kernel, side, rot_count),
        grid=(rows // chunk,),
        out_shape=jax.ShapeDtypeStruct((group_total, 128), jnp.float32),
        in_specs=[
            smem,
            smem,
            smem,
            pl.BlockSpec((count, chunk, side), lambda i: (0, i, 0)),
            pl.BlockSpec((slices.shape[0], chunk, side), lambda i: (0, i, 0)),
            pl.BlockSpec((chunk, side), lambda i: (i, 0)),
            pl.BlockSpec((chunk, side), lambda i: (i, 0)),
            pl.BlockSpec((1, count), lambda i: (0, 0)),
        ],
        out_specs=pl.BlockSpec((group_total, 128), lambda i: (0, 0)),
        scratch_shapes=[
            pltpu.VMEM((count * (chunk + 8), side), jnp.float32),
            pltpu.VMEM((count, side // 2), jnp.float32),
        ],
        compiler_params=pltpu.CompilerParams(vmem_limit_bytes=20 * 1024 * 1024),
        name="shell_power",
    )(classes, rotations, defocus, images, slices, jnp.asarray(slope), jnp.asarray(offset), groups.reshape(1, count))


def exchange_kernel(sizes, shells, parts_ref, weight_ref, out_ref, held, send_sem, recv_sem):
    doms, clss = sizes
    n = doms * clss
    me = lax.axis_index("dom") * clss + lax.axis_index("cls")
    barrier = pltpu.get_barrier_semaphore()

    def device(k):
        peer = lax.rem(me + k, n)
        return peer, (peer // clss, lax.rem(peer, clss))

    def greet(k, carry):
        pl.semaphore_signal(barrier, inc=1, device_id=device(k)[1], device_id_type=MESH)
        return carry

    lax.fori_loop(1, n, greet, 0)
    pl.semaphore_wait(barrier, n - 1)

    def copy(k):
        peer, to = device(k)
        return pltpu.make_async_remote_copy(
            src_ref=parts_ref.at[peer],
            dst_ref=held.at[k],
            send_sem=send_sem.at[k],
            recv_sem=recv_sem.at[k],
            device_id=to,
            device_id_type=MESH,
        )

    def send(k, carry):
        copy(k).start()
        return carry

    lax.fori_loop(1, n, send, 0)

    def take(k, total):
        copy(k).wait_recv()
        return total + held[k]

    total = lax.fori_loop(1, n, take, parts_ref[me])

    def sent(k, carry):
        copy(k).wait_send()
        return carry

    lax.fori_loop(1, n, sent, 0)
    counts = total[:, shells : shells + 1]
    out_ref[...] = total[:, :shells] / (2.0 * counts * weight_ref[...])


def exchange(sizes, parts, weight):
    n = sizes[0] * sizes[1]
    shells = weight.shape[1]
    vmem = pl.BlockSpec(memory_space=pltpu.VMEM)
    return pl.pallas_call(
        functools.partial(exchange_kernel, sizes, shells),
        out_shape=jax.ShapeDtypeStruct((GROUPS_DEV, shells), jnp.float32),
        in_specs=[vmem, vmem],
        out_specs=vmem,
        scratch_shapes=[
            pltpu.VMEM((n, GROUPS_DEV, parts.shape[-1]), jnp.float32),
            pltpu.SemaphoreType.DMA((n,)),
            pltpu.SemaphoreType.DMA((n,)),
        ],
        compiler_params=pltpu.CompilerParams(
            collective_id=1, has_side_effects=True, vmem_limit_bytes=4 * 1024 * 1024
        ),
        name="exchange_groups",
    )(parts.reshape(n, GROUPS_DEV, parts.shape[-1]), weight)


PIECES = ((0, 4), (1, 6), (2, 6))
UNIT = 8


def fused_kernel(
    nz,
    side,
    classes_here,
    rot_count,
    layout,
    classes_ref,
    rotations_ref,
    defocus_ref,
    slope_ref,
    offset_ref,
    groups_ref,
    weight_ref,
    own_hbm,
    images_hbm,
    out_ref,
    *scratch,
):
    pieces, tiles = layout
    count = images_hbm.shape[0]
    shells = side // 2
    rows = 16 * tiles
    half = rows // 2
    bufs = scratch[: len(pieces)]
    (
        images,
        sine,
        power,
        table,
        acc,
        parts,
        held,
        local_sem,
        send_sem,
        recv_sem,
        pair_send,
        pair_recv,
        part_send,
        part_recv,
    ) = scratch[len(pieces) :]
    dom, cls = lax.axis_index("dom"), lax.axis_index("cls")
    x, core, y, z = cls // 2, cls % 2, dom % 2, dom // 2
    slot = classes_here * rot_count

    def device(x_, y_, z_, core_):
        return (z_ * 2 + y_, x_ * 2 + core_)

    partner = device(x, y, z, 1 - core)
    up, down = device(x, y, z + 1, core), device(x, y, z - 1, core)
    across = {"x": device(1 - x, y, z, core), "y": device(x, 1 - y, z, core)}

    def when(conds, fn):
        conds = [c for c in conds if c is not None]
        if not conds:
            fn()
        else:
            pl.when(functools.reduce(jnp.logical_and, conds))(fn)

    image_copies = []
    own_copies = []
    start = 0
    for p, (route, n) in enumerate(pieces):
        q1, q2 = (x, y) if route == 1 else (y, x)
        at = (((core * nz + z) * 2 + q1) * 2 + q2) * slot
        own_copies.append(
            pltpu.make_async_copy(
                own_hbm.at[:, pl.ds(16 * start, 16 * n), :], bufs[p].at[pl.ds(at, slot)], local_sem.at[p]
            )
        )
        start += n
    for c in own_copies:
        c.start()
    image_copy = pltpu.make_async_copy(images_hbm, images, local_sem.at[len(pieces)])
    image_copy.start()

    barrier = pltpu.get_barrier_semaphore()
    for to in (partner, across["x"], across["y"]):
        pl.semaphore_signal(barrier, inc=1, device_id=to, device_id_type=MESH)
    has_up, has_down = z < nz - 1, z > 0
    when([has_up], lambda: pl.semaphore_signal(barrier, inc=1, device_id=up, device_id_type=MESH))
    when([has_down], lambda: pl.semaphore_signal(barrier, inc=1, device_id=down, device_id_type=MESH))
    for c in own_copies:
        c.wait()
    pl.semaphore_wait(barrier, 3 + has_up.astype(jnp.int32) + has_down.astype(jnp.int32))

    events = []
    for p, (route, n) in enumerate(pieces):
        q1, q2 = (x, y) if route == 1 else (y, x)
        to_q1, to_q2 = (across["x"], across["y"]) if route == 1 else (across["y"], across["x"])
        buf = bufs[p]

        def region(core_, z_, a=None, b=None, buf=buf):
            first = (core_ * nz + z_) * 4 * slot
            size = 4 * slot
            if a is not None:
                first, size = first + a * 2 * slot, 2 * slot
            if b is not None:
                first, size = first + b * slot, slot
            return buf.at[pl.ds(first, size)]

        def link(stage, zs, number, where, to, p=p):
            return pltpu.make_async_remote_copy(
                src_ref=where,
                dst_ref=where,
                send_sem=send_sem.at[p, stage, number],
                recv_sem=recv_sem.at[p, stage, zs],
                device_id=to,
                device_id_type=MESH,
            )

        def pair(stage, zs, where, p=p):
            return pltpu.make_async_remote_copy(
                src_ref=where,
                dst_ref=where,
                send_sem=pair_send.at[p, stage, zs],
                recv_sem=pair_recv.at[p, stage, zs],
                device_id=partner,
                device_id_type=MESH,
            )

        reach = [(z, None, 0, None)]
        for t in range(1, nz):
            reach.append((z - t, z >= t, t, -1))
            reach.append((z + t, z + t < nz, t, 1))

        if route == 0:
            one = region(core, z, q1, q2)
            other = region(core, z, q1, 1 - q2)
            mine = region(core, z, q1)
            events.append((0, p, [], [], [(None, link(0, z, 0, one, to_q2))], None))
            events.append((1, p, [], [link(0, z, 0, other, to_q2)], [(None, link(1, z, 0, mine, to_q1))], None))
            for k, (zs, ok, t, way) in enumerate(reach):
                block = region(core, zs)
                sends = []
                if way in (None, -1):
                    sends.append((has_up, link(2, zs, 2 * k, block, up)))
                if way in (None, 1):
                    sends.append((has_down, link(2, zs, 2 * k + 1, block, down)))
                arrival = link(1, z, 0, region(core, z, 1 - q1), to_q1) if way is None else link(2, zs, 0, block, up)
                twin = region(1 - core, zs)
                events.append((2 + t, p, [ok], [arrival], sends, (pair(0, zs, block), pair(0, zs, twin))))
        else:
            for k, (zs, ok, t, way) in enumerate(reach):
                one = region(core, zs, q1, q2)
                sends = []
                if way in (None, -1):
                    sends.append((has_up, link(0, zs, 2 * k, one, up)))
                if way in (None, 1):
                    sends.append((has_down, link(0, zs, 2 * k + 1, one, down)))
                sends.append((None, link(1, zs, k, one, to_q2)))
                arrival = [] if way is None else [link(0, zs, 0, one, up)]
                events.append((t, p, [ok], arrival, sends, None))
                line, far = region(core, zs, q1), region(core, zs, 1 - q1)
                events.append(
                    (
                        t + 1,
                        p,
                        [ok],
                        [link(1, zs, 0, region(core, zs, q1, 1 - q2), to_q2)],
                        [(None, link(2, zs, k, line, to_q1))],
                        (pair(0, zs, line), pair(0, zs, region(1 - core, zs, q1))),
                    )
                )
                events.append(
                    (
                        t + 2,
                        p,
                        [ok],
                        [link(2, zs, 0, far, to_q1)],
                        [],
                        (pair(1, zs, far), pair(1, zs, region(1 - core, zs, 1 - q1))),
                    )
                )
    events.sort(key=lambda e: e[:2])

    def make_sine(i, carry):
        turns = defocus_ref[i].astype(jnp.float32) * slope_ref[...] + offset_ref[...]
        v = turns - ((turns + ROUND) - ROUND)
        w = v * v
        s = jnp.full_like(w, SINE[-1])
        for value in SINE[-2::-1]:
            s = s * w + value
        s = s * v
        base = pl.multiple_of(i * rows, 8)
        sine[pl.ds(base, half, stride=2), :] = s
        sine[pl.ds(base + 1, half, stride=2), :] = s
        return carry

    def sine_unit(j):
        return lambda: lax.fori_loop(j * UNIT, (j + 1) * UNIT, make_sine, 0, unroll=2)

    def make_table(a, carry):
        b = lax.broadcasted_iota(jnp.int32, (side, shells), 0)
        s = lax.broadcasted_iota(jnp.int32, (side, shells), 1)
        fb = jnp.where(b < side // 2, b, b - side)
        fa = jnp.where(a < side // 2, a, a - side)
        r = fa * fa + fb * fb
        inside = (s * s <= r) & (r < (s + 1) * (s + 1))
        table[a] = jnp.where(inside, 1.0, 0.0).astype(jnp.bfloat16)
        return carry

    def table_unit(j, n):
        return lambda: lax.fori_loop(j * n, (j + 1) * n, make_table, 0)

    fillers = [table_unit(j, half // 8) for j in range(8)] + [sine_unit(j) for j in range(count // UNIT)]
    fillers.reverse()
    spread = max(1, len(events) * 2 // 3 // len(fillers))

    acc[...] = jnp.zeros_like(acc)
    for number, (_, p, exists, arrivals, sends, twin) in enumerate(events):

        def arrive(arrivals=arrivals, sends=sends, twin=twin):
            for c in arrivals:
                c.wait_recv()
            for ok, c in sends:
                when([ok], c.start)
            if twin is not None:
                twin[0].start()

        when(exists, arrive)
        if fillers and number % spread == 0:
            fillers.pop()()
    while fillers:
        fillers.pop()()
    image_copy.wait()

    start = 0
    for p, (route, n) in enumerate(pieces):
        for _, p_, exists, arrivals, sends, twin in events:
            if p_ == p and twin is not None:
                when(exists, twin[1].wait_recv)
        size = 16 * n
        pitch = size + 8
        first = 16 * start

        def one(i, carry, p=p, route=route, size=size, pitch=pitch, first=first):
            c = classes_ref[i]
            owner, sub = (c, 0) if classes_here == 1 else (c // classes_here, c % classes_here)
            place = owner >> 1
            if route == 1:
                place = (place & ~3) | ((place & 1) << 1) | ((place >> 1) & 1)
            at = ((owner & 1) * (nz * 4) + place) * slot + sub * rot_count + rotations_ref[i]
            f = bufs[p][at].astype(jnp.float32)
            s = sine[pl.ds(pl.multiple_of(i * rows + first, 8), size), :]
            d = images[i, pl.ds(first, size), :].astype(jnp.float32) + s * f
            power[pl.ds(pl.multiple_of(i * pitch, 8), size), :] = d * d
            return carry

        lax.fori_loop(0, count, one, 0, unroll=8)
        total = acc[...]
        for k in range(size // 2):
            v = power[pl.ds(2 * k, count, stride=pitch), :] + power[pl.ds(2 * k + 1, count, stride=pitch), :]
            high = v.astype(jnp.bfloat16)
            low = (v - high.astype(jnp.float32)).astype(jnp.bfloat16)
            t = table[first // 2 + k]
            total = total + jnp.dot(
                jnp.concatenate([high, low], axis=1),
                jnp.concatenate([t, t], axis=0),
                preferred_element_type=jnp.float32,
            )
        acc[...] = total
        start += n

    owners, groups_here = parts.shape[:2]
    ids = lax.broadcasted_iota(jnp.int32, (owners * groups_here, count), 0)
    member = jnp.where(ids == groups_ref[...], 1.0, 0.0)
    both = jnp.concatenate([acc[...], jnp.ones((count, parts.shape[2] - shells), jnp.float32)], axis=1)
    parts[...] = jnp.dot(member, both, precision=lax.Precision.HIGHEST, preferred_element_type=jnp.float32).reshape(
        parts.shape
    )

    clss = lax.axis_size("cls")
    me = dom * clss + cls

    def part_copy(k):
        peer = lax.rem(me + k, owners)
        return pltpu.make_async_remote_copy(
            src_ref=parts.at[peer],
            dst_ref=held.at[k],
            send_sem=part_send.at[k],
            recv_sem=part_recv.at[k],
            device_id=(peer // clss, lax.rem(peer, clss)),
            device_id_type=MESH,
        )

    def send(k, carry):
        part_copy(k).start()
        return carry

    lax.fori_loop(1, owners, send, 0)
    for _, p, exists, arrivals, sends, twin in events:

        def done(sends=sends, twin=twin):
            for ok, c in sends:
                when([ok], c.wait_send)
            if twin is not None:
                twin[0].wait_send()

        when(exists, done)

    def take(k, total):
        part_copy(k).wait_recv()
        return total + held[k]

    total = lax.fori_loop(1, owners, take, parts[me])

    def sent(k, carry):
        part_copy(k).wait_send()
        return carry

    lax.fori_loop(1, owners, sent, 0)
    counts = total[:, shells : shells + 1]
    out_ref[...] = total[:, :shells] / (2.0 * counts * weight_ref[...])


def pixel_tables(side):
    offsets = np.arange(side)
    signed = np.where(offsets < side // 2, offsets, offsets - side)
    radius = (signed[:, None] ** 2 + signed[None, :] ** 2).astype(np.float64)
    spatial = radius / (side * PIXEL_SIZE) ** 2
    slope = (0.5 * WAVELENGTH * spatial).astype(np.float32)
    offset = -0.25 * SPHERICAL * WAVELENGTH**3 * spatial**2 + math.asin(AMPLITUDE) / (2 * math.pi)
    offset = (offset - np.round(offset)).astype(np.float32)
    s = np.arange(side // 2)[:, None, None]
    weight = ((s * s <= radius) & (radius < (s + 1) ** 2)).sum(axis=(1, 2)).astype(np.float32)
    return slope, offset, weight.reshape(1, -1)


def fused(nz, images, own, classes, rotations, defocus, groups, classes_here, rot_count, owners):
    count, rows, side = images.shape
    shells = side // 2
    pieces = PIECES
    tiles = sum(n for _, n in pieces)
    slots = owners * classes_here * rot_count
    slope, offset, weight = pixel_tables(side)
    smem = pl.BlockSpec(memory_space=pltpu.SMEM)
    vmem = pl.BlockSpec(memory_space=pltpu.VMEM)
    hbm = pl.BlockSpec(memory_space=pltpu.HBM)
    dma = pltpu.SemaphoreType.DMA
    widest = max(n for _, n in pieces)
    return pl.pallas_call(
        functools.partial(fused_kernel, nz, side, classes_here, rot_count, (pieces, tiles)),
        out_shape=jax.ShapeDtypeStruct((GROUPS_DEV, shells), jnp.float32),
        in_specs=[smem, smem, smem, vmem, vmem, vmem, vmem, hbm, hbm],
        out_specs=vmem,
        scratch_shapes=[pltpu.VMEM((slots, 16 * n, side), jnp.bfloat16) for _, n in pieces]
        + [
            pltpu.VMEM((count, 16 * tiles, side), jnp.bfloat16),
            pltpu.VMEM((count * 16 * tiles, side), jnp.float32),
            pltpu.VMEM((count * (16 * widest + 8), side), jnp.float32),
            pltpu.VMEM((8 * tiles, side, shells), jnp.bfloat16),
            pltpu.VMEM((count, shells), jnp.float32),
            pltpu.VMEM((owners, GROUPS_DEV, 128), jnp.float32),
            pltpu.VMEM((owners, GROUPS_DEV, 128), jnp.float32),
            dma((len(pieces) + 1,)),
            dma((len(pieces), 3, 4 * nz)),
            dma((len(pieces), 3, nz)),
            dma((len(pieces), 2, nz)),
            dma((len(pieces), 2, nz)),
            dma((owners,)),
            dma((owners,)),
        ],
        compiler_params=pltpu.CompilerParams(
            collective_id=0, has_side_effects=True, vmem_limit_bytes=60 * 1024 * 1024
        ),
        name="fused_spectrum",
    )(
        classes,
        rotations,
        defocus,
        jnp.asarray(slope),
        jnp.asarray(offset),
        groups.reshape(1, count),
        jnp.asarray(weight),
        own,
        images,
    )


def body(sizes, images, slices, classes, rotations, defocus, groups):
    doms, clss = sizes
    n = doms * clss
    count, _, pixels = images.shape
    side = math.isqrt(pixels)
    classes_here, rot_count = slices.shape[:2]

    def rows_of(array):
        lead = array.shape[:-2]
        split = array.reshape(lead + (2, side, side))
        return jnp.swapaxes(split, -3, -2).reshape(lead + (2 * side, side))

    own = rows_of(slices).reshape(classes_here * rot_count, 2 * side, side)
    if clss == 4 and doms % 2 == 0 and n <= 32:
        return fused(
            doms // 2, rows_of(images), own, classes, rotations, defocus, groups, classes_here, rot_count, n
        )
    ny = clss // 2
    if clss % 2 == 0 and doms % ny == 0 and n <= 32:
        every = gather((ny, ny, doms // ny), own)
    else:
        every = lax.all_gather(own, AXES, axis=0)
    every = every.reshape(n * own.shape[0], 2 * side, side)
    parts = shell_power(rows_of(images), every, classes, rotations, rot_count, defocus, groups, GROUPS_DEV * n)
    offsets = np.arange(side)
    signed = np.where(offsets < side // 2, offsets, offsets - side)
    radius = signed[:, None] ** 2 + signed[None, :] ** 2
    s = np.arange(side // 2)[:, None, None]
    weight = ((s * s <= radius) & (radius < (s + 1) ** 2)).sum(axis=(1, 2)).astype(np.float32)
    return exchange(sizes, parts, jnp.asarray(weight).reshape(1, -1))


def solution(mesh):
    sizes = (mesh.shape["dom"], mesh.shape["cls"])
    return jax.shard_map(
        functools.partial(body, sizes),
        mesh=mesh,
        in_specs=(
            P(AXES, None, None),
            P(AXES, None, None, None),
            P(AXES),
            P(AXES),
            P(AXES),
            P(AXES),
        ),
        out_specs=P(AXES, None),
        check_vma=False,
    )
```

```python
import functools
import math

import jax
import jax.numpy as jnp
import numpy as np
from jax import lax
from jax.experimental import pallas as pl
from jax.experimental.pallas import tpu as pltpu
from jax.sharding import PartitionSpec as P

GROUPS_DEV = 8
PIXEL_SIZE = 1.5
WAVELENGTH = 0.0197
SPHERICAL = 27000000.0
AMPLITUDE = 0.1
ROUND = 12582912.0
MESH = pl.DeviceIdType.MESH
AXES = ("dom", "cls")
ROUTES = (("x", "y", "z"), ("z", "y", "x"), ("z", "x", "y"))
SHARE = (8, 12, 12)


def sine_coefficients(terms):
    nodes = 0.5 * np.cos((np.arange(400) + 0.5) * math.pi / 400)
    nodes = nodes[np.abs(nodes) > 1e-3]
    basis = np.stack([nodes ** (2 * k + 1) for k in range(terms)], 1)
    return np.linalg.lstsq(basis, np.sin(2 * math.pi * nodes), rcond=None)[0]


SINE = [float(v) for v in sine_coefficients(5)]


def gather_kernel(shape, own_ref, out_ref, local_sem, send_sem, recv_sem, pair_send, pair_recv):
    size = dict(x=shape[0], y=shape[1], z=shape[2])
    dom, cls = lax.axis_index("dom"), lax.axis_index("cls")
    here = dict(x=cls // 2, y=dom % size["y"], z=dom // size["y"])
    core = cls % 2
    rows = out_ref.shape[2]
    starts = [0]
    for share in SHARE:
        starts.append(starts[-1] + rows * share // 32)

    def device(at, which):
        return (at["z"] * size["y"] + at["y"], at["x"] * 2 + which)

    def slot(at, which):
        d = device(at, which)
        return d[0] * (size["x"] * 2) + d[1]

    def moved(at, dim, step):
        new = dict(at)
        new[dim] = at[dim] + step
        return new

    ways = []
    for dim in "xyz":
        if size[dim] == 1:
            continue
        if size[dim] == 2:
            other = dict(here)
            other[dim] = 1 - here[dim]
            ways.append((dim, 0, other, None))
        else:
            ways.append((dim, 1, moved(here, dim, 1), here[dim] < size[dim] - 1))
            ways.append((dim, -1, moved(here, dim, -1), here[dim] > 0))

    def when(conds, fn):
        conds = [c for c in conds if c is not None]
        if not conds:
            fn()
        else:
            pl.when(functools.reduce(jnp.logical_and, conds))(fn)

    barrier = pltpu.get_barrier_semaphore()
    partner = device(here, 1 - core)
    pl.semaphore_signal(barrier, inc=1, device_id=partner, device_id_type=MESH)
    for dim, sign, other, ok in ways:

        def greet(other=other):
            pl.semaphore_signal(barrier, inc=1, device_id=device(other, core), device_id_type=MESH)

        when([ok], greet)
    peers = 1
    for dim, sign, other, ok in ways:
        peers = peers + (1 if ok is None else ok.astype(jnp.int32))
    pl.semaphore_wait(barrier, peers)

    mine = slot(here, core)
    local = pltpu.make_async_copy(own_ref, out_ref.at[mine], local_sem)
    local.start()

    def part(ref, index):
        return ref.at[:, pl.ds(starts[index], starts[index + 1] - starts[index]), :]

    def copy(index, source, src_slot, to, way, own):
        src = part(own_ref, index) if own else part(out_ref.at[src_slot], index)
        return pltpu.make_async_remote_copy(
            src_ref=src,
            dst_ref=part(out_ref.at[src_slot], index),
            send_sem=send_sem.at[index, source, way],
            recv_sem=recv_sem.at[index, src_slot],
            device_id=to,
            device_id_type=MESH,
        )

    def pair_copy(index, source, src_slot, own):
        src = part(own_ref, index) if own else part(out_ref.at[src_slot], index)
        return pltpu.make_async_remote_copy(
            src_ref=src,
            dst_ref=part(out_ref.at[src_slot], index),
            send_sem=pair_send.at[index, source],
            recv_sem=pair_recv.at[index, src_slot],
            device_id=partner,
            device_id_type=MESH,
        )

    choices = {}
    for dim in "xyz":
        n = size[dim]
        if n == 1:
            choices[dim] = [(0, here[dim], None, 0)]
        elif n == 2:
            choices[dim] = [(0, here[dim], None, 0), (0, 1 - here[dim], None, 1)]
        else:
            listed = [(0, here[dim], None, 0)]
            for t in range(1, n):
                listed.append((1, here[dim] - t, here[dim] >= t, t))
                listed.append((-1, here[dim] + t, here[dim] + t < n, t))
            choices[dim] = listed
    events = []
    for ix, cx in enumerate(choices["x"]):
        for iy, cy in enumerate(choices["y"]):
            for iz, cz in enumerate(choices["z"]):
                pick = dict(x=cx, y=cy, z=cz)
                depth = cx[3] + cy[3] + cz[3]
                number = (ix * len(choices["y"]) + iy) * len(choices["z"]) + iz
                for index in range(3):
                    events.append((depth, index, number, pick))
    events.sort(key=lambda e: e[:3])
    finish = []
    for depth, index, number, pick in events:
        at = {dim: pick[dim][1] for dim in "xyz"}
        exists = [pick[dim][2] for dim in "xyz"]
        src_slot = slot(at, core)
        order = ROUTES[index]
        last = max([k for k, dim in enumerate(order) if pick[dim][3] > 0], default=-1)
        sends = []
        for number_way, (dim, sign, other, ok) in enumerate(ways):
            k = order.index(dim)
            if k < last:
                continue
            if k == last and (size[dim] == 2 or sign != pick[dim][0]):
                continue
            sends.append((number_way, device(other, core), ok))

        def arrive(index=index, number=number, src_slot=src_slot, depth=depth, sends=sends):
            own = depth == 0
            if not own:
                copy(index, number, src_slot, partner, 0, False).wait_recv()
            for way, to, ok in sends:
                when([ok], copy(index, number, src_slot, to, way, own).start)
            pair_copy(index, number, src_slot, own).start()

        def done(index=index, number=number, src_slot=src_slot, depth=depth, sends=sends, at=at):
            own = depth == 0
            for way, to, ok in sends:
                when([ok], copy(index, number, src_slot, to, way, own).wait_send)
            pair_copy(index, number, src_slot, own).wait_send()
            pair_copy(index, number, slot(at, 1 - core), False).wait_recv()

        when(exists, arrive)
        finish.append((exists, done))
    for exists, done in finish:
        when(exists, done)
    local.wait()


def gather(shape, own):
    devices = 2 * shape[0] * shape[1] * shape[2]
    total = 1
    for n in shape:
        total *= n if n <= 2 else 2 * n - 1
    return pl.pallas_call(
        functools.partial(gather_kernel, shape),
        out_shape=jax.ShapeDtypeStruct((devices,) + own.shape, own.dtype),
        in_specs=[pl.BlockSpec(memory_space=pltpu.VMEM)],
        out_specs=pl.BlockSpec(memory_space=pltpu.VMEM),
        scratch_shapes=[
            pltpu.SemaphoreType.DMA,
            pltpu.SemaphoreType.DMA((3, total, 4)),
            pltpu.SemaphoreType.DMA((3, devices)),
            pltpu.SemaphoreType.DMA((3, total)),
            pltpu.SemaphoreType.DMA((3, devices)),
        ],
        compiler_params=pltpu.CompilerParams(
            collective_id=0, has_side_effects=True, vmem_limit_bytes=12 * 1024 * 1024
        ),
        name="gather_slices",
    )(own)


def power_kernel(
    side, rot_count, classes_ref, rotations_ref, defocus_ref, images_ref, slices_ref, slope_ref, offset_ref, groups_ref, out_ref, power, acc
):
    step = pl.program_id(0)
    count, chunk, lanes = images_ref.shape
    shells = side // 2
    pitch = power.shape[0] // count

    @pl.when(step == 0)
    def _():
        acc[...] = jnp.zeros_like(acc)

    slope = slope_ref[...]
    offset = offset_ref[...]

    def one(i, carry):
        turns = defocus_ref[i].astype(jnp.float32) * slope + offset
        x = turns - ((turns + ROUND) - ROUND)
        y = x * x
        s = jnp.full_like(y, SINE[-1])
        for value in SINE[-2::-1]:
            s = s * y + value
        s = s * x
        d = images_ref[i].astype(jnp.float32) + s * slices_ref[classes_ref[i] * rot_count + rotations_ref[i]].astype(jnp.float32)
        power[pl.ds(pl.multiple_of(i * pitch, 8), chunk), :] = d * d
        return carry

    lax.fori_loop(0, count, one, 0, unroll=8)

    b = lax.broadcasted_iota(jnp.int32, (lanes, shells), 0)
    s = lax.broadcasted_iota(jnp.int32, (lanes, shells), 1)
    fb = jnp.where(b < side // 2, b, b - side)
    total = acc[...]
    for k in range(chunk // 2):
        a = step * (chunk // 2) + k
        fa = jnp.where(a < side // 2, a, a - side)
        r = fa * fa + fb * fb
        table = jnp.where((s * s <= r) & (r < (s + 1) * (s + 1)), 1.0, 0.0).astype(jnp.bfloat16)
        p = power[pl.ds(2 * k, count, stride=pitch), :] + power[pl.ds(2 * k + 1, count, stride=pitch), :]
        high = p.astype(jnp.bfloat16)
        low = (p - high.astype(jnp.float32)).astype(jnp.bfloat16)
        total = total + jnp.dot(
            jnp.concatenate([high, low], axis=1),
            jnp.concatenate([table, table], axis=0),
            preferred_element_type=jnp.float32,
        )
    acc[...] = total

    @pl.when(step == pl.num_programs(0) - 1)
    def _():
        groups = out_ref.shape[0]
        ids = lax.broadcasted_iota(jnp.int32, (groups, count), 0)
        member = jnp.where(ids == groups_ref[...], 1.0, 0.0)
        both = jnp.concatenate([acc[...], jnp.ones((count, out_ref.shape[1] - shells), jnp.float32)], axis=1)
        out_ref[...] = jnp.dot(
            member, both, precision=lax.Precision.HIGHEST, preferred_element_type=jnp.float32
        )


def shell_power(images, slices, classes, rotations, rot_count, defocus, groups, group_total):
    count, rows, side = images.shape
    chunk = 32
    offsets = np.arange(side)
    signed = np.where(offsets < side // 2, offsets, offsets - side)
    radius = (signed[:, None] ** 2 + signed[None, :] ** 2).astype(np.float64)
    spatial = np.repeat(radius / (side * PIXEL_SIZE) ** 2, 2, axis=0)
    slope = (0.5 * WAVELENGTH * spatial).astype(np.float32)
    offset = -0.25 * SPHERICAL * WAVELENGTH**3 * spatial**2 + math.asin(AMPLITUDE) / (2 * math.pi)
    offset = (offset - np.round(offset)).astype(np.float32)
    smem = pl.BlockSpec(memory_space=pltpu.SMEM)
    return pl.pallas_call(
        functools.partial(power_kernel, side, rot_count),
        grid=(rows // chunk,),
        out_shape=jax.ShapeDtypeStruct((group_total, 128), jnp.float32),
        in_specs=[
            smem,
            smem,
            smem,
            pl.BlockSpec((count, chunk, side), lambda i: (0, i, 0)),
            pl.BlockSpec((slices.shape[0], chunk, side), lambda i: (0, i, 0)),
            pl.BlockSpec((chunk, side), lambda i: (i, 0)),
            pl.BlockSpec((chunk, side), lambda i: (i, 0)),
            pl.BlockSpec((1, count), lambda i: (0, 0)),
        ],
        out_specs=pl.BlockSpec((group_total, 128), lambda i: (0, 0)),
        scratch_shapes=[
            pltpu.VMEM((count * (chunk + 8), side), jnp.float32),
            pltpu.VMEM((count, side // 2), jnp.float32),
        ],
        compiler_params=pltpu.CompilerParams(vmem_limit_bytes=20 * 1024 * 1024),
        name="shell_power",
    )(classes, rotations, defocus, images, slices, jnp.asarray(slope), jnp.asarray(offset), groups.reshape(1, count))


def exchange_kernel(sizes, shells, parts_ref, weight_ref, out_ref, held, send_sem, recv_sem):
    doms, clss = sizes
    n = doms * clss
    me = lax.axis_index("dom") * clss + lax.axis_index("cls")
    barrier = pltpu.get_barrier_semaphore()

    def device(k):
        peer = lax.rem(me + k, n)
        return peer, (peer // clss, lax.rem(peer, clss))

    def greet(k, carry):
        pl.semaphore_signal(barrier, inc=1, device_id=device(k)[1], device_id_type=MESH)
        return carry

    lax.fori_loop(1, n, greet, 0)
    pl.semaphore_wait(barrier, n - 1)

    def copy(k):
        peer, to = device(k)
        return pltpu.make_async_remote_copy(
            src_ref=parts_ref.at[peer],
            dst_ref=held.at[k],
            send_sem=send_sem.at[k],
            recv_sem=recv_sem.at[k],
            device_id=to,
            device_id_type=MESH,
        )

    def send(k, carry):
        copy(k).start()
        return carry

    lax.fori_loop(1, n, send, 0)

    def take(k, total):
        copy(k).wait_recv()
        return total + held[k]

    total = lax.fori_loop(1, n, take, parts_ref[me])

    def sent(k, carry):
        copy(k).wait_send()
        return carry

    lax.fori_loop(1, n, sent, 0)
    counts = total[:, shells : shells + 1]
    out_ref[...] = total[:, :shells] / (2.0 * counts * weight_ref[...])


def exchange(sizes, parts, weight):
    n = sizes[0] * sizes[1]
    shells = weight.shape[1]
    vmem = pl.BlockSpec(memory_space=pltpu.VMEM)
    return pl.pallas_call(
        functools.partial(exchange_kernel, sizes, shells),
        out_shape=jax.ShapeDtypeStruct((GROUPS_DEV, shells), jnp.float32),
        in_specs=[vmem, vmem],
        out_specs=vmem,
        scratch_shapes=[
            pltpu.VMEM((n, GROUPS_DEV, parts.shape[-1]), jnp.float32),
            pltpu.SemaphoreType.DMA((n,)),
            pltpu.SemaphoreType.DMA((n,)),
        ],
        compiler_params=pltpu.CompilerParams(
            collective_id=1, has_side_effects=True, vmem_limit_bytes=4 * 1024 * 1024
        ),
        name="exchange_groups",
    )(parts.reshape(n, GROUPS_DEV, parts.shape[-1]), weight)


PIECES = ((0, 3), (1, 6), (2, 5))
ORDER = (
    (0, "o", 0), (1, "o", 0), (2, "o", 0), (0, "x", 0), (1, "a", 0), (1, "z", 1), (2, "z", 1), (2, "a", 0),
    (1, "z", 2), (2, "z", 2), (1, "a", 1), (0, "y", 0), (1, "z", 3), (2, "z", 3), (2, "b", 0), (2, "a", 1),
    (1, "a", 2), (2, "a", 2), (0, "z", 1), (2, "a", 3), (1, "b", 1), (1, "a", 3), (1, "b", 0), (0, "z", 2),
    (2, "b", 3), (1, "b", 2), (2, "b", 1), (1, "b", 3), (0, "z", 3), (2, "b", 2),
)
UNIT = 8
TILE = 8


def folded_rows(side):
    half = side // 2
    low, high = half - TILE, half + TILE
    kept = np.concatenate([np.arange(low), np.arange(high, side)])
    other = kept.copy()
    other[low - TILE : low] = half - 1 - np.arange(TILE)
    other[low : low + TILE] = high - np.arange(TILE)
    return kept, other


def folded_radius(side):
    half = side // 2
    offsets = np.arange(side)
    signed = np.where(offsets < half, offsets, offsets - side)
    radius = signed[:, None] ** 2 + signed[None, :] ** 2
    kept, other = folded_rows(side)
    own, far = radius[kept], np.roll(radius[other], half, axis=1)
    inside = own < half * half
    fold = (other != kept)[:, None] & ~inside
    assert not np.any((other != kept)[:, None] & inside & (far < half * half))
    packed = np.where(fold, far, own)
    assert np.sum(packed < half * half) == np.sum(radius < half * half)
    return packed


def fold(keep, far, shifted, first_row, side):
    lines = 2 * TILE
    order = [(-i if shifted else TILE - 1 - i) % TILE for i in range(TILE)]
    far = far.astype(jnp.float32)
    far = jnp.concatenate([far[2 * k : 2 * k + 2] for k in order], axis=0)
    far = pltpu.roll(far, side // 2, axis=1)
    a = first_row + lax.broadcasted_iota(jnp.int32, (lines, side), 0) // 2
    b = lax.broadcasted_iota(jnp.int32, (lines, side), 1)
    fa = jnp.where(a < side // 2, a, a - side)
    fb = jnp.where(b < side // 2, b, b - side)
    inside = fa * fa + fb * fb < (side // 2) * (side // 2)
    return jnp.where(inside, keep.astype(jnp.float32), far).astype(keep.dtype)


def rank(name, pieces):
    if name in ORDER:
        return ORDER.index(name)
    p, kind, t = name
    depth = dict(o=0, x=1, y=2, a=1, b=2, z=2 if pieces[p][0] == 0 else 0)[kind] + t
    return len(ORDER) + depth * len(pieces) + p


def fused_kernel(
    nz,
    side,
    classes_here,
    rot_count,
    layout,
    classes_ref,
    rotations_ref,
    defocus_ref,
    slope_ref,
    offset_ref,
    groups_ref,
    weight_ref,
    own_hbm,
    images_hbm,
    out_ref,
    *scratch,
):
    pieces, tiles = layout
    count = images_hbm.shape[0]
    shells = side // 2
    rows = 16 * tiles
    half = rows // 2
    bufs = scratch[: len(pieces)]
    (
        images,
        image_rim,
        own_rim,
        sine,
        power,
        table,
        acc,
        parts,
        held,
        local_sem,
        image_sem,
        send_sem,
        recv_sem,
        pair_send,
        pair_recv,
        part_send,
        part_recv,
    ) = scratch[len(pieces) :]
    dom, cls = lax.axis_index("dom"), lax.axis_index("cls")
    x, core, y, z = cls // 2, cls % 2, dom % 2, dom // 2
    slot = classes_here * rot_count

    def device(x_, y_, z_, core_):
        return (z_ * 2 + y_, x_ * 2 + core_)

    partner = device(x, y, z, 1 - core)
    up, down = device(x, y, z + 1, core), device(x, y, z - 1, core)
    across = {"x": device(1 - x, y, z, core), "y": device(x, 1 - y, z, core)}

    def when(conds, fn):
        conds = [c for c in conds if c is not None]
        if not conds:
            fn()
        else:
            pl.when(functools.reduce(jnp.logical_and, conds))(fn)

    line = 2 * TILE
    rim = tiles // 2 - 1
    own_copies = [
        pltpu.make_async_copy(own_hbm.at[:, pl.ds(line * rim, 4 * line), :], own_rim, local_sem.at[0])
    ]
    rim_stores = []
    start = 0
    for p, (route, n) in enumerate(pieces):
        q1, q2 = (x, y) if route == 1 else (y, x)
        at = (((core * nz + z) * 2 + q1) * 2 + q2) * slot
        for first, last, skip in ((start, min(start + n, rim), 0), (max(start, rim + 2), start + n, 2)):
            if first < last:
                own_copies.append(
                    pltpu.make_async_copy(
                        own_hbm.at[:, pl.ds(line * (first + skip), line * (last - first)), :],
                        bufs[p].at[pl.ds(at, slot), pl.ds(line * (first - start), line * (last - first)), :],
                        local_sem.at[len(own_copies)],
                    )
                )
        for k in range(2):
            if start <= rim + k < start + n:
                rim_stores.append((p, at, line * (rim + k - start), k))
        start += n
    for c in own_copies:
        c.start()
    edge = line * rim
    image_copies = [
        pltpu.make_async_copy(images_hbm.at[:, pl.ds(edge, 4 * line), :], image_rim, image_sem.at[0]),
        pltpu.make_async_copy(images_hbm.at[:, pl.ds(0, edge), :], images.at[:, pl.ds(0, edge), :], image_sem.at[1]),
        pltpu.make_async_copy(
            images_hbm.at[:, pl.ds(edge + 4 * line, edge), :],
            images.at[:, pl.ds(edge + 2 * line, edge), :],
            image_sem.at[2],
        ),
    ]
    for c in image_copies:
        c.start()

    def folded(ref, i, k):
        keep = ref[i, pl.ds(3 * line * k, line), :]
        far = ref[i, pl.ds(line * (1 + k), line), :]
        return fold(keep, far, k == 1, TILE * (rim + 3 * k), side)

    barrier = pltpu.get_barrier_semaphore()
    for to in (partner, across["x"], across["y"]):
        pl.semaphore_signal(barrier, inc=1, device_id=to, device_id_type=MESH)
    has_up, has_down = z < nz - 1, z > 0
    when([has_up], lambda: pl.semaphore_signal(barrier, inc=1, device_id=up, device_id_type=MESH))
    when([has_down], lambda: pl.semaphore_signal(barrier, inc=1, device_id=down, device_id_type=MESH))
    for c in own_copies:
        c.wait()
    for p, at, row, k in rim_stores:
        for j in range(slot):
            bufs[p][at + j, pl.ds(row, line), :] = folded(own_rim, j, k)
    pl.semaphore_wait(barrier, 3 + has_up.astype(jnp.int32) + has_down.astype(jnp.int32))

    events = []
    for p, (route, n) in enumerate(pieces):
        q1, q2 = (x, y) if route == 1 else (y, x)
        to_q1, to_q2 = (across["x"], across["y"]) if route == 1 else (across["y"], across["x"])
        buf = bufs[p]

        def region(core_, z_, a=None, b=None, buf=buf):
            first = (core_ * nz + z_) * 4 * slot
            size = 4 * slot
            if a is not None:
                first, size = first + a * 2 * slot, 2 * slot
            if b is not None:
                first, size = first + b * slot, slot
            return buf.at[pl.ds(first, size)]

        def link(stage, zs, number, where, to, p=p):
            return pltpu.make_async_remote_copy(
                src_ref=where,
                dst_ref=where,
                send_sem=send_sem.at[p, stage, number],
                recv_sem=recv_sem.at[p, stage, zs],
                device_id=to,
                device_id_type=MESH,
            )

        def pair(stage, zs, where, p=p):
            return pltpu.make_async_remote_copy(
                src_ref=where,
                dst_ref=where,
                send_sem=pair_send.at[p, stage, zs],
                recv_sem=pair_recv.at[p, stage, zs],
                device_id=partner,
                device_id_type=MESH,
            )

        reach = [(z, None, 0, None)]
        for t in range(1, nz):
            reach.append((z - t, z >= t, t, -1))
            reach.append((z + t, z + t < nz, t, 1))

        if route == 0:
            one = region(core, z, q1, q2)
            other = region(core, z, q1, 1 - q2)
            mine = region(core, z, q1)
            events.append(((p, "o", 0), p, [], [], [(None, link(0, z, 0, one, to_q2))], None))
            events.append(((p, "x", 0), p, [], [link(0, z, 0, other, to_q2)], [(None, link(1, z, 0, mine, to_q1))], None))
            for k, (zs, ok, t, way) in enumerate(reach):
                block = region(core, zs)
                sends = []
                if way in (None, -1):
                    sends.append((has_up, link(2, zs, 2 * k, block, up)))
                if way in (None, 1):
                    sends.append((has_down, link(2, zs, 2 * k + 1, block, down)))
                arrival = link(1, z, 0, region(core, z, 1 - q1), to_q1) if way is None else link(2, zs, 0, block, up)
                twin = region(1 - core, zs)
                name = (p, "z" if t else "y", t)
                events.append((name, p, [ok], [arrival], sends, (pair(0, zs, block), pair(0, zs, twin))))
        else:
            for k, (zs, ok, t, way) in enumerate(reach):
                one = region(core, zs, q1, q2)
                sends = []
                if way in (None, -1):
                    sends.append((has_up, link(0, zs, 2 * k, one, up)))
                if way in (None, 1):
                    sends.append((has_down, link(0, zs, 2 * k + 1, one, down)))
                sends.append((None, link(1, zs, k, one, to_q2)))
                arrival = [] if way is None else [link(0, zs, 0, one, up)]
                events.append(((p, "z" if t else "o", t), p, [ok], arrival, sends, None))
                near, far = region(core, zs, q1), region(core, zs, 1 - q1)
                events.append(
                    (
                        (p, "a", t),
                        p,
                        [ok],
                        [link(1, zs, 0, region(core, zs, q1, 1 - q2), to_q2)],
                        [(None, link(2, zs, k, near, to_q1))],
                        (pair(0, zs, near), pair(0, zs, region(1 - core, zs, q1))),
                    )
                )
                events.append(
                    (
                        (p, "b", t),
                        p,
                        [ok],
                        [link(2, zs, 0, far, to_q1)],
                        [],
                        (pair(1, zs, far), pair(1, zs, region(1 - core, zs, 1 - q1))),
                    )
                )
    events.sort(key=lambda e: rank(e[0], pieces))

    def make_sine(i, carry):
        turns = defocus_ref[i].astype(jnp.float32) * slope_ref[...] + offset_ref[...]
        v = turns - ((turns + ROUND) - ROUND)
        w = v * v
        s = jnp.full_like(w, SINE[-1])
        for value in SINE[-2::-1]:
            s = s * w + value
        s = s * v
        base = pl.multiple_of(i * rows, 8)
        sine[pl.ds(base, half, stride=2), :] = s
        sine[pl.ds(base + 1, half, stride=2), :] = s
        return carry

    def sine_unit(j):
        return lambda: lax.fori_loop(j * UNIT, (j + 1) * UNIT, make_sine, 0, unroll=2)

    def make_table(a, carry):
        b = lax.broadcasted_iota(jnp.int32, (side, shells), 0)
        s = lax.broadcasted_iota(jnp.int32, (side, shells), 1)
        low = TILE * (rim + 1)
        row = jnp.where(a < low, a, a + 2 * TILE)
        far = jnp.where(a < low, side // 2 - 1 + TILE * rim - a, side // 2 + TILE + low - a)
        fb = jnp.where(b < side // 2, b, b - side)
        gb = b - side // 2
        fa = jnp.where(row < side // 2, row, row - side)
        ga = jnp.where(far < side // 2, far, far - side)
        r = fa * fa + fb * fb
        folds = (a >= TILE * rim) & (a < TILE * (rim + 2)) & (a != low)
        r = jnp.where(folds & (r >= (side // 2) * (side // 2)), ga * ga + gb * gb, r)
        inside = (s * s <= r) & (r < (s + 1) * (s + 1))
        table[a] = jnp.where(inside, 1.0, 0.0).astype(jnp.bfloat16)
        return carry

    def table_unit(j, n):
        return lambda: lax.fori_loop(j * n, (j + 1) * n, make_table, 0)

    def fold_image(i, carry):
        for k in range(2):
            images[i, pl.ds(line * (rim + k), line), :] = folded(image_rim, i, k)
        return carry

    def fold_unit(j):
        def run():
            if j == 0:
                image_copies[0].wait()
            lax.fori_loop(j * 4 * UNIT, (j + 1) * 4 * UNIT, fold_image, 0, unroll=4)

        return run

    fillers = [table_unit(j, half // 8) for j in range(8)] + [sine_unit(j) for j in range(count // UNIT)]
    fillers += [fold_unit(j) for j in range(count // (4 * UNIT))]
    fillers.reverse()
    spread = max(1, len(events) * 2 // 3 // len(fillers))

    acc[...] = jnp.zeros_like(acc)
    for number, (_, p, exists, arrivals, sends, twin) in enumerate(events):

        def arrive(arrivals=arrivals, sends=sends, twin=twin):
            for c in arrivals:
                c.wait_recv()
            for ok, c in sends:
                when([ok], c.start)
            if twin is not None:
                twin[0].start()

        when(exists, arrive)
        if fillers and number % spread == 0:
            fillers.pop()()
    while fillers:
        fillers.pop()()
    for c in image_copies[1:]:
        c.wait()

    start = 0
    for p, (route, n) in enumerate(pieces):
        for _, p_, exists, arrivals, sends, twin in events:
            if p_ == p and twin is not None:
                when(exists, twin[1].wait_recv)
        size = 16 * n
        pitch = size + 8
        first = 16 * start

        def one(i, carry, p=p, route=route, size=size, pitch=pitch, first=first):
            c = classes_ref[i]
            owner, sub = (c, 0) if classes_here == 1 else (c // classes_here, c % classes_here)
            place = owner >> 1
            if route == 1:
                place = (place & ~3) | ((place & 1) << 1) | ((place >> 1) & 1)
            at = ((owner & 1) * (nz * 4) + place) * slot + sub * rot_count + rotations_ref[i]
            f = bufs[p][at].astype(jnp.float32)
            s = sine[pl.ds(pl.multiple_of(i * rows + first, 8), size), :]
            d = images[i, pl.ds(first, size), :].astype(jnp.float32) + s * f
            power[pl.ds(pl.multiple_of(i * pitch, 8), size), :] = d * d
            return carry

        lax.fori_loop(0, count, one, 0, unroll=8)
        total = acc[...]
        for k in range(size // 2):
            v = power[pl.ds(2 * k, count, stride=pitch), :] + power[pl.ds(2 * k + 1, count, stride=pitch), :]
            high = v.astype(jnp.bfloat16)
            low = (v - high.astype(jnp.float32)).astype(jnp.bfloat16)
            t = table[first // 2 + k]
            total = total + jnp.dot(
                jnp.concatenate([high, low], axis=1),
                jnp.concatenate([t, t], axis=0),
                preferred_element_type=jnp.float32,
            )
        acc[...] = total
        start += n

    owners, groups_here = parts.shape[:2]
    ids = lax.broadcasted_iota(jnp.int32, (owners * groups_here, count), 0)
    member = jnp.where(ids == groups_ref[...], 1.0, 0.0)
    both = jnp.concatenate([acc[...], jnp.ones((count, parts.shape[2] - shells), jnp.float32)], axis=1)
    parts[...] = jnp.dot(member, both, precision=lax.Precision.HIGHEST, preferred_element_type=jnp.float32).reshape(
        parts.shape
    )

    clss = lax.axis_size("cls")
    me = dom * clss + cls

    def part_copy(k):
        peer = lax.rem(me + k, owners)
        return pltpu.make_async_remote_copy(
            src_ref=parts.at[peer],
            dst_ref=held.at[k],
            send_sem=part_send.at[k],
            recv_sem=part_recv.at[k],
            device_id=(peer // clss, lax.rem(peer, clss)),
            device_id_type=MESH,
        )

    def send(k, carry):
        part_copy(k).start()
        return carry

    lax.fori_loop(1, owners, send, 0)
    for _, p, exists, arrivals, sends, twin in events:

        def done(sends=sends, twin=twin):
            for ok, c in sends:
                when([ok], c.wait_send)
            if twin is not None:
                twin[0].wait_send()

        when(exists, done)

    def take(k, total):
        part_copy(k).wait_recv()
        return total + held[k]

    total = lax.fori_loop(1, owners, take, parts[me])

    def sent(k, carry):
        part_copy(k).wait_send()
        return carry

    lax.fori_loop(1, owners, sent, 0)
    counts = total[:, shells : shells + 1]
    out_ref[...] = total[:, :shells] / (2.0 * counts * weight_ref[...])


def pixel_tables(side):
    offsets = np.arange(side)
    signed = np.where(offsets < side // 2, offsets, offsets - side)
    radius = (signed[:, None] ** 2 + signed[None, :] ** 2).astype(np.float64)
    spatial = folded_radius(side).astype(np.float64) / (side * PIXEL_SIZE) ** 2
    slope = (0.5 * WAVELENGTH * spatial).astype(np.float32)
    offset = -0.25 * SPHERICAL * WAVELENGTH**3 * spatial**2 + math.asin(AMPLITUDE) / (2 * math.pi)
    offset = (offset - np.round(offset)).astype(np.float32)
    s = np.arange(side // 2)[:, None, None]
    weight = ((s * s <= radius) & (radius < (s + 1) ** 2)).sum(axis=(1, 2)).astype(np.float32)
    return slope, offset, weight.reshape(1, -1)


def fused(nz, images, own, classes, rotations, defocus, groups, classes_here, rot_count, owners):
    count, rows, side = images.shape
    shells = side // 2
    pieces = PIECES
    tiles = sum(n for _, n in pieces)
    slots = owners * classes_here * rot_count
    slope, offset, weight = pixel_tables(side)
    smem = pl.BlockSpec(memory_space=pltpu.SMEM)
    vmem = pl.BlockSpec(memory_space=pltpu.VMEM)
    hbm = pl.BlockSpec(memory_space=pltpu.HBM)
    dma = pltpu.SemaphoreType.DMA
    widest = max(n for _, n in pieces)
    return pl.pallas_call(
        functools.partial(fused_kernel, nz, side, classes_here, rot_count, (pieces, tiles)),
        out_shape=jax.ShapeDtypeStruct((GROUPS_DEV, shells), jnp.float32),
        in_specs=[smem, smem, smem, vmem, vmem, vmem, vmem, hbm, hbm],
        out_specs=vmem,
        scratch_shapes=[pltpu.VMEM((slots, 16 * n, side), jnp.bfloat16) for _, n in pieces]
        + [
            pltpu.VMEM((count, 16 * tiles, side), jnp.bfloat16),
            pltpu.VMEM((count, 8 * TILE, side), jnp.bfloat16),
            pltpu.VMEM((classes_here * rot_count, 8 * TILE, side), jnp.bfloat16),
            pltpu.VMEM((count * 16 * tiles, side), jnp.float32),
            pltpu.VMEM((count * (16 * widest + 8), side), jnp.float32),
            pltpu.VMEM((8 * tiles, side, shells), jnp.bfloat16),
            pltpu.VMEM((count, shells), jnp.float32),
            pltpu.VMEM((owners, GROUPS_DEV, 128), jnp.float32),
            pltpu.VMEM((owners, GROUPS_DEV, 128), jnp.float32),
            dma((2 * len(pieces) + 1,)),
            dma((3,)),
            dma((len(pieces), 3, 4 * nz)),
            dma((len(pieces), 3, nz)),
            dma((len(pieces), 2, nz)),
            dma((len(pieces), 2, nz)),
            dma((owners,)),
            dma((owners,)),
        ],
        compiler_params=pltpu.CompilerParams(
            collective_id=0, has_side_effects=True, vmem_limit_bytes=62 * 1024 * 1024
        ),
        name="fused_spectrum",
    )(
        classes,
        rotations,
        defocus,
        jnp.asarray(slope),
        jnp.asarray(offset),
        groups.reshape(1, count),
        jnp.asarray(weight),
        own,
        images,
    )


def body(sizes, images, slices, classes, rotations, defocus, groups):
    doms, clss = sizes
    n = doms * clss
    count, _, pixels = images.shape
    side = math.isqrt(pixels)
    classes_here, rot_count = slices.shape[:2]

    def rows_of(array):
        lead = array.shape[:-2]
        split = array.reshape(lead + (2, side, side))
        return jnp.swapaxes(split, -3, -2).reshape(lead + (2 * side, side))

    own = rows_of(slices).reshape(classes_here * rot_count, 2 * side, side)
    if clss == 4 and doms % 2 == 0 and n <= 32 and side == 16 * TILE:
        return fused(
            doms // 2, rows_of(images), own, classes, rotations, defocus, groups, classes_here, rot_count, n
        )
    ny = clss // 2
    if clss % 2 == 0 and doms % ny == 0 and n <= 32:
        every = gather((ny, ny, doms // ny), own)
    else:
        every = lax.all_gather(own, AXES, axis=0)
    every = every.reshape(n * own.shape[0], 2 * side, side)
    parts = shell_power(rows_of(images), every, classes, rotations, rot_count, defocus, groups, GROUPS_DEV * n)
    offsets = np.arange(side)
    signed = np.where(offsets < side // 2, offsets, offsets - side)
    radius = signed[:, None] ** 2 + signed[None, :] ** 2
    s = np.arange(side // 2)[:, None, None]
    weight = ((s * s <= radius) & (radius < (s + 1) ** 2)).sum(axis=(1, 2)).astype(np.float32)
    return exchange(sizes, parts, jnp.asarray(weight).reshape(1, -1))


def solution(mesh):
    sizes = (mesh.shape["dom"], mesh.shape["cls"])
    return jax.shard_map(
        functools.partial(body, sizes),
        mesh=mesh,
        in_specs=(
            P(AXES, None, None),
            P(AXES, None, None, None),
            P(AXES),
            P(AXES),
            P(AXES),
            P(AXES),
        ),
        out_specs=P(AXES, None),
        check_vma=False,
    )
```

```python
import functools
import math

import jax
import jax.numpy as jnp
import numpy as np
from jax import lax
from jax.experimental import pallas as pl
from jax.experimental.pallas import tpu as pltpu
from jax.sharding import PartitionSpec as P

GROUPS_DEV = 8
PIXEL_SIZE = 1.5
WAVELENGTH = 0.0197
SPHERICAL = 27000000.0
AMPLITUDE = 0.1
ROUND = 12582912.0
MESH = pl.DeviceIdType.MESH
AXES = ("dom", "cls")
ROUTES = (("x", "y", "z"), ("z", "y", "x"), ("z", "x", "y"))
SHARE = (8, 12, 12)


def sine_coefficients(terms):
    nodes = 0.5 * np.cos((np.arange(400) + 0.5) * math.pi / 400)
    nodes = nodes[np.abs(nodes) > 1e-3]
    basis = np.stack([nodes ** (2 * k + 1) for k in range(terms)], 1)
    return np.linalg.lstsq(basis, np.sin(2 * math.pi * nodes), rcond=None)[0]


SINE = [float(v) for v in sine_coefficients(5)]


def gather_kernel(shape, own_ref, out_ref, local_sem, send_sem, recv_sem, pair_send, pair_recv):
    size = dict(x=shape[0], y=shape[1], z=shape[2])
    dom, cls = lax.axis_index("dom"), lax.axis_index("cls")
    here = dict(x=cls // 2, y=dom % size["y"], z=dom // size["y"])
    core = cls % 2
    rows = out_ref.shape[2]
    starts = [0]
    for share in SHARE:
        starts.append(starts[-1] + rows * share // 32)

    def device(at, which):
        return (at["z"] * size["y"] + at["y"], at["x"] * 2 + which)

    def slot(at, which):
        d = device(at, which)
        return d[0] * (size["x"] * 2) + d[1]

    def moved(at, dim, step):
        new = dict(at)
        new[dim] = at[dim] + step
        return new

    ways = []
    for dim in "xyz":
        if size[dim] == 1:
            continue
        if size[dim] == 2:
            other = dict(here)
            other[dim] = 1 - here[dim]
            ways.append((dim, 0, other, None))
        else:
            ways.append((dim, 1, moved(here, dim, 1), here[dim] < size[dim] - 1))
            ways.append((dim, -1, moved(here, dim, -1), here[dim] > 0))

    def when(conds, fn):
        conds = [c for c in conds if c is not None]
        if not conds:
            fn()
        else:
            pl.when(functools.reduce(jnp.logical_and, conds))(fn)

    barrier = pltpu.get_barrier_semaphore()
    partner = device(here, 1 - core)
    pl.semaphore_signal(barrier, inc=1, device_id=partner, device_id_type=MESH)
    for dim, sign, other, ok in ways:

        def greet(other=other):
            pl.semaphore_signal(barrier, inc=1, device_id=device(other, core), device_id_type=MESH)

        when([ok], greet)
    peers = 1
    for dim, sign, other, ok in ways:
        peers = peers + (1 if ok is None else ok.astype(jnp.int32))
    pl.semaphore_wait(barrier, peers)

    mine = slot(here, core)
    local = pltpu.make_async_copy(own_ref, out_ref.at[mine], local_sem)
    local.start()

    def part(ref, index):
        return ref.at[:, pl.ds(starts[index], starts[index + 1] - starts[index]), :]

    def copy(index, source, src_slot, to, way, own):
        src = part(own_ref, index) if own else part(out_ref.at[src_slot], index)
        return pltpu.make_async_remote_copy(
            src_ref=src,
            dst_ref=part(out_ref.at[src_slot], index),
            send_sem=send_sem.at[index, source, way],
            recv_sem=recv_sem.at[index, src_slot],
            device_id=to,
            device_id_type=MESH,
        )

    def pair_copy(index, source, src_slot, own):
        src = part(own_ref, index) if own else part(out_ref.at[src_slot], index)
        return pltpu.make_async_remote_copy(
            src_ref=src,
            dst_ref=part(out_ref.at[src_slot], index),
            send_sem=pair_send.at[index, source],
            recv_sem=pair_recv.at[index, src_slot],
            device_id=partner,
            device_id_type=MESH,
        )

    choices = {}
    for dim in "xyz":
        n = size[dim]
        if n == 1:
            choices[dim] = [(0, here[dim], None, 0)]
        elif n == 2:
            choices[dim] = [(0, here[dim], None, 0), (0, 1 - here[dim], None, 1)]
        else:
            listed = [(0, here[dim], None, 0)]
            for t in range(1, n):
                listed.append((1, here[dim] - t, here[dim] >= t, t))
                listed.append((-1, here[dim] + t, here[dim] + t < n, t))
            choices[dim] = listed
    events = []
    for ix, cx in enumerate(choices["x"]):
        for iy, cy in enumerate(choices["y"]):
            for iz, cz in enumerate(choices["z"]):
                pick = dict(x=cx, y=cy, z=cz)
                depth = cx[3] + cy[3] + cz[3]
                number = (ix * len(choices["y"]) + iy) * len(choices["z"]) + iz
                for index in range(3):
                    events.append((depth, index, number, pick))
    events.sort(key=lambda e: e[:3])
    finish = []
    for depth, index, number, pick in events:
        at = {dim: pick[dim][1] for dim in "xyz"}
        exists = [pick[dim][2] for dim in "xyz"]
        src_slot = slot(at, core)
        order = ROUTES[index]
        last = max([k for k, dim in enumerate(order) if pick[dim][3] > 0], default=-1)
        sends = []
        for number_way, (dim, sign, other, ok) in enumerate(ways):
            k = order.index(dim)
            if k < last:
                continue
            if k == last and (size[dim] == 2 or sign != pick[dim][0]):
                continue
            sends.append((number_way, device(other, core), ok))

        def arrive(index=index, number=number, src_slot=src_slot, depth=depth, sends=sends):
            own = depth == 0
            if not own:
                copy(index, number, src_slot, partner, 0, False).wait_recv()
            for way, to, ok in sends:
                when([ok], copy(index, number, src_slot, to, way, own).start)
            pair_copy(index, number, src_slot, own).start()

        def done(index=index, number=number, src_slot=src_slot, depth=depth, sends=sends, at=at):
            own = depth == 0
            for way, to, ok in sends:
                when([ok], copy(index, number, src_slot, to, way, own).wait_send)
            pair_copy(index, number, src_slot, own).wait_send()
            pair_copy(index, number, slot(at, 1 - core), False).wait_recv()

        when(exists, arrive)
        finish.append((exists, done))
    for exists, done in finish:
        when(exists, done)
    local.wait()


def gather(shape, own):
    devices = 2 * shape[0] * shape[1] * shape[2]
    total = 1
    for n in shape:
        total *= n if n <= 2 else 2 * n - 1
    return pl.pallas_call(
        functools.partial(gather_kernel, shape),
        out_shape=jax.ShapeDtypeStruct((devices,) + own.shape, own.dtype),
        in_specs=[pl.BlockSpec(memory_space=pltpu.VMEM)],
        out_specs=pl.BlockSpec(memory_space=pltpu.VMEM),
        scratch_shapes=[
            pltpu.SemaphoreType.DMA,
            pltpu.SemaphoreType.DMA((3, total, 4)),
            pltpu.SemaphoreType.DMA((3, devices)),
            pltpu.SemaphoreType.DMA((3, total)),
            pltpu.SemaphoreType.DMA((3, devices)),
        ],
        compiler_params=pltpu.CompilerParams(
            collective_id=0, has_side_effects=True, vmem_limit_bytes=12 * 1024 * 1024
        ),
        name="gather_slices",
    )(own)


def power_kernel(
    side, rot_count, classes_ref, rotations_ref, defocus_ref, images_ref, slices_ref, slope_ref, offset_ref, groups_ref, out_ref, power, acc
):
    step = pl.program_id(0)
    count, chunk, lanes = images_ref.shape
    shells = side // 2
    pitch = power.shape[0] // count

    @pl.when(step == 0)
    def _():
        acc[...] = jnp.zeros_like(acc)

    slope = slope_ref[...]
    offset = offset_ref[...]

    def one(i, carry):
        turns = defocus_ref[i].astype(jnp.float32) * slope + offset
        x = turns - ((turns + ROUND) - ROUND)
        y = x * x
        s = jnp.full_like(y, SINE[-1])
        for value in SINE[-2::-1]:
            s = s * y + value
        s = s * x
        d = images_ref[i].astype(jnp.float32) + s * slices_ref[classes_ref[i] * rot_count + rotations_ref[i]].astype(jnp.float32)
        power[pl.ds(pl.multiple_of(i * pitch, 8), chunk), :] = d * d
        return carry

    lax.fori_loop(0, count, one, 0, unroll=8)

    b = lax.broadcasted_iota(jnp.int32, (lanes, shells), 0)
    s = lax.broadcasted_iota(jnp.int32, (lanes, shells), 1)
    fb = jnp.where(b < side // 2, b, b - side)
    total = acc[...]
    for k in range(chunk // 2):
        a = step * (chunk // 2) + k
        fa = jnp.where(a < side // 2, a, a - side)
        r = fa * fa + fb * fb
        table = jnp.where((s * s <= r) & (r < (s + 1) * (s + 1)), 1.0, 0.0).astype(jnp.bfloat16)
        p = power[pl.ds(2 * k, count, stride=pitch), :] + power[pl.ds(2 * k + 1, count, stride=pitch), :]
        high = p.astype(jnp.bfloat16)
        low = (p - high.astype(jnp.float32)).astype(jnp.bfloat16)
        total = total + jnp.dot(
            jnp.concatenate([high, low], axis=1),
            jnp.concatenate([table, table], axis=0),
            preferred_element_type=jnp.float32,
        )
    acc[...] = total

    @pl.when(step == pl.num_programs(0) - 1)
    def _():
        groups = out_ref.shape[0]
        ids = lax.broadcasted_iota(jnp.int32, (groups, count), 0)
        member = jnp.where(ids == groups_ref[...], 1.0, 0.0)
        both = jnp.concatenate([acc[...], jnp.ones((count, out_ref.shape[1] - shells), jnp.float32)], axis=1)
        out_ref[...] = jnp.dot(
            member, both, precision=lax.Precision.HIGHEST, preferred_element_type=jnp.float32
        )


def shell_power(images, slices, classes, rotations, rot_count, defocus, groups, group_total):
    count, rows, side = images.shape
    chunk = 32
    offsets = np.arange(side)
    signed = np.where(offsets < side // 2, offsets, offsets - side)
    radius = (signed[:, None] ** 2 + signed[None, :] ** 2).astype(np.float64)
    spatial = np.repeat(radius / (side * PIXEL_SIZE) ** 2, 2, axis=0)
    slope = (0.5 * WAVELENGTH * spatial).astype(np.float32)
    offset = -0.25 * SPHERICAL * WAVELENGTH**3 * spatial**2 + math.asin(AMPLITUDE) / (2 * math.pi)
    offset = (offset - np.round(offset)).astype(np.float32)
    smem = pl.BlockSpec(memory_space=pltpu.SMEM)
    return pl.pallas_call(
        functools.partial(power_kernel, side, rot_count),
        grid=(rows // chunk,),
        out_shape=jax.ShapeDtypeStruct((group_total, 128), jnp.float32),
        in_specs=[
            smem,
            smem,
            smem,
            pl.BlockSpec((count, chunk, side), lambda i: (0, i, 0)),
            pl.BlockSpec((slices.shape[0], chunk, side), lambda i: (0, i, 0)),
            pl.BlockSpec((chunk, side), lambda i: (i, 0)),
            pl.BlockSpec((chunk, side), lambda i: (i, 0)),
            pl.BlockSpec((1, count), lambda i: (0, 0)),
        ],
        out_specs=pl.BlockSpec((group_total, 128), lambda i: (0, 0)),
        scratch_shapes=[
            pltpu.VMEM((count * (chunk + 8), side), jnp.float32),
            pltpu.VMEM((count, side // 2), jnp.float32),
        ],
        compiler_params=pltpu.CompilerParams(vmem_limit_bytes=20 * 1024 * 1024),
        name="shell_power",
    )(classes, rotations, defocus, images, slices, jnp.asarray(slope), jnp.asarray(offset), groups.reshape(1, count))


def exchange_kernel(sizes, shells, parts_ref, weight_ref, out_ref, held, send_sem, recv_sem):
    doms, clss = sizes
    n = doms * clss
    me = lax.axis_index("dom") * clss + lax.axis_index("cls")
    barrier = pltpu.get_barrier_semaphore()

    def device(k):
        peer = lax.rem(me + k, n)
        return peer, (peer // clss, lax.rem(peer, clss))

    def greet(k, carry):
        pl.semaphore_signal(barrier, inc=1, device_id=device(k)[1], device_id_type=MESH)
        return carry

    lax.fori_loop(1, n, greet, 0)
    pl.semaphore_wait(barrier, n - 1)

    def copy(k):
        peer, to = device(k)
        return pltpu.make_async_remote_copy(
            src_ref=parts_ref.at[peer],
            dst_ref=held.at[k],
            send_sem=send_sem.at[k],
            recv_sem=recv_sem.at[k],
            device_id=to,
            device_id_type=MESH,
        )

    def send(k, carry):
        copy(k).start()
        return carry

    lax.fori_loop(1, n, send, 0)

    def take(k, total):
        copy(k).wait_recv()
        return total + held[k]

    total = lax.fori_loop(1, n, take, parts_ref[me])

    def sent(k, carry):
        copy(k).wait_send()
        return carry

    lax.fori_loop(1, n, sent, 0)
    counts = total[:, shells : shells + 1]
    out_ref[...] = total[:, :shells] / (2.0 * counts * weight_ref[...])


def exchange(sizes, parts, weight):
    n = sizes[0] * sizes[1]
    shells = weight.shape[1]
    vmem = pl.BlockSpec(memory_space=pltpu.VMEM)
    return pl.pallas_call(
        functools.partial(exchange_kernel, sizes, shells),
        out_shape=jax.ShapeDtypeStruct((GROUPS_DEV, shells), jnp.float32),
        in_specs=[vmem, vmem],
        out_specs=vmem,
        scratch_shapes=[
            pltpu.VMEM((n, GROUPS_DEV, parts.shape[-1]), jnp.float32),
            pltpu.SemaphoreType.DMA((n,)),
            pltpu.SemaphoreType.DMA((n,)),
        ],
        compiler_params=pltpu.CompilerParams(
            collective_id=1, has_side_effects=True, vmem_limit_bytes=4 * 1024 * 1024
        ),
        name="exchange_groups",
    )(parts.reshape(n, GROUPS_DEV, parts.shape[-1]), weight)


PIECES = ((0, (0, 6, 13)), (1, (1, 2, 3, 10, 11, 12)), (2, (4, 5, 7, 8, 9)))
ORDER = (
    (0, "o", 0), (1, "o", 0), (2, "o", 0), (0, "x", 0), (1, "a", 0), (1, "z", 1), (2, "z", 1), (2, "a", 0),
    (1, "z", 2), (2, "z", 2), (1, "a", 1), (0, "y", 0), (1, "z", 3), (2, "z", 3), (2, "b", 0), (2, "a", 1),
    (1, "a", 2), (2, "a", 2), (0, "z", 1), (2, "a", 3), (1, "b", 1), (1, "a", 3), (1, "b", 0), (0, "z", 2),
    (2, "b", 3), (1, "b", 2), (2, "b", 1), (1, "b", 3), (0, "z", 3), (2, "b", 2),
)
UNIT = 8
TILE = 8


def folded_rows(side):
    half = side // 2
    low, high = half - TILE, half + TILE
    kept = np.concatenate([np.arange(low), np.arange(high, side)])
    other = kept.copy()
    other[low - TILE : low] = half - 1 - np.arange(TILE)
    other[low : low + TILE] = high - np.arange(TILE)
    return kept, other


def folded_radius(side):
    half = side // 2
    offsets = np.arange(side)
    signed = np.where(offsets < half, offsets, offsets - side)
    radius = signed[:, None] ** 2 + signed[None, :] ** 2
    kept, other = folded_rows(side)
    own, far = radius[kept], np.roll(radius[other], half, axis=1)
    inside = own < half * half
    fold = (other != kept)[:, None] & ~inside
    assert not np.any((other != kept)[:, None] & inside & (far < half * half))
    packed = np.where(fold, far, own)
    assert np.sum(packed < half * half) == np.sum(radius < half * half)
    return packed


def runs_of(tiles):
    runs = []
    for k, t in enumerate(tiles):
        if runs and runs[-1][1] + runs[-1][2] == t:
            runs[-1][2] += 1
        else:
            runs.append([k, t, 1])
    return runs


def row_groups(tiles, side):
    place = {TILE * t + r: TILE * k + r for k, t in enumerate(tiles) for r in range(TILE)}
    kept, other = folded_rows(side)
    plain = {int(a): j for j, a in enumerate(kept) if other[j] == a and (a == 0 or other[j - 1] == kept[j - 1])}
    groups, used = [], set()
    for j in sorted(place):
        if j in used:
            continue
        a = int(kept[j])
        mate = plain.get(side - a) if plain.get(a) == j else None
        if mate is not None and mate != j and mate in place:
            used.add(mate)
            groups.append((j, (place[j], place[mate])))
        else:
            groups.append((j, (place[j],)))
    return groups


def fold(keep, far, shifted, first_row, side):
    lines = 2 * TILE
    order = [(-i if shifted else TILE - 1 - i) % TILE for i in range(TILE)]
    far = far.astype(jnp.float32)
    far = jnp.concatenate([far[2 * k : 2 * k + 2] for k in order], axis=0)
    far = pltpu.roll(far, side // 2, axis=1)
    a = first_row + lax.broadcasted_iota(jnp.int32, (lines, side), 0) // 2
    b = lax.broadcasted_iota(jnp.int32, (lines, side), 1)
    fa = jnp.where(a < side // 2, a, a - side)
    fb = jnp.where(b < side // 2, b, b - side)
    inside = fa * fa + fb * fb < (side // 2) * (side // 2)
    return jnp.where(inside, keep.astype(jnp.float32), far).astype(keep.dtype)


def rank(name, pieces):
    if name in ORDER:
        return ORDER.index(name)
    p, kind, t = name
    depth = dict(o=0, x=1, y=2, a=1, b=2, z=2 if pieces[p][0] == 0 else 0)[kind] + t
    return len(ORDER) + depth * len(pieces) + p


def fused_kernel(
    nz,
    side,
    classes_here,
    rot_count,
    layout,
    classes_hbm,
    rotations_hbm,
    defocus_hbm,
    slope_hbm,
    offset_hbm,
    groups_hbm,
    weight_hbm,
    own_hbm,
    images_hbm,
    out_ref,
    *scratch,
):
    pieces, tiles = layout
    count = images_hbm.shape[0]
    shells = side // 2
    rows = 16 * tiles
    half = rows // 2
    bufs = scratch[: len(pieces)]
    (
        classes_ref,
        rotations_ref,
        defocus_ref,
        slope_ref,
        offset_ref,
        groups_ref,
        weight_ref,
        images,
        image_rim,
        own_rim,
        sine,
        power,
        table,
        acc,
        parts,
        held,
        local_sem,
        image_sem,
        small_sem,
        send_sem,
        recv_sem,
        pair_send,
        pair_recv,
        part_send,
        part_recv,
    ) = scratch[len(pieces) :]
    dom, cls = lax.axis_index("dom"), lax.axis_index("cls")
    x, core, y, z = cls // 2, cls % 2, dom % 2, dom // 2
    slot = classes_here * rot_count

    def device(x_, y_, z_, core_):
        return (z_ * 2 + y_, x_ * 2 + core_)

    partner = device(x, y, z, 1 - core)
    up, down = device(x, y, z + 1, core), device(x, y, z - 1, core)
    across = {"x": device(1 - x, y, z, core), "y": device(x, 1 - y, z, core)}

    def when(conds, fn):
        conds = [c for c in conds if c is not None]
        if not conds:
            fn()
        else:
            pl.when(functools.reduce(jnp.logical_and, conds))(fn)

    barrier = pltpu.get_barrier_semaphore()
    for to in (partner, across["x"], across["y"]):
        pl.semaphore_signal(barrier, inc=1, device_id=to, device_id_type=MESH)
    has_up, has_down = z < nz - 1, z > 0
    when([has_up], lambda: pl.semaphore_signal(barrier, inc=1, device_id=up, device_id_type=MESH))
    when([has_down], lambda: pl.semaphore_signal(barrier, inc=1, device_id=down, device_id_type=MESH))

    line = 2 * TILE
    rim = tiles // 2 - 1
    own_copies = [
        pltpu.make_async_copy(own_hbm.at[:, pl.ds(line * rim, 4 * line), :], own_rim, local_sem.at[0])
    ]
    rim_stores = []
    for p, (route, held_tiles) in enumerate(pieces):
        q1, q2 = (x, y) if route == 1 else (y, x)
        at = (((core * nz + z) * 2 + q1) * 2 + q2) * slot
        for k, t in enumerate(held_tiles):
            if rim <= t < rim + 2:
                rim_stores.append((p, at, line * k, t - rim))
        for k, t, n in runs_of([t if not rim <= t < rim + 2 else -line * t for t in held_tiles]):
            if t >= 0:
                own_copies.append(
                    pltpu.make_async_copy(
                        own_hbm.at[:, pl.ds(line * (t + 2 * (t > rim)), line * n), :],
                        bufs[p].at[pl.ds(at, slot), pl.ds(line * k, line * n), :],
                        local_sem.at[len(own_copies)],
                    )
                )
    for c in own_copies:
        c.start()
    edge = line * rim
    image_copies = [
        pltpu.make_async_copy(images_hbm.at[:, pl.ds(edge, 4 * line), :], image_rim, image_sem.at[0]),
        pltpu.make_async_copy(images_hbm.at[:, pl.ds(0, edge), :], images.at[:, pl.ds(0, edge), :], image_sem.at[1]),
        pltpu.make_async_copy(
            images_hbm.at[:, pl.ds(edge + 4 * line, edge), :],
            images.at[:, pl.ds(edge + 2 * line, edge), :],
            image_sem.at[2],
        ),
    ]
    small = (
        (slope_hbm, slope_ref),
        (offset_hbm, offset_ref),
        (defocus_hbm, defocus_ref),
        (classes_hbm, classes_ref),
        (rotations_hbm, rotations_ref),
        (groups_hbm, groups_ref),
        (weight_hbm, weight_ref),
    )
    small_copies = [pltpu.make_async_copy(src, dst, small_sem.at[k]) for k, (src, dst) in enumerate(small)]
    for c in small_copies + image_copies:
        c.start()

    def folded(ref, i, k):
        keep = ref[i, pl.ds(3 * line * k, line), :]
        far = ref[i, pl.ds(line * (1 + k), line), :]
        return fold(keep, far, k == 1, TILE * (rim + 3 * k), side)

    for c in own_copies:
        c.wait()
    for p, at, row, k in rim_stores:
        for j in range(slot):
            bufs[p][at + j, pl.ds(row, line), :] = folded(own_rim, j, k)
    pl.semaphore_wait(barrier, 3 + has_up.astype(jnp.int32) + has_down.astype(jnp.int32))

    events = []
    for p, (route, n) in enumerate(pieces):
        q1, q2 = (x, y) if route == 1 else (y, x)
        to_q1, to_q2 = (across["x"], across["y"]) if route == 1 else (across["y"], across["x"])
        buf = bufs[p]

        def region(core_, z_, a=None, b=None, buf=buf):
            first = (core_ * nz + z_) * 4 * slot
            size = 4 * slot
            if a is not None:
                first, size = first + a * 2 * slot, 2 * slot
            if b is not None:
                first, size = first + b * slot, slot
            return buf.at[pl.ds(first, size)]

        def link(stage, zs, number, where, to, p=p):
            return pltpu.make_async_remote_copy(
                src_ref=where,
                dst_ref=where,
                send_sem=send_sem.at[p, stage, number],
                recv_sem=recv_sem.at[p, stage, zs],
                device_id=to,
                device_id_type=MESH,
            )

        def pair(stage, zs, where, p=p):
            return pltpu.make_async_remote_copy(
                src_ref=where,
                dst_ref=where,
                send_sem=pair_send.at[p, stage, zs],
                recv_sem=pair_recv.at[p, stage, zs],
                device_id=partner,
                device_id_type=MESH,
            )

        reach = [(z, None, 0, None)]
        for t in range(1, nz):
            reach.append((z - t, z >= t, t, -1))
            reach.append((z + t, z + t < nz, t, 1))

        if route == 0:
            one = region(core, z, q1, q2)
            other = region(core, z, q1, 1 - q2)
            mine = region(core, z, q1)
            events.append(((p, "o", 0), p, [], [], [(None, link(0, z, 0, one, to_q2))], None))
            events.append(((p, "x", 0), p, [], [link(0, z, 0, other, to_q2)], [(None, link(1, z, 0, mine, to_q1))], None))
            for k, (zs, ok, t, way) in enumerate(reach):
                block = region(core, zs)
                sends = []
                if way in (None, -1):
                    sends.append((has_up, link(2, zs, 2 * k, block, up)))
                if way in (None, 1):
                    sends.append((has_down, link(2, zs, 2 * k + 1, block, down)))
                arrival = link(1, z, 0, region(core, z, 1 - q1), to_q1) if way is None else link(2, zs, 0, block, up)
                twin = region(1 - core, zs)
                name = (p, "z" if t else "y", t)
                events.append((name, p, [ok], [arrival], sends, (pair(0, zs, block), pair(0, zs, twin))))
        else:
            for k, (zs, ok, t, way) in enumerate(reach):
                one = region(core, zs, q1, q2)
                sends = []
                if way in (None, -1):
                    sends.append((has_up, link(0, zs, 2 * k, one, up)))
                if way in (None, 1):
                    sends.append((has_down, link(0, zs, 2 * k + 1, one, down)))
                sends.append((None, link(1, zs, k, one, to_q2)))
                arrival = [] if way is None else [link(0, zs, 0, one, up)]
                events.append(((p, "z" if t else "o", t), p, [ok], arrival, sends, None))
                near, far = region(core, zs, q1), region(core, zs, 1 - q1)
                events.append(
                    (
                        (p, "a", t),
                        p,
                        [ok],
                        [link(1, zs, 0, region(core, zs, q1, 1 - q2), to_q2)],
                        [(None, link(2, zs, k, near, to_q1))],
                        (pair(0, zs, near), pair(0, zs, region(1 - core, zs, q1))),
                    )
                )
                events.append(
                    (
                        (p, "b", t),
                        p,
                        [ok],
                        [link(2, zs, 0, far, to_q1)],
                        [],
                        (pair(1, zs, far), pair(1, zs, region(1 - core, zs, 1 - q1))),
                    )
                )
    events.sort(key=lambda e: rank(e[0], pieces))

    def make_sine(i, carry):
        turns = defocus_ref[i].astype(jnp.float32) * slope_ref[...] + offset_ref[...]
        v = turns - ((turns + ROUND) - ROUND)
        w = v * v
        s = jnp.full_like(w, SINE[-1])
        for value in SINE[-2::-1]:
            s = s * w + value
        s = s * v
        base = pl.multiple_of(i * rows, 8)
        sine[pl.ds(base, half, stride=2), :] = s
        sine[pl.ds(base + 1, half, stride=2), :] = s
        return carry

    def sine_unit(j):
        return lambda: lax.fori_loop(j * UNIT, (j + 1) * UNIT, make_sine, 0, unroll=2)

    def make_table(a, carry):
        b = lax.broadcasted_iota(jnp.int32, (side, shells), 0)
        s = lax.broadcasted_iota(jnp.int32, (side, shells), 1)
        low = TILE * (rim + 1)
        row = jnp.where(a < low, a, a + 2 * TILE)
        far = jnp.where(a < low, side // 2 - 1 + TILE * rim - a, side // 2 + TILE + low - a)
        fb = jnp.where(b < side // 2, b, b - side)
        gb = b - side // 2
        fa = jnp.where(row < side // 2, row, row - side)
        ga = jnp.where(far < side // 2, far, far - side)
        r = fa * fa + fb * fb
        folds = (a >= TILE * rim) & (a < TILE * (rim + 2)) & (a != low)
        r = jnp.where(folds & (r >= (side // 2) * (side // 2)), ga * ga + gb * gb, r)
        inside = (s * s <= r) & (r < (s + 1) * (s + 1))
        table[a] = jnp.where(inside, 1.0, 0.0).astype(jnp.bfloat16)
        return carry

    def table_unit(j, n):
        return lambda: lax.fori_loop(j * n, (j + 1) * n, make_table, 0)

    def fold_image(i, carry):
        for k in range(2):
            images[i, pl.ds(line * (rim + k), line), :] = folded(image_rim, i, k)
        return carry

    def fold_unit(j):
        def run():
            if j == 0:
                image_copies[0].wait()
            lax.fori_loop(j * 4 * UNIT, (j + 1) * 4 * UNIT, fold_image, 0, unroll=4)

        return run

    fillers = [table_unit(j, half // 8) for j in range(8)] + [sine_unit(j) for j in range(count // UNIT)]
    fillers += [fold_unit(j) for j in range(count // (4 * UNIT))]
    fillers.reverse()
    waits = small_copies[:3]
    spread = max(1, len(events) * 2 // 3 // len(fillers))

    acc[...] = jnp.zeros_like(acc)
    for number, (_, p, exists, arrivals, sends, twin) in enumerate(events):

        def arrive(arrivals=arrivals, sends=sends, twin=twin):
            for c in arrivals:
                c.wait_recv()
            for ok, c in sends:
                when([ok], c.start)
            if twin is not None:
                twin[0].start()

        when(exists, arrive)
        if number == len(events) // len(pieces) // 8:
            for c in waits:
                c.wait()
        if fillers and number > len(events) // len(pieces) // 8 and number % spread == 0:
            fillers.pop()()
    while fillers:
        fillers.pop()()
    for c in image_copies[1:] + small_copies[3:]:
        c.wait()

    for p, (route, held_tiles) in enumerate(pieces):
        for _, p_, exists, arrivals, sends, twin in events:
            if p_ == p and twin is not None:
                when(exists, twin[1].wait_recv)
        pitch = line * len(held_tiles) + TILE

        def one(i, carry, p=p, route=route, held_tiles=held_tiles, pitch=pitch):
            c = classes_ref[i]
            owner, sub = (c, 0) if classes_here == 1 else (c // classes_here, c % classes_here)
            place = owner >> 1
            if route == 1:
                place = (place & ~3) | ((place & 1) << 1) | ((place >> 1) & 1)
            at = ((owner & 1) * (nz * 4) + place) * slot + sub * rot_count + rotations_ref[i]
            for k, t, n in runs_of(held_tiles):
                f = bufs[p][at, pl.ds(line * k, line * n), :].astype(jnp.float32)
                s = sine[pl.ds(pl.multiple_of(i * rows + line * t, 8), line * n), :]
                d = images[i, pl.ds(line * t, line * n), :].astype(jnp.float32) + s * f
                power[pl.ds(pl.multiple_of(i * pitch + line * k, 8), line * n), :] = d * d
            return carry

        lax.fori_loop(0, count, one, 0, unroll=8)
        total = acc[...]
        for j, places in row_groups(held_tiles, side):
            v = None
            for k in places:
                for part in range(2):
                    w = power[pl.ds(2 * k + part, count, stride=pitch), :]
                    v = w if v is None else v + w
            high = v.astype(jnp.bfloat16)
            low = (v - high.astype(jnp.float32)).astype(jnp.bfloat16)
            t = table[j]
            total = total + jnp.dot(
                jnp.concatenate([high, low], axis=1),
                jnp.concatenate([t, t], axis=0),
                preferred_element_type=jnp.float32,
            )
        acc[...] = total

    owners, groups_here = parts.shape[:2]
    ids = lax.broadcasted_iota(jnp.int32, (owners * groups_here, count), 0)
    member = jnp.where(ids == groups_ref[...], 1.0, 0.0)
    both = jnp.concatenate([acc[...], jnp.ones((count, parts.shape[2] - shells), jnp.float32)], axis=1)
    parts[...] = jnp.dot(member, both, precision=lax.Precision.HIGHEST, preferred_element_type=jnp.float32).reshape(
        parts.shape
    )

    clss = lax.axis_size("cls")
    me = dom * clss + cls

    def part_copy(k):
        peer = lax.rem(me + k, owners)
        return pltpu.make_async_remote_copy(
            src_ref=parts.at[peer],
            dst_ref=held.at[k],
            send_sem=part_send.at[k],
            recv_sem=part_recv.at[k],
            device_id=(peer // clss, lax.rem(peer, clss)),
            device_id_type=MESH,
        )

    def send(k, carry):
        part_copy(k).start()
        return carry

    lax.fori_loop(1, owners, send, 0)
    for _, p, exists, arrivals, sends, twin in events:

        def done(sends=sends, twin=twin):
            for ok, c in sends:
                when([ok], c.wait_send)
            if twin is not None:
                twin[0].wait_send()

        when(exists, done)

    def take(k, total):
        part_copy(k).wait_recv()
        return total + held[k]

    total = lax.fori_loop(1, owners, take, parts[me])

    def sent(k, carry):
        part_copy(k).wait_send()
        return carry

    lax.fori_loop(1, owners, sent, 0)
    counts = total[:, shells : shells + 1]
    out_ref[...] = total[:, :shells] / (2.0 * counts * weight_ref[...])


def pixel_tables(side):
    offsets = np.arange(side)
    signed = np.where(offsets < side // 2, offsets, offsets - side)
    radius = (signed[:, None] ** 2 + signed[None, :] ** 2).astype(np.float64)
    spatial = folded_radius(side).astype(np.float64) / (side * PIXEL_SIZE) ** 2
    slope = (0.5 * WAVELENGTH * spatial).astype(np.float32)
    offset = -0.25 * SPHERICAL * WAVELENGTH**3 * spatial**2 + math.asin(AMPLITUDE) / (2 * math.pi)
    offset = (offset - np.round(offset)).astype(np.float32)
    s = np.arange(side // 2)[:, None, None]
    weight = ((s * s <= radius) & (radius < (s + 1) ** 2)).sum(axis=(1, 2)).astype(np.float32)
    return slope, offset, weight.reshape(1, -1)


def fused(nz, images, own, classes, rotations, defocus, groups, classes_here, rot_count, owners):
    count, rows, side = images.shape
    shells = side // 2
    pieces = PIECES
    tiles = sum(len(held) for _, held in pieces)
    slots = owners * classes_here * rot_count
    slope, offset, weight = pixel_tables(side)
    vmem = pl.BlockSpec(memory_space=pltpu.VMEM)
    hbm = pl.BlockSpec(memory_space=pltpu.HBM)
    dma = pltpu.SemaphoreType.DMA
    widest = max(len(held) for _, held in pieces)
    return pl.pallas_call(
        functools.partial(fused_kernel, nz, side, classes_here, rot_count, (pieces, tiles)),
        out_shape=jax.ShapeDtypeStruct((GROUPS_DEV, shells), jnp.float32),
        in_specs=[hbm] * 9,
        out_specs=vmem,
        scratch_shapes=[pltpu.VMEM((slots, 16 * len(held), side), jnp.bfloat16) for _, held in pieces]
        + [pltpu.SMEM((count,), jnp.int32)] * 3
        + [
            pltpu.VMEM(slope.shape, jnp.float32),
            pltpu.VMEM(slope.shape, jnp.float32),
            pltpu.VMEM((1, count), jnp.int32),
            pltpu.VMEM(weight.shape, jnp.float32),
            pltpu.VMEM((count, 16 * tiles, side), jnp.bfloat16),
            pltpu.VMEM((count, 8 * TILE, side), jnp.bfloat16),
            pltpu.VMEM((classes_here * rot_count, 8 * TILE, side), jnp.bfloat16),
            pltpu.VMEM((count * 16 * tiles, side), jnp.float32),
            pltpu.VMEM((count * (16 * widest + 8), side), jnp.float32),
            pltpu.VMEM((8 * tiles, side, shells), jnp.bfloat16),
            pltpu.VMEM((count, shells), jnp.float32),
            pltpu.VMEM((owners, GROUPS_DEV, 128), jnp.float32),
            pltpu.VMEM((owners, GROUPS_DEV, 128), jnp.float32),
            dma((tiles + 1,)),
            dma((3,)),
            dma((7,)),
            dma((len(pieces), 3, 4 * nz)),
            dma((len(pieces), 3, nz)),
            dma((len(pieces), 2, nz)),
            dma((len(pieces), 2, nz)),
            dma((owners,)),
            dma((owners,)),
        ],
        compiler_params=pltpu.CompilerParams(
            collective_id=0, has_side_effects=True, vmem_limit_bytes=50 * 1024 * 1024
        ),
        name="fused_spectrum",
    )(
        *(
            pltpu.with_memory_space_constraint(operand, pltpu.HBM)
            for operand in (
                classes,
                rotations,
                defocus,
                jnp.asarray(slope),
                jnp.asarray(offset),
                groups.reshape(1, count),
                jnp.asarray(weight),
                own,
                images,
            )
        )
    )


def body(sizes, images, slices, classes, rotations, defocus, groups):
    doms, clss = sizes
    n = doms * clss
    count, _, pixels = images.shape
    side = math.isqrt(pixels)
    classes_here, rot_count = slices.shape[:2]

    def rows_of(array):
        lead = array.shape[:-2]
        split = array.reshape(lead + (2, side, side))
        return jnp.swapaxes(split, -3, -2).reshape(lead + (2 * side, side))

    own = rows_of(slices).reshape(classes_here * rot_count, 2 * side, side)
    if clss == 4 and doms % 2 == 0 and n <= 32 and side == 16 * TILE:
        return fused(
            doms // 2, rows_of(images), own, classes, rotations, defocus, groups, classes_here, rot_count, n
        )
    ny = clss // 2
    if clss % 2 == 0 and doms % ny == 0 and n <= 32:
        every = gather((ny, ny, doms // ny), own)
    else:
        every = lax.all_gather(own, AXES, axis=0)
    every = every.reshape(n * own.shape[0], 2 * side, side)
    parts = shell_power(rows_of(images), every, classes, rotations, rot_count, defocus, groups, GROUPS_DEV * n)
    offsets = np.arange(side)
    signed = np.where(offsets < side // 2, offsets, offsets - side)
    radius = signed[:, None] ** 2 + signed[None, :] ** 2
    s = np.arange(side // 2)[:, None, None]
    weight = ((s * s <= radius) & (radius < (s + 1) ** 2)).sum(axis=(1, 2)).astype(np.float32)
    return exchange(sizes, parts, jnp.asarray(weight).reshape(1, -1))


def solution(mesh):
    sizes = (mesh.shape["dom"], mesh.shape["cls"])
    return jax.shard_map(
        functools.partial(body, sizes),
        mesh=mesh,
        in_specs=(
            P(AXES, None, None),
            P(AXES, None, None, None),
            P(AXES),
            P(AXES),
            P(AXES),
            P(AXES),
        ),
        out_specs=P(AXES, None),
        check_vma=False,
    )
```

```python
import functools
import math

import jax
import jax.numpy as jnp
import numpy as np
from jax import lax
from jax.experimental import pallas as pl
from jax.experimental.pallas import tpu as pltpu
from jax.sharding import PartitionSpec as P

GROUPS_DEV = 8
PIXEL_SIZE = 1.5
WAVELENGTH = 0.0197
SPHERICAL = 27000000.0
AMPLITUDE = 0.1
ROUND = 12582912.0
MESH = pl.DeviceIdType.MESH
AXES = ("dom", "cls")
ROUTES = (("x", "y", "z"), ("z", "y", "x"), ("z", "x", "y"))
SHARE = (8, 12, 12)


def sine_coefficients(terms):
    nodes = 0.5 * np.cos((np.arange(400) + 0.5) * math.pi / 400)
    nodes = nodes[np.abs(nodes) > 1e-3]
    basis = np.stack([nodes ** (2 * k + 1) for k in range(terms)], 1)
    return np.linalg.lstsq(basis, np.sin(2 * math.pi * nodes), rcond=None)[0]


SINE = [float(v) for v in sine_coefficients(5)]


def gather_kernel(shape, own_ref, out_ref, local_sem, send_sem, recv_sem, pair_send, pair_recv):
    size = dict(x=shape[0], y=shape[1], z=shape[2])
    dom, cls = lax.axis_index("dom"), lax.axis_index("cls")
    here = dict(x=cls // 2, y=dom % size["y"], z=dom // size["y"])
    core = cls % 2
    rows = out_ref.shape[2]
    starts = [0]
    for share in SHARE:
        starts.append(starts[-1] + rows * share // 32)

    def device(at, which):
        return (at["z"] * size["y"] + at["y"], at["x"] * 2 + which)

    def slot(at, which):
        d = device(at, which)
        return d[0] * (size["x"] * 2) + d[1]

    def moved(at, dim, step):
        new = dict(at)
        new[dim] = at[dim] + step
        return new

    ways = []
    for dim in "xyz":
        if size[dim] == 1:
            continue
        if size[dim] == 2:
            other = dict(here)
            other[dim] = 1 - here[dim]
            ways.append((dim, 0, other, None))
        else:
            ways.append((dim, 1, moved(here, dim, 1), here[dim] < size[dim] - 1))
            ways.append((dim, -1, moved(here, dim, -1), here[dim] > 0))

    def when(conds, fn):
        conds = [c for c in conds if c is not None]
        if not conds:
            fn()
        else:
            pl.when(functools.reduce(jnp.logical_and, conds))(fn)

    barrier = pltpu.get_barrier_semaphore()
    partner = device(here, 1 - core)
    pl.semaphore_signal(barrier, inc=1, device_id=partner, device_id_type=MESH)
    for dim, sign, other, ok in ways:

        def greet(other=other):
            pl.semaphore_signal(barrier, inc=1, device_id=device(other, core), device_id_type=MESH)

        when([ok], greet)
    peers = 1
    for dim, sign, other, ok in ways:
        peers = peers + (1 if ok is None else ok.astype(jnp.int32))
    pl.semaphore_wait(barrier, peers)

    mine = slot(here, core)
    local = pltpu.make_async_copy(own_ref, out_ref.at[mine], local_sem)
    local.start()

    def part(ref, index):
        return ref.at[:, pl.ds(starts[index], starts[index + 1] - starts[index]), :]

    def copy(index, source, src_slot, to, way, own):
        src = part(own_ref, index) if own else part(out_ref.at[src_slot], index)
        return pltpu.make_async_remote_copy(
            src_ref=src,
            dst_ref=part(out_ref.at[src_slot], index),
            send_sem=send_sem.at[index, source, way],
            recv_sem=recv_sem.at[index, src_slot],
            device_id=to,
            device_id_type=MESH,
        )

    def pair_copy(index, source, src_slot, own):
        src = part(own_ref, index) if own else part(out_ref.at[src_slot], index)
        return pltpu.make_async_remote_copy(
            src_ref=src,
            dst_ref=part(out_ref.at[src_slot], index),
            send_sem=pair_send.at[index, source],
            recv_sem=pair_recv.at[index, src_slot],
            device_id=partner,
            device_id_type=MESH,
        )

    choices = {}
    for dim in "xyz":
        n = size[dim]
        if n == 1:
            choices[dim] = [(0, here[dim], None, 0)]
        elif n == 2:
            choices[dim] = [(0, here[dim], None, 0), (0, 1 - here[dim], None, 1)]
        else:
            listed = [(0, here[dim], None, 0)]
            for t in range(1, n):
                listed.append((1, here[dim] - t, here[dim] >= t, t))
                listed.append((-1, here[dim] + t, here[dim] + t < n, t))
            choices[dim] = listed
    events = []
    for ix, cx in enumerate(choices["x"]):
        for iy, cy in enumerate(choices["y"]):
            for iz, cz in enumerate(choices["z"]):
                pick = dict(x=cx, y=cy, z=cz)
                depth = cx[3] + cy[3] + cz[3]
                number = (ix * len(choices["y"]) + iy) * len(choices["z"]) + iz
                for index in range(3):
                    events.append((depth, index, number, pick))
    events.sort(key=lambda e: e[:3])
    finish = []
    for depth, index, number, pick in events:
        at = {dim: pick[dim][1] for dim in "xyz"}
        exists = [pick[dim][2] for dim in "xyz"]
        src_slot = slot(at, core)
        order = ROUTES[index]
        last = max([k for k, dim in enumerate(order) if pick[dim][3] > 0], default=-1)
        sends = []
        for number_way, (dim, sign, other, ok) in enumerate(ways):
            k = order.index(dim)
            if k < last:
                continue
            if k == last and (size[dim] == 2 or sign != pick[dim][0]):
                continue
            sends.append((number_way, device(other, core), ok))

        def arrive(index=index, number=number, src_slot=src_slot, depth=depth, sends=sends):
            own = depth == 0
            if not own:
                copy(index, number, src_slot, partner, 0, False).wait_recv()
            for way, to, ok in sends:
                when([ok], copy(index, number, src_slot, to, way, own).start)
            pair_copy(index, number, src_slot, own).start()

        def done(index=index, number=number, src_slot=src_slot, depth=depth, sends=sends, at=at):
            own = depth == 0
            for way, to, ok in sends:
                when([ok], copy(index, number, src_slot, to, way, own).wait_send)
            pair_copy(index, number, src_slot, own).wait_send()
            pair_copy(index, number, slot(at, 1 - core), False).wait_recv()

        when(exists, arrive)
        finish.append((exists, done))
    for exists, done in finish:
        when(exists, done)
    local.wait()


def gather(shape, own):
    devices = 2 * shape[0] * shape[1] * shape[2]
    total = 1
    for n in shape:
        total *= n if n <= 2 else 2 * n - 1
    return pl.pallas_call(
        functools.partial(gather_kernel, shape),
        out_shape=jax.ShapeDtypeStruct((devices,) + own.shape, own.dtype),
        in_specs=[pl.BlockSpec(memory_space=pltpu.VMEM)],
        out_specs=pl.BlockSpec(memory_space=pltpu.VMEM),
        scratch_shapes=[
            pltpu.SemaphoreType.DMA,
            pltpu.SemaphoreType.DMA((3, total, 4)),
            pltpu.SemaphoreType.DMA((3, devices)),
            pltpu.SemaphoreType.DMA((3, total)),
            pltpu.SemaphoreType.DMA((3, devices)),
        ],
        compiler_params=pltpu.CompilerParams(
            collective_id=0, has_side_effects=True, vmem_limit_bytes=12 * 1024 * 1024
        ),
        name="gather_slices",
    )(own)


def power_kernel(
    side, rot_count, classes_ref, rotations_ref, defocus_ref, images_ref, slices_ref, slope_ref, offset_ref, groups_ref, out_ref, power, acc
):
    step = pl.program_id(0)
    count, chunk, lanes = images_ref.shape
    shells = side // 2
    pitch = power.shape[0] // count

    @pl.when(step == 0)
    def _():
        acc[...] = jnp.zeros_like(acc)

    slope = slope_ref[...]
    offset = offset_ref[...]

    def one(i, carry):
        turns = defocus_ref[i].astype(jnp.float32) * slope + offset
        x = turns - ((turns + ROUND) - ROUND)
        y = x * x
        s = jnp.full_like(y, SINE[-1])
        for value in SINE[-2::-1]:
            s = s * y + value
        s = s * x
        d = images_ref[i].astype(jnp.float32) + s * slices_ref[classes_ref[i] * rot_count + rotations_ref[i]].astype(jnp.float32)
        power[pl.ds(pl.multiple_of(i * pitch, 8), chunk), :] = d * d
        return carry

    lax.fori_loop(0, count, one, 0, unroll=8)

    b = lax.broadcasted_iota(jnp.int32, (lanes, shells), 0)
    s = lax.broadcasted_iota(jnp.int32, (lanes, shells), 1)
    fb = jnp.where(b < side // 2, b, b - side)
    total = acc[...]
    for k in range(chunk // 2):
        a = step * (chunk // 2) + k
        fa = jnp.where(a < side // 2, a, a - side)
        r = fa * fa + fb * fb
        table = jnp.where((s * s <= r) & (r < (s + 1) * (s + 1)), 1.0, 0.0).astype(jnp.bfloat16)
        p = power[pl.ds(2 * k, count, stride=pitch), :] + power[pl.ds(2 * k + 1, count, stride=pitch), :]
        high = p.astype(jnp.bfloat16)
        low = (p - high.astype(jnp.float32)).astype(jnp.bfloat16)
        total = total + jnp.dot(
            jnp.concatenate([high, low], axis=1),
            jnp.concatenate([table, table], axis=0),
            preferred_element_type=jnp.float32,
        )
    acc[...] = total

    @pl.when(step == pl.num_programs(0) - 1)
    def _():
        groups = out_ref.shape[0]
        ids = lax.broadcasted_iota(jnp.int32, (groups, count), 0)
        member = jnp.where(ids == groups_ref[...], 1.0, 0.0)
        both = jnp.concatenate([acc[...], jnp.ones((count, out_ref.shape[1] - shells), jnp.float32)], axis=1)
        out_ref[...] = jnp.dot(
            member, both, precision=lax.Precision.HIGHEST, preferred_element_type=jnp.float32
        )


def shell_power(images, slices, classes, rotations, rot_count, defocus, groups, group_total):
    count, rows, side = images.shape
    chunk = 32
    offsets = np.arange(side)
    signed = np.where(offsets < side // 2, offsets, offsets - side)
    radius = (signed[:, None] ** 2 + signed[None, :] ** 2).astype(np.float64)
    spatial = np.repeat(radius / (side * PIXEL_SIZE) ** 2, 2, axis=0)
    slope = (0.5 * WAVELENGTH * spatial).astype(np.float32)
    offset = -0.25 * SPHERICAL * WAVELENGTH**3 * spatial**2 + math.asin(AMPLITUDE) / (2 * math.pi)
    offset = (offset - np.round(offset)).astype(np.float32)
    smem = pl.BlockSpec(memory_space=pltpu.SMEM)
    return pl.pallas_call(
        functools.partial(power_kernel, side, rot_count),
        grid=(rows // chunk,),
        out_shape=jax.ShapeDtypeStruct((group_total, 128), jnp.float32),
        in_specs=[
            smem,
            smem,
            smem,
            pl.BlockSpec((count, chunk, side), lambda i: (0, i, 0)),
            pl.BlockSpec((slices.shape[0], chunk, side), lambda i: (0, i, 0)),
            pl.BlockSpec((chunk, side), lambda i: (i, 0)),
            pl.BlockSpec((chunk, side), lambda i: (i, 0)),
            pl.BlockSpec((1, count), lambda i: (0, 0)),
        ],
        out_specs=pl.BlockSpec((group_total, 128), lambda i: (0, 0)),
        scratch_shapes=[
            pltpu.VMEM((count * (chunk + 8), side), jnp.float32),
            pltpu.VMEM((count, side // 2), jnp.float32),
        ],
        compiler_params=pltpu.CompilerParams(vmem_limit_bytes=20 * 1024 * 1024),
        name="shell_power",
    )(classes, rotations, defocus, images, slices, jnp.asarray(slope), jnp.asarray(offset), groups.reshape(1, count))


def exchange_kernel(sizes, shells, parts_ref, weight_ref, out_ref, held, send_sem, recv_sem):
    doms, clss = sizes
    n = doms * clss
    me = lax.axis_index("dom") * clss + lax.axis_index("cls")
    barrier = pltpu.get_barrier_semaphore()

    def device(k):
        peer = lax.rem(me + k, n)
        return peer, (peer // clss, lax.rem(peer, clss))

    def greet(k, carry):
        pl.semaphore_signal(barrier, inc=1, device_id=device(k)[1], device_id_type=MESH)
        return carry

    lax.fori_loop(1, n, greet, 0)
    pl.semaphore_wait(barrier, n - 1)

    def copy(k):
        peer, to = device(k)
        return pltpu.make_async_remote_copy(
            src_ref=parts_ref.at[peer],
            dst_ref=held.at[k],
            send_sem=send_sem.at[k],
            recv_sem=recv_sem.at[k],
            device_id=to,
            device_id_type=MESH,
        )

    def send(k, carry):
        copy(k).start()
        return carry

    lax.fori_loop(1, n, send, 0)

    def take(k, total):
        copy(k).wait_recv()
        return total + held[k]

    total = lax.fori_loop(1, n, take, parts_ref[me])

    def sent(k, carry):
        copy(k).wait_send()
        return carry

    lax.fori_loop(1, n, sent, 0)
    counts = total[:, shells : shells + 1]
    out_ref[...] = total[:, :shells] / (2.0 * counts * weight_ref[...])


def exchange(sizes, parts, weight):
    n = sizes[0] * sizes[1]
    shells = weight.shape[1]
    vmem = pl.BlockSpec(memory_space=pltpu.VMEM)
    return pl.pallas_call(
        functools.partial(exchange_kernel, sizes, shells),
        out_shape=jax.ShapeDtypeStruct((GROUPS_DEV, shells), jnp.float32),
        in_specs=[vmem, vmem],
        out_specs=vmem,
        scratch_shapes=[
            pltpu.VMEM((n, GROUPS_DEV, parts.shape[-1]), jnp.float32),
            pltpu.SemaphoreType.DMA((n,)),
            pltpu.SemaphoreType.DMA((n,)),
        ],
        compiler_params=pltpu.CompilerParams(
            collective_id=1, has_side_effects=True, vmem_limit_bytes=4 * 1024 * 1024
        ),
        name="exchange_groups",
    )(parts.reshape(n, GROUPS_DEV, parts.shape[-1]), weight)


PIECES = ((0, (0, 6, 13)), (1, (1, 2, 3, 10, 11, 12)), (2, (4, 5, 7, 8, 9)))
SCHEDULE = (
    (0, "o", 0), (1, "o", 0), (2, "o", 0), ("fill", 7), (0, "x", 0), (1, "a", 0), (1, "z", 1), ("fill", 2),
    (2, "a", 0), (2, "z", 1), ("fill", 4), (0, "y", 0), (1, "z", 2), ("fill", 2), (1, "a", 1), (2, "z", 2),
    (2, "b", 0), ("fill", 4), (1, "z", 3), (2, "a", 1), (1, "a", 2), ("fill", 3), (2, "z", 3), (0, "z", 1),
    ("fill", 3), (2, "a", 2), (1, "b", 0), (1, "a", 3), ("fill", 1), (2, "b", 1), (2, "a", 3), (1, "b", 1),
    ("fill", 1), (0, "z", 2), (2, "b", 2), (1, "b", 2), ("fill", 1), (2, "b", 3), (1, "b", 3), ("calc", 2),
    (0, "z", 3), ("calc", 1), ("calc", 0),
)
UNIT = 8
TILE = 8


def folded_rows(side):
    half = side // 2
    low, high = half - TILE, half + TILE
    kept = np.concatenate([np.arange(low), np.arange(high, side)])
    other = kept.copy()
    other[low - TILE : low] = half - 1 - np.arange(TILE)
    other[low : low + TILE] = high - np.arange(TILE)
    return kept, other


def folded_radius(side):
    half = side // 2
    offsets = np.arange(side)
    signed = np.where(offsets < half, offsets, offsets - side)
    radius = signed[:, None] ** 2 + signed[None, :] ** 2
    kept, other = folded_rows(side)
    own, far = radius[kept], np.roll(radius[other], half, axis=1)
    inside = own < half * half
    fold = (other != kept)[:, None] & ~inside
    assert not np.any((other != kept)[:, None] & inside & (far < half * half))
    packed = np.where(fold, far, own)
    assert np.sum(packed < half * half) == np.sum(radius < half * half)
    return packed


def runs_of(tiles):
    runs = []
    for k, t in enumerate(tiles):
        if runs and runs[-1][1] + runs[-1][2] == t:
            runs[-1][2] += 1
        else:
            runs.append([k, t, 1])
    return runs


def row_groups(tiles, side):
    place = {TILE * t + r: TILE * k + r for k, t in enumerate(tiles) for r in range(TILE)}
    kept, other = folded_rows(side)
    plain = {int(a): j for j, a in enumerate(kept) if other[j] == a and (a == 0 or other[j - 1] == kept[j - 1])}
    groups, used = [], set()
    for j in sorted(place):
        if j in used:
            continue
        a = int(kept[j])
        mate = plain.get(side - a) if plain.get(a) == j else None
        if mate is not None and mate != j and mate in place:
            used.add(mate)
            groups.append((j, (place[j], place[mate])))
        else:
            groups.append((j, (place[j],)))
    return groups


def fold(keep, far, shifted, first_row, side):
    lines = 2 * TILE
    order = [(-i if shifted else TILE - 1 - i) % TILE for i in range(TILE)]
    far = far.astype(jnp.float32)
    far = jnp.concatenate([far[2 * k : 2 * k + 2] for k in order], axis=0)
    far = pltpu.roll(far, side // 2, axis=1)
    a = first_row + lax.broadcasted_iota(jnp.int32, (lines, side), 0) // 2
    b = lax.broadcasted_iota(jnp.int32, (lines, side), 1)
    fa = jnp.where(a < side // 2, a, a - side)
    fb = jnp.where(b < side // 2, b, b - side)
    inside = fa * fa + fb * fb < (side // 2) * (side // 2)
    return jnp.where(inside, keep.astype(jnp.float32), far).astype(keep.dtype)


def fused_kernel(
    nz,
    side,
    classes_here,
    rot_count,
    layout,
    classes_hbm,
    rotations_hbm,
    defocus_hbm,
    slope_hbm,
    offset_hbm,
    groups_hbm,
    weight_hbm,
    own_hbm,
    images_hbm,
    out_ref,
    *scratch,
):
    pieces, tiles = layout
    count = images_hbm.shape[0]
    shells = side // 2
    rows = 16 * tiles
    half = rows // 2
    bufs = scratch[: len(pieces)]
    (
        classes_ref,
        rotations_ref,
        defocus_ref,
        slope_ref,
        offset_ref,
        groups_ref,
        weight_ref,
        images,
        image_rim,
        own_rim,
        sine,
        power,
        table,
        acc,
        parts,
        held,
        local_sem,
        image_sem,
        small_sem,
        send_sem,
        recv_sem,
        pair_send,
        pair_recv,
        part_send,
        part_recv,
    ) = scratch[len(pieces) :]
    dom, cls = lax.axis_index("dom"), lax.axis_index("cls")
    x, core, y, z = cls // 2, cls % 2, dom % 2, dom // 2
    slot = classes_here * rot_count

    def device(x_, y_, z_, core_):
        return (z_ * 2 + y_, x_ * 2 + core_)

    partner = device(x, y, z, 1 - core)
    up, down = device(x, y, z + 1, core), device(x, y, z - 1, core)
    across = {"x": device(1 - x, y, z, core), "y": device(x, 1 - y, z, core)}

    def when(conds, fn):
        conds = [c for c in conds if c is not None]
        if not conds:
            fn()
        else:
            pl.when(functools.reduce(jnp.logical_and, conds))(fn)

    barrier = pltpu.get_barrier_semaphore()
    for to in (partner, across["x"], across["y"]):
        pl.semaphore_signal(barrier, inc=1, device_id=to, device_id_type=MESH)
    has_up, has_down = z < nz - 1, z > 0
    when([has_up], lambda: pl.semaphore_signal(barrier, inc=1, device_id=up, device_id_type=MESH))
    when([has_down], lambda: pl.semaphore_signal(barrier, inc=1, device_id=down, device_id_type=MESH))

    line = 2 * TILE
    rim = tiles // 2 - 1
    own_copies = [
        pltpu.make_async_copy(own_hbm.at[:, pl.ds(line * rim, 4 * line), :], own_rim, local_sem.at[0])
    ]
    rim_stores = []
    for p, (route, held_tiles) in enumerate(pieces):
        q1, q2 = (x, y) if route == 1 else (y, x)
        at = (((core * nz + z) * 2 + q1) * 2 + q2) * slot
        for k, t in enumerate(held_tiles):
            if rim <= t < rim + 2:
                rim_stores.append((p, at, line * k, t - rim))
        for k, t, n in runs_of([t if not rim <= t < rim + 2 else -line * t for t in held_tiles]):
            if t >= 0:
                own_copies.append(
                    pltpu.make_async_copy(
                        own_hbm.at[:, pl.ds(line * (t + 2 * (t > rim)), line * n), :],
                        bufs[p].at[pl.ds(at, slot), pl.ds(line * k, line * n), :],
                        local_sem.at[len(own_copies)],
                    )
                )
    for c in own_copies:
        c.start()
    edge = line * rim
    image_copies = [
        pltpu.make_async_copy(images_hbm.at[:, pl.ds(edge, 4 * line), :], image_rim, image_sem.at[0]),
        pltpu.make_async_copy(images_hbm.at[:, pl.ds(0, edge), :], images.at[:, pl.ds(0, edge), :], image_sem.at[1]),
        pltpu.make_async_copy(
            images_hbm.at[:, pl.ds(edge + 4 * line, edge), :],
            images.at[:, pl.ds(edge + 2 * line, edge), :],
            image_sem.at[2],
        ),
    ]
    small = (
        (slope_hbm, slope_ref),
        (offset_hbm, offset_ref),
        (defocus_hbm, defocus_ref),
        (classes_hbm, classes_ref),
        (rotations_hbm, rotations_ref),
        (groups_hbm, groups_ref),
        (weight_hbm, weight_ref),
    )
    small_copies = [pltpu.make_async_copy(src, dst, small_sem.at[k]) for k, (src, dst) in enumerate(small)]
    for c in small_copies:
        c.start()

    def folded(ref, i, k):
        keep = ref[i, pl.ds(3 * line * k, line), :]
        far = ref[i, pl.ds(line * (1 + k), line), :]
        return fold(keep, far, k == 1, TILE * (rim + 3 * k), side)

    for c in own_copies:
        c.wait()
    for c in image_copies:
        c.start()
    for p, at, row, k in rim_stores:
        for j in range(slot):
            bufs[p][at + j, pl.ds(row, line), :] = folded(own_rim, j, k)
    pl.semaphore_wait(barrier, 3 + has_up.astype(jnp.int32) + has_down.astype(jnp.int32))

    events = []
    for p, (route, n) in enumerate(pieces):
        q1, q2 = (x, y) if route == 1 else (y, x)
        to_q1, to_q2 = (across["x"], across["y"]) if route == 1 else (across["y"], across["x"])
        buf = bufs[p]

        def region(core_, z_, a=None, b=None, buf=buf):
            first = (core_ * nz + z_) * 4 * slot
            size = 4 * slot
            if a is not None:
                first, size = first + a * 2 * slot, 2 * slot
            if b is not None:
                first, size = first + b * slot, slot
            return buf.at[pl.ds(first, size)]

        def link(stage, zs, number, where, to, p=p):
            return pltpu.make_async_remote_copy(
                src_ref=where,
                dst_ref=where,
                send_sem=send_sem.at[p],
                recv_sem=recv_sem.at[p, stage, zs],
                device_id=to,
                device_id_type=MESH,
            )

        def pair(stage, zs, where, p=p):
            return pltpu.make_async_remote_copy(
                src_ref=where,
                dst_ref=where,
                send_sem=pair_send.at[p],
                recv_sem=pair_recv.at[p],
                device_id=partner,
                device_id_type=MESH,
            )

        reach = [(z, None, 0, None)]
        for t in range(1, nz):
            reach.append((z - t, z >= t, t, -1))
            reach.append((z + t, z + t < nz, t, 1))

        if route == 0:
            one = region(core, z, q1, q2)
            other = region(core, z, q1, 1 - q2)
            mine = region(core, z, q1)
            events.append(((p, "o", 0), p, [], [], [(None, link(0, z, 0, one, to_q2))], None))
            events.append(((p, "x", 0), p, [], [link(0, z, 0, other, to_q2)], [(None, link(1, z, 0, mine, to_q1))], None))
            for k, (zs, ok, t, way) in enumerate(reach):
                block = region(core, zs)
                sends = []
                if way in (None, -1):
                    sends.append((has_up, link(2, zs, 2 * k, block, up)))
                if way in (None, 1):
                    sends.append((has_down, link(2, zs, 2 * k + 1, block, down)))
                arrival = link(1, z, 0, region(core, z, 1 - q1), to_q1) if way is None else link(2, zs, 0, block, up)
                twin = region(1 - core, zs)
                name = (p, "z" if t else "y", t)
                events.append((name, p, [ok], [arrival], sends, (pair(0, zs, block), pair(0, zs, twin))))
        else:
            for k, (zs, ok, t, way) in enumerate(reach):
                one = region(core, zs, q1, q2)
                sends = []
                if way in (None, -1):
                    sends.append((has_up, link(0, zs, 2 * k, one, up)))
                if way in (None, 1):
                    sends.append((has_down, link(0, zs, 2 * k + 1, one, down)))
                sends.append((None, link(1, zs, k, one, to_q2)))
                arrival = [] if way is None else [link(0, zs, 0, one, up)]
                events.append(((p, "z" if t else "o", t), p, [ok], arrival, sends, None))
                near, far = region(core, zs, q1), region(core, zs, 1 - q1)
                events.append(
                    (
                        (p, "a", t),
                        p,
                        [ok],
                        [link(1, zs, 0, region(core, zs, q1, 1 - q2), to_q2)],
                        [(None, link(2, zs, k, near, to_q1))],
                        (pair(0, zs, near), pair(0, zs, region(1 - core, zs, q1))),
                    )
                )
                events.append(
                    (
                        (p, "b", t),
                        p,
                        [ok],
                        [link(2, zs, 0, far, to_q1)],
                        [],
                        (pair(1, zs, far), pair(1, zs, region(1 - core, zs, 1 - q1))),
                    )
                )

    def make_sine(i, carry):
        turns = defocus_ref[i].astype(jnp.float32) * slope_ref[...] + offset_ref[...]
        v = turns - ((turns + ROUND) - ROUND)
        w = v * v
        s = jnp.full_like(w, SINE[-1])
        for value in SINE[-2::-1]:
            s = s * w + value
        s = s * v
        base = pl.multiple_of(i * rows, 8)
        sine[pl.ds(base, half, stride=2), :] = s
        sine[pl.ds(base + 1, half, stride=2), :] = s
        return carry

    def sine_unit(j):
        def run():
            if j == 0:
                for c in small_copies[:3]:
                    c.wait()
            lax.fori_loop(j * UNIT, (j + 1) * UNIT, make_sine, 0, unroll=2)

        return run

    def make_table(a, carry):
        b = lax.broadcasted_iota(jnp.int32, (side, shells), 0)
        s = lax.broadcasted_iota(jnp.int32, (side, shells), 1)
        low = TILE * (rim + 1)
        row = jnp.where(a < low, a, a + 2 * TILE)
        far = jnp.where(a < low, side // 2 - 1 + TILE * rim - a, side // 2 + TILE + low - a)
        fb = jnp.where(b < side // 2, b, b - side)
        gb = b - side // 2
        fa = jnp.where(row < side // 2, row, row - side)
        ga = jnp.where(far < side // 2, far, far - side)
        r = fa * fa + fb * fb
        folds = (a >= TILE * rim) & (a < TILE * (rim + 2)) & (a != low)
        r = jnp.where(folds & (r >= (side // 2) * (side // 2)), ga * ga + gb * gb, r)
        inside = (s * s <= r) & (r < (s + 1) * (s + 1))
        table[a] = jnp.where(inside, 1.0, 0.0).astype(jnp.bfloat16)
        return carry

    def table_unit(j, n):
        return lambda: lax.fori_loop(j * n, (j + 1) * n, make_table, 0)

    def fold_image(i, carry):
        for k in range(2):
            images[i, pl.ds(line * (rim + k), line), :] = folded(image_rim, i, k)
        return carry

    def fold_unit(j):
        def run():
            if j == 0:
                image_copies[0].wait()
            lax.fori_loop(j * 4 * UNIT, (j + 1) * 4 * UNIT, fold_image, 0, unroll=4)

        return run

    fillers = [table_unit(j, half // 8) for j in range(8)] + [sine_unit(j) for j in range(count // UNIT)]
    fillers += [fold_unit(j) for j in range(count // (4 * UNIT))]
    fillers.reverse()
    calculated = []
    acc[...] = jnp.zeros_like(acc)

    def twins(p):
        where = bufs[p].at[pl.ds((1 - core) * (4 * nz * slot), 4 * nz * slot)]
        return pltpu.make_async_remote_copy(
            src_ref=where,
            dst_ref=where,
            send_sem=pair_send.at[p],
            recv_sem=pair_recv.at[p],
            device_id=partner,
            device_id_type=MESH,
        )

    def calc(p):
        route, held_tiles = pieces[p]
        if not calculated:
            for c in image_copies[1:] + small_copies[3:]:
                c.wait()
        calculated.append(p)
        twins(p).wait_recv()
        pitch = line * len(held_tiles) + TILE

        def one(i, carry, p=p, route=route, held_tiles=held_tiles, pitch=pitch):
            c = classes_ref[i]
            owner, sub = (c, 0) if classes_here == 1 else (c // classes_here, c % classes_here)
            place = owner >> 1
            if route == 1:
                place = (place & ~3) | ((place & 1) << 1) | ((place >> 1) & 1)
            at = ((owner & 1) * (nz * 4) + place) * slot + sub * rot_count + rotations_ref[i]
            for k, t, n in runs_of(held_tiles):
                f = bufs[p][at, pl.ds(line * k, line * n), :].astype(jnp.float32)
                s = sine[pl.ds(pl.multiple_of(i * rows + line * t, 8), line * n), :]
                d = images[i, pl.ds(line * t, line * n), :].astype(jnp.float32) + s * f
                power[pl.ds(pl.multiple_of(i * pitch + line * k, 8), line * n), :] = d * d
            return carry

        lax.fori_loop(0, count, one, 0, unroll=8)
        total = acc[...]
        for j, places in row_groups(held_tiles, side):
            v = None
            for k in places:
                for part in range(2):
                    w = power[pl.ds(2 * k + part, count, stride=pitch), :]
                    v = w if v is None else v + w
            high = v.astype(jnp.bfloat16)
            low = (v - high.astype(jnp.float32)).astype(jnp.bfloat16)
            t = table[j]
            total = total + jnp.dot(
                jnp.concatenate([high, low], axis=1),
                jnp.concatenate([t, t], axis=0),
                preferred_element_type=jnp.float32,
            )
        acc[...] = total

    def amount(p, slots):
        where = bufs[p].at[pl.ds(0, slots * slot)]
        return pltpu.make_async_remote_copy(
            src_ref=where,
            dst_ref=where,
            send_sem=send_sem.at[p],
            recv_sem=pair_recv.at[p],
            device_id=partner,
            device_id_type=MESH,
        )

    def handle(event):
        _, _, exists, arrivals, sends, twin = event

        def arrive():
            for c in arrivals:
                c.wait_recv()
            for ok, c in sends:
                when([ok], c.start)
            if twin is not None:
                twin[0].start()

        when(exists, arrive)

    for step in SCHEDULE:
        if step[0] == "fill":
            for _ in range(step[1]):
                fillers.pop()()
        elif step[0] == "calc":
            calc(step[1])
        else:
            for event in events:
                if event[0] == step:
                    handle(event)
    assert not fillers and len(calculated) == len(pieces)

    owners, groups_here = parts.shape[:2]
    ids = lax.broadcasted_iota(jnp.int32, (owners * groups_here, count), 0)
    member = jnp.where(ids == groups_ref[...], 1.0, 0.0)
    both = jnp.concatenate([acc[...], jnp.ones((count, parts.shape[2] - shells), jnp.float32)], axis=1)
    parts[...] = jnp.dot(member, both, precision=lax.Precision.HIGHEST, preferred_element_type=jnp.float32).reshape(
        parts.shape
    )

    me = dom * 4 + cls
    everyone = pl.ds(1, owners - 1)

    def part_copy(k):
        peer = me + k
        peer = jnp.where(peer >= owners, peer - owners, peer)
        return pltpu.make_async_remote_copy(
            src_ref=parts.at[peer],
            dst_ref=held.at[k],
            send_sem=part_send,
            recv_sem=part_recv,
            device_id=(peer >> 2, peer & 3),
            device_id_type=MESH,
        )

    for k in range(1, owners):
        part_copy(k).start()
    for p, (route, held_tiles) in enumerate(pieces):
        twins(p).wait_send()
        inner = (3 + 4 * (nz + 1)) if route == 0 else 3 * nz + nz + 1
        outer = (3 + 4) if route == 0 else 3 * nz + 1
        inside = has_up & has_down
        when([inside], amount(p, inner).wait_send)
        when([jnp.logical_not(inside)], amount(p, outer).wait_send)

    all_parts = pltpu.make_async_remote_copy(
        src_ref=held.at[everyone],
        dst_ref=held.at[everyone],
        send_sem=part_send,
        recv_sem=part_recv,
        device_id=partner,
        device_id_type=MESH,
    )
    all_parts.wait_recv()
    total = parts[me] + jnp.sum(held[everyone], axis=0)
    all_parts.wait_send()
    counts = total[:, shells : shells + 1]
    out_ref[...] = total[:, :shells] / (2.0 * counts * weight_ref[...])


def pixel_tables(side):
    offsets = np.arange(side)
    signed = np.where(offsets < side // 2, offsets, offsets - side)
    radius = (signed[:, None] ** 2 + signed[None, :] ** 2).astype(np.float64)
    spatial = folded_radius(side).astype(np.float64) / (side * PIXEL_SIZE) ** 2
    slope = (0.5 * WAVELENGTH * spatial).astype(np.float32)
    offset = -0.25 * SPHERICAL * WAVELENGTH**3 * spatial**2 + math.asin(AMPLITUDE) / (2 * math.pi)
    offset = (offset - np.round(offset)).astype(np.float32)
    s = np.arange(side // 2)[:, None, None]
    weight = ((s * s <= radius) & (radius < (s + 1) ** 2)).sum(axis=(1, 2)).astype(np.float32)
    return slope, offset, weight.reshape(1, -1)


def fused(nz, images, own, classes, rotations, defocus, groups, classes_here, rot_count, owners):
    count, rows, side = images.shape
    shells = side // 2
    pieces = PIECES
    tiles = sum(len(held) for _, held in pieces)
    slots = owners * classes_here * rot_count
    slope, offset, weight = pixel_tables(side)
    vmem = pl.BlockSpec(memory_space=pltpu.VMEM)
    hbm = pl.BlockSpec(memory_space=pltpu.HBM)
    dma = pltpu.SemaphoreType.DMA
    widest = max(len(held) for _, held in pieces)
    return pl.pallas_call(
        functools.partial(fused_kernel, nz, side, classes_here, rot_count, (pieces, tiles)),
        out_shape=jax.ShapeDtypeStruct((GROUPS_DEV, shells), jnp.float32),
        in_specs=[hbm] * 9,
        out_specs=vmem,
        scratch_shapes=[pltpu.VMEM((slots, 16 * len(held), side), jnp.bfloat16) for _, held in pieces]
        + [pltpu.SMEM((count,), jnp.int32)] * 3
        + [
            pltpu.VMEM(slope.shape, jnp.float32),
            pltpu.VMEM(slope.shape, jnp.float32),
            pltpu.VMEM((1, count), jnp.int32),
            pltpu.VMEM(weight.shape, jnp.float32),
            pltpu.VMEM((count, 16 * tiles, side), jnp.bfloat16),
            pltpu.VMEM((count, 8 * TILE, side), jnp.bfloat16),
            pltpu.VMEM((classes_here * rot_count, 8 * TILE, side), jnp.bfloat16),
            pltpu.VMEM((count * 16 * tiles, side), jnp.float32),
            pltpu.VMEM((count * (16 * widest + 8), side), jnp.float32),
            pltpu.VMEM((8 * tiles, side, shells), jnp.bfloat16),
            pltpu.VMEM((count, shells), jnp.float32),
            pltpu.VMEM((owners, GROUPS_DEV, 128), jnp.float32),
            pltpu.VMEM((owners, GROUPS_DEV, 128), jnp.float32),
            dma((sum(len(runs_of(held)) for _, held in pieces) + 3,)),
            dma((3,)),
            dma((7,)),
            dma((len(pieces),)),
            dma((len(pieces), 3, nz)),
            dma((len(pieces),)),
            dma((len(pieces),)),
            dma,
            dma,
        ],
        compiler_params=pltpu.CompilerParams(
            collective_id=0, has_side_effects=True, vmem_limit_bytes=50 * 1024 * 1024
        ),
        name="fused_spectrum",
    )(
        *(
            pltpu.with_memory_space_constraint(operand, pltpu.HBM)
            for operand in (
                classes,
                rotations,
                defocus,
                jnp.asarray(slope),
                jnp.asarray(offset),
                groups.reshape(1, count),
                jnp.asarray(weight),
                own,
                images,
            )
        )
    )


def body(sizes, images, slices, classes, rotations, defocus, groups):
    doms, clss = sizes
    n = doms * clss
    count, _, pixels = images.shape
    side = math.isqrt(pixels)
    classes_here, rot_count = slices.shape[:2]

    def rows_of(array):
        lead = array.shape[:-2]
        split = array.reshape(lead + (2, side, side))
        return jnp.swapaxes(split, -3, -2).reshape(lead + (2 * side, side))

    own = rows_of(slices).reshape(classes_here * rot_count, 2 * side, side)
    if clss == 4 and doms == 8 and side == 16 * TILE:
        return fused(
            doms // 2, rows_of(images), own, classes, rotations, defocus, groups, classes_here, rot_count, n
        )
    ny = clss // 2
    if clss % 2 == 0 and doms % ny == 0 and n <= 32:
        every = gather((ny, ny, doms // ny), own)
    else:
        every = lax.all_gather(own, AXES, axis=0)
    every = every.reshape(n * own.shape[0], 2 * side, side)
    parts = shell_power(rows_of(images), every, classes, rotations, rot_count, defocus, groups, GROUPS_DEV * n)
    offsets = np.arange(side)
    signed = np.where(offsets < side // 2, offsets, offsets - side)
    radius = signed[:, None] ** 2 + signed[None, :] ** 2
    s = np.arange(side // 2)[:, None, None]
    weight = ((s * s <= radius) & (radius < (s + 1) ** 2)).sum(axis=(1, 2)).astype(np.float32)
    return exchange(sizes, parts, jnp.asarray(weight).reshape(1, -1))


def solution(mesh):
    sizes = (mesh.shape["dom"], mesh.shape["cls"])
    return jax.shard_map(
        functools.partial(body, sizes),
        mesh=mesh,
        in_specs=(
            P(AXES, None, None),
            P(AXES, None, None, None),
            P(AXES),
            P(AXES),
            P(AXES),
            P(AXES),
        ),
        out_specs=P(AXES, None),
        check_vma=False,
    )
```

```python
import functools
import math

import jax
import jax.numpy as jnp
import numpy as np
from jax import lax
from jax.experimental import pallas as pl
from jax.experimental.pallas import tpu as pltpu
from jax.sharding import PartitionSpec as P

GROUPS_DEV = 8
PIXEL_SIZE = 1.5
WAVELENGTH = 0.0197
SPHERICAL = 27000000.0
AMPLITUDE = 0.1
ROUND = 12582912.0
MESH = pl.DeviceIdType.MESH
AXES = ("dom", "cls")
ROUTES = (("x", "y", "z"), ("z", "y", "x"), ("z", "x", "y"))
SHARE = (8, 12, 12)


def sine_coefficients(terms):
    nodes = 0.5 * np.cos((np.arange(400) + 0.5) * math.pi / 400)
    nodes = nodes[np.abs(nodes) > 1e-3]
    basis = np.stack([nodes ** (2 * k + 1) for k in range(terms)], 1)
    return np.linalg.lstsq(basis, np.sin(2 * math.pi * nodes), rcond=None)[0]


SINE = [float(v) for v in sine_coefficients(5)]


def gather_kernel(shape, own_ref, out_ref, local_sem, send_sem, recv_sem, pair_send, pair_recv):
    size = dict(x=shape[0], y=shape[1], z=shape[2])
    dom, cls = lax.axis_index("dom"), lax.axis_index("cls")
    here = dict(x=cls // 2, y=dom % size["y"], z=dom // size["y"])
    core = cls % 2
    rows = out_ref.shape[2]
    starts = [0]
    for share in SHARE:
        starts.append(starts[-1] + rows * share // 32)

    def device(at, which):
        return (at["z"] * size["y"] + at["y"], at["x"] * 2 + which)

    def slot(at, which):
        d = device(at, which)
        return d[0] * (size["x"] * 2) + d[1]

    def moved(at, dim, step):
        new = dict(at)
        new[dim] = at[dim] + step
        return new

    ways = []
    for dim in "xyz":
        if size[dim] == 1:
            continue
        if size[dim] == 2:
            other = dict(here)
            other[dim] = 1 - here[dim]
            ways.append((dim, 0, other, None))
        else:
            ways.append((dim, 1, moved(here, dim, 1), here[dim] < size[dim] - 1))
            ways.append((dim, -1, moved(here, dim, -1), here[dim] > 0))

    def when(conds, fn):
        conds = [c for c in conds if c is not None]
        if not conds:
            fn()
        else:
            pl.when(functools.reduce(jnp.logical_and, conds))(fn)

    barrier = pltpu.get_barrier_semaphore()
    partner = device(here, 1 - core)
    pl.semaphore_signal(barrier, inc=1, device_id=partner, device_id_type=MESH)
    for dim, sign, other, ok in ways:

        def greet(other=other):
            pl.semaphore_signal(barrier, inc=1, device_id=device(other, core), device_id_type=MESH)

        when([ok], greet)
    peers = 1
    for dim, sign, other, ok in ways:
        peers = peers + (1 if ok is None else ok.astype(jnp.int32))
    pl.semaphore_wait(barrier, peers)

    mine = slot(here, core)
    local = pltpu.make_async_copy(own_ref, out_ref.at[mine], local_sem)
    local.start()

    def part(ref, index):
        return ref.at[:, pl.ds(starts[index], starts[index + 1] - starts[index]), :]

    def copy(index, source, src_slot, to, way, own):
        src = part(own_ref, index) if own else part(out_ref.at[src_slot], index)
        return pltpu.make_async_remote_copy(
            src_ref=src,
            dst_ref=part(out_ref.at[src_slot], index),
            send_sem=send_sem.at[index, source, way],
            recv_sem=recv_sem.at[index, src_slot],
            device_id=to,
            device_id_type=MESH,
        )

    def pair_copy(index, source, src_slot, own):
        src = part(own_ref, index) if own else part(out_ref.at[src_slot], index)
        return pltpu.make_async_remote_copy(
            src_ref=src,
            dst_ref=part(out_ref.at[src_slot], index),
            send_sem=pair_send.at[index, source],
            recv_sem=pair_recv.at[index, src_slot],
            device_id=partner,
            device_id_type=MESH,
        )

    choices = {}
    for dim in "xyz":
        n = size[dim]
        if n == 1:
            choices[dim] = [(0, here[dim], None, 0)]
        elif n == 2:
            choices[dim] = [(0, here[dim], None, 0), (0, 1 - here[dim], None, 1)]
        else:
            listed = [(0, here[dim], None, 0)]
            for t in range(1, n):
                listed.append((1, here[dim] - t, here[dim] >= t, t))
                listed.append((-1, here[dim] + t, here[dim] + t < n, t))
            choices[dim] = listed
    events = []
    for ix, cx in enumerate(choices["x"]):
        for iy, cy in enumerate(choices["y"]):
            for iz, cz in enumerate(choices["z"]):
                pick = dict(x=cx, y=cy, z=cz)
                depth = cx[3] + cy[3] + cz[3]
                number = (ix * len(choices["y"]) + iy) * len(choices["z"]) + iz
                for index in range(3):
                    events.append((depth, index, number, pick))
    events.sort(key=lambda e: e[:3])
    finish = []
    for depth, index, number, pick in events:
        at = {dim: pick[dim][1] for dim in "xyz"}
        exists = [pick[dim][2] for dim in "xyz"]
        src_slot = slot(at, core)
        order = ROUTES[index]
        last = max([k for k, dim in enumerate(order) if pick[dim][3] > 0], default=-1)
        sends = []
        for number_way, (dim, sign, other, ok) in enumerate(ways):
            k = order.index(dim)
            if k < last:
                continue
            if k == last and (size[dim] == 2 or sign != pick[dim][0]):
                continue
            sends.append((number_way, device(other, core), ok))

        def arrive(index=index, number=number, src_slot=src_slot, depth=depth, sends=sends):
            own = depth == 0
            if not own:
                copy(index, number, src_slot, partner, 0, False).wait_recv()
            for way, to, ok in sends:
                when([ok], copy(index, number, src_slot, to, way, own).start)
            pair_copy(index, number, src_slot, own).start()

        def done(index=index, number=number, src_slot=src_slot, depth=depth, sends=sends, at=at):
            own = depth == 0
            for way, to, ok in sends:
                when([ok], copy(index, number, src_slot, to, way, own).wait_send)
            pair_copy(index, number, src_slot, own).wait_send()
            pair_copy(index, number, slot(at, 1 - core), False).wait_recv()

        when(exists, arrive)
        finish.append((exists, done))
    for exists, done in finish:
        when(exists, done)
    local.wait()


def gather(shape, own):
    devices = 2 * shape[0] * shape[1] * shape[2]
    total = 1
    for n in shape:
        total *= n if n <= 2 else 2 * n - 1
    return pl.pallas_call(
        functools.partial(gather_kernel, shape),
        out_shape=jax.ShapeDtypeStruct((devices,) + own.shape, own.dtype),
        in_specs=[pl.BlockSpec(memory_space=pltpu.VMEM)],
        out_specs=pl.BlockSpec(memory_space=pltpu.VMEM),
        scratch_shapes=[
            pltpu.SemaphoreType.DMA,
            pltpu.SemaphoreType.DMA((3, total, 4)),
            pltpu.SemaphoreType.DMA((3, devices)),
            pltpu.SemaphoreType.DMA((3, total)),
            pltpu.SemaphoreType.DMA((3, devices)),
        ],
        compiler_params=pltpu.CompilerParams(
            collective_id=0, has_side_effects=True, vmem_limit_bytes=12 * 1024 * 1024
        ),
        name="gather_slices",
    )(own)


def power_kernel(
    side, rot_count, classes_ref, rotations_ref, defocus_ref, images_ref, slices_ref, slope_ref, offset_ref, groups_ref, out_ref, power, acc
):
    step = pl.program_id(0)
    count, chunk, lanes = images_ref.shape
    shells = side // 2
    pitch = power.shape[0] // count

    @pl.when(step == 0)
    def _():
        acc[...] = jnp.zeros_like(acc)

    slope = slope_ref[...]
    offset = offset_ref[...]

    def one(i, carry):
        turns = defocus_ref[i].astype(jnp.float32) * slope + offset
        x = turns - ((turns + ROUND) - ROUND)
        y = x * x
        s = jnp.full_like(y, SINE[-1])
        for value in SINE[-2::-1]:
            s = s * y + value
        s = s * x
        d = images_ref[i].astype(jnp.float32) + s * slices_ref[classes_ref[i] * rot_count + rotations_ref[i]].astype(jnp.float32)
        power[pl.ds(pl.multiple_of(i * pitch, 8), chunk), :] = d * d
        return carry

    lax.fori_loop(0, count, one, 0, unroll=8)

    b = lax.broadcasted_iota(jnp.int32, (lanes, shells), 0)
    s = lax.broadcasted_iota(jnp.int32, (lanes, shells), 1)
    fb = jnp.where(b < side // 2, b, b - side)
    total = acc[...]
    for k in range(chunk // 2):
        a = step * (chunk // 2) + k
        fa = jnp.where(a < side // 2, a, a - side)
        r = fa * fa + fb * fb
        table = jnp.where((s * s <= r) & (r < (s + 1) * (s + 1)), 1.0, 0.0).astype(jnp.bfloat16)
        p = power[pl.ds(2 * k, count, stride=pitch), :] + power[pl.ds(2 * k + 1, count, stride=pitch), :]
        high = p.astype(jnp.bfloat16)
        low = (p - high.astype(jnp.float32)).astype(jnp.bfloat16)
        total = total + jnp.dot(
            jnp.concatenate([high, low], axis=1),
            jnp.concatenate([table, table], axis=0),
            preferred_element_type=jnp.float32,
        )
    acc[...] = total

    @pl.when(step == pl.num_programs(0) - 1)
    def _():
        groups = out_ref.shape[0]
        ids = lax.broadcasted_iota(jnp.int32, (groups, count), 0)
        member = jnp.where(ids == groups_ref[...], 1.0, 0.0)
        both = jnp.concatenate([acc[...], jnp.ones((count, out_ref.shape[1] - shells), jnp.float32)], axis=1)
        out_ref[...] = jnp.dot(
            member, both, precision=lax.Precision.HIGHEST, preferred_element_type=jnp.float32
        )


def shell_power(images, slices, classes, rotations, rot_count, defocus, groups, group_total):
    count, rows, side = images.shape
    chunk = 32
    offsets = np.arange(side)
    signed = np.where(offsets < side // 2, offsets, offsets - side)
    radius = (signed[:, None] ** 2 + signed[None, :] ** 2).astype(np.float64)
    spatial = np.repeat(radius / (side * PIXEL_SIZE) ** 2, 2, axis=0)
    slope = (0.5 * WAVELENGTH * spatial).astype(np.float32)
    offset = -0.25 * SPHERICAL * WAVELENGTH**3 * spatial**2 + math.asin(AMPLITUDE) / (2 * math.pi)
    offset = (offset - np.round(offset)).astype(np.float32)
    smem = pl.BlockSpec(memory_space=pltpu.SMEM)
    return pl.pallas_call(
        functools.partial(power_kernel, side, rot_count),
        grid=(rows // chunk,),
        out_shape=jax.ShapeDtypeStruct((group_total, 128), jnp.float32),
        in_specs=[
            smem,
            smem,
            smem,
            pl.BlockSpec((count, chunk, side), lambda i: (0, i, 0)),
            pl.BlockSpec((slices.shape[0], chunk, side), lambda i: (0, i, 0)),
            pl.BlockSpec((chunk, side), lambda i: (i, 0)),
            pl.BlockSpec((chunk, side), lambda i: (i, 0)),
            pl.BlockSpec((1, count), lambda i: (0, 0)),
        ],
        out_specs=pl.BlockSpec((group_total, 128), lambda i: (0, 0)),
        scratch_shapes=[
            pltpu.VMEM((count * (chunk + 8), side), jnp.float32),
            pltpu.VMEM((count, side // 2), jnp.float32),
        ],
        compiler_params=pltpu.CompilerParams(vmem_limit_bytes=20 * 1024 * 1024),
        name="shell_power",
    )(classes, rotations, defocus, images, slices, jnp.asarray(slope), jnp.asarray(offset), groups.reshape(1, count))


def exchange_kernel(sizes, shells, parts_ref, weight_ref, out_ref, held, send_sem, recv_sem):
    doms, clss = sizes
    n = doms * clss
    me = lax.axis_index("dom") * clss + lax.axis_index("cls")
    barrier = pltpu.get_barrier_semaphore()

    def device(k):
        peer = lax.rem(me + k, n)
        return peer, (peer // clss, lax.rem(peer, clss))

    def greet(k, carry):
        pl.semaphore_signal(barrier, inc=1, device_id=device(k)[1], device_id_type=MESH)
        return carry

    lax.fori_loop(1, n, greet, 0)
    pl.semaphore_wait(barrier, n - 1)

    def copy(k):
        peer, to = device(k)
        return pltpu.make_async_remote_copy(
            src_ref=parts_ref.at[peer],
            dst_ref=held.at[k],
            send_sem=send_sem.at[k],
            recv_sem=recv_sem.at[k],
            device_id=to,
            device_id_type=MESH,
        )

    def send(k, carry):
        copy(k).start()
        return carry

    lax.fori_loop(1, n, send, 0)

    def take(k, total):
        copy(k).wait_recv()
        return total + held[k]

    total = lax.fori_loop(1, n, take, parts_ref[me])

    def sent(k, carry):
        copy(k).wait_send()
        return carry

    lax.fori_loop(1, n, sent, 0)
    counts = total[:, shells : shells + 1]
    out_ref[...] = total[:, :shells] / (2.0 * counts * weight_ref[...])


def exchange(sizes, parts, weight):
    n = sizes[0] * sizes[1]
    shells = weight.shape[1]
    vmem = pl.BlockSpec(memory_space=pltpu.VMEM)
    return pl.pallas_call(
        functools.partial(exchange_kernel, sizes, shells),
        out_shape=jax.ShapeDtypeStruct((GROUPS_DEV, shells), jnp.float32),
        in_specs=[vmem, vmem],
        out_specs=vmem,
        scratch_shapes=[
            pltpu.VMEM((n, GROUPS_DEV, parts.shape[-1]), jnp.float32),
            pltpu.SemaphoreType.DMA((n,)),
            pltpu.SemaphoreType.DMA((n,)),
        ],
        compiler_params=pltpu.CompilerParams(
            collective_id=1, has_side_effects=True, vmem_limit_bytes=4 * 1024 * 1024
        ),
        name="exchange_groups",
    )(parts.reshape(n, GROUPS_DEV, parts.shape[-1]), weight)


PIECES = ((0, (0, 6, 13)), (1, (1, 2, 3, 10, 11, 12)), (2, (4, 5, 7, 8, 9)))
SCHEDULE = (
    (0, "o", 0), (1, "o", 0), (2, "o", 0), ("fill", 6), (0, "x", 0), (1, "a", 0), (1, "z", 1), (2, "a", 0),
    ("fill", 2), (2, "z", 1), (0, "y", 0), ("fill", 4), (1, "z", 2), (1, "a", 1), ("fill", 2), (2, "z", 2),
    (2, "a", 1), ("fill", 4), (1, "z", 3), (1, "a", 2), (0, "z", 1), ("fill", 4), (2, "z", 3), (2, "a", 2),
    ("fill", 4), (1, "a", 3), (2, "a", 3), (0, "z", 2), (2, "b", 0), (1, "b", 0), (2, "b", 1), (1, "b", 1),
    ("fill", 2), (2, "b", 2), (1, "b", 2), (2, "b", 3), (1, "b", 3), ("calc", 2), (0, "z", 3), ("calc", 1),
    ("calc", 0),
)
UNIT = 8
TILE = 8


def folded_rows(side):
    half = side // 2
    low, high = half - TILE, half + TILE
    kept = np.concatenate([np.arange(low), np.arange(high, side)])
    other = kept.copy()
    other[low - TILE : low] = half - 1 - np.arange(TILE)
    other[low : low + TILE] = high - np.arange(TILE)
    return kept, other


def folded_radius(side):
    half = side // 2
    offsets = np.arange(side)
    signed = np.where(offsets < half, offsets, offsets - side)
    radius = signed[:, None] ** 2 + signed[None, :] ** 2
    kept, other = folded_rows(side)
    own, far = radius[kept], np.roll(radius[other], half, axis=1)
    inside = own < half * half
    fold = (other != kept)[:, None] & ~inside
    assert not np.any((other != kept)[:, None] & inside & (far < half * half))
    packed = np.where(fold, far, own)
    assert np.sum(packed < half * half) == np.sum(radius < half * half)
    return packed


def runs_of(tiles):
    runs = []
    for k, t in enumerate(tiles):
        if runs and runs[-1][1] + runs[-1][2] == t:
            runs[-1][2] += 1
        else:
            runs.append([k, t, 1])
    return runs


def row_groups(tiles, side):
    place = {TILE * t + r: TILE * k + r for k, t in enumerate(tiles) for r in range(TILE)}
    kept, other = folded_rows(side)
    plain = {int(a): j for j, a in enumerate(kept) if other[j] == a and (a == 0 or other[j - 1] == kept[j - 1])}
    groups, used = [], set()
    for j in sorted(place):
        if j in used:
            continue
        a = int(kept[j])
        mate = plain.get(side - a) if plain.get(a) == j else None
        if mate is not None and mate != j and mate in place:
            used.add(mate)
            groups.append((j, (place[j], place[mate])))
        else:
            groups.append((j, (place[j],)))
    return groups


def fold(keep, far, shifted, first_row, side):
    lines = 2 * TILE
    order = [(-i if shifted else TILE - 1 - i) % TILE for i in range(TILE)]
    far = far.astype(jnp.float32)
    far = jnp.concatenate([far[2 * k : 2 * k + 2] for k in order], axis=0)
    far = pltpu.roll(far, side // 2, axis=1)
    a = first_row + lax.broadcasted_iota(jnp.int32, (lines, side), 0) // 2
    b = lax.broadcasted_iota(jnp.int32, (lines, side), 1)
    fa = jnp.where(a < side // 2, a, a - side)
    fb = jnp.where(b < side // 2, b, b - side)
    inside = fa * fa + fb * fb < (side // 2) * (side // 2)
    return jnp.where(inside, keep.astype(jnp.float32), far).astype(keep.dtype)


def fused_kernel(
    nz,
    side,
    classes_here,
    rot_count,
    layout,
    classes_hbm,
    rotations_hbm,
    defocus_hbm,
    slope_hbm,
    offset_hbm,
    groups_hbm,
    weight_hbm,
    own_hbm,
    images_hbm,
    out_ref,
    *scratch,
):
    pieces, tiles = layout
    count = images_hbm.shape[0]
    shells = side // 2
    rows = 16 * tiles
    half = rows // 2
    bufs = scratch[: len(pieces)]
    (
        classes_ref,
        rotations_ref,
        defocus_ref,
        slope_ref,
        offset_ref,
        groups_ref,
        weight_ref,
        images,
        image_rim,
        own_rim,
        sine,
        power,
        table,
        acc,
        parts,
        held,
        local_sem,
        image_sem,
        small_sem,
        send_sem,
        recv_sem,
        pair_send,
        pair_recv,
        part_send,
        part_recv,
    ) = scratch[len(pieces) :]
    dom, cls = lax.axis_index("dom"), lax.axis_index("cls")
    x, core, y, z = cls // 2, cls % 2, dom % 2, dom // 2
    slot = classes_here * rot_count

    def device(x_, y_, z_, core_):
        return (z_ * 2 + y_, x_ * 2 + core_)

    partner = device(x, y, z, 1 - core)
    up, down = device(x, y, z + 1, core), device(x, y, z - 1, core)
    across = {"x": device(1 - x, y, z, core), "y": device(x, 1 - y, z, core)}

    def when(conds, fn):
        conds = [c for c in conds if c is not None]
        if not conds:
            fn()
        else:
            pl.when(functools.reduce(jnp.logical_and, conds))(fn)

    barrier = pltpu.get_barrier_semaphore()
    for to in (partner, across["x"], across["y"]):
        pl.semaphore_signal(barrier, inc=1, device_id=to, device_id_type=MESH)
    has_up, has_down = z < nz - 1, z > 0
    when([has_up], lambda: pl.semaphore_signal(barrier, inc=1, device_id=up, device_id_type=MESH))
    when([has_down], lambda: pl.semaphore_signal(barrier, inc=1, device_id=down, device_id_type=MESH))

    line = 2 * TILE
    rim = tiles // 2 - 1
    own_copies = [
        pltpu.make_async_copy(own_hbm.at[:, pl.ds(line * rim, 4 * line), :], own_rim, local_sem.at[0])
    ]
    rim_stores = []
    for p, (route, held_tiles) in enumerate(pieces):
        q1, q2 = (x, y) if route == 1 else (y, x)
        at = (((core * nz + z) * 2 + q1) * 2 + q2) * slot
        for k, t in enumerate(held_tiles):
            if rim <= t < rim + 2:
                rim_stores.append((p, at, line * k, t - rim))
        for k, t, n in runs_of([t if not rim <= t < rim + 2 else -line * t for t in held_tiles]):
            if t >= 0:
                own_copies.append(
                    pltpu.make_async_copy(
                        own_hbm.at[:, pl.ds(line * (t + 2 * (t > rim)), line * n), :],
                        bufs[p].at[pl.ds(at, slot), pl.ds(line * k, line * n), :],
                        local_sem.at[len(own_copies)],
                    )
                )
    for c in own_copies:
        c.start()
    edge = line * rim
    image_copies = [
        pltpu.make_async_copy(images_hbm.at[:, pl.ds(edge, 4 * line), :], image_rim, image_sem.at[0]),
        pltpu.make_async_copy(images_hbm.at[:, pl.ds(0, edge), :], images.at[:, pl.ds(0, edge), :], image_sem.at[1]),
        pltpu.make_async_copy(
            images_hbm.at[:, pl.ds(edge + 4 * line, edge), :],
            images.at[:, pl.ds(edge + 2 * line, edge), :],
            image_sem.at[2],
        ),
    ]
    small = (
        (slope_hbm, slope_ref),
        (offset_hbm, offset_ref),
        (defocus_hbm, defocus_ref),
        (classes_hbm, classes_ref),
        (rotations_hbm, rotations_ref),
        (groups_hbm, groups_ref),
        (weight_hbm, weight_ref),
    )
    small_copies = [pltpu.make_async_copy(src, dst, small_sem.at[k]) for k, (src, dst) in enumerate(small)]
    for c in small_copies:
        c.start()

    def folded(ref, i, k):
        keep = ref[i, pl.ds(3 * line * k, line), :]
        far = ref[i, pl.ds(line * (1 + k), line), :]
        return fold(keep, far, k == 1, TILE * (rim + 3 * k), side)

    for c in own_copies:
        c.wait()
    for c in image_copies:
        c.start()
    for p, at, row, k in rim_stores:
        for j in range(slot):
            bufs[p][at + j, pl.ds(row, line), :] = folded(own_rim, j, k)
    pl.semaphore_wait(barrier, 3 + has_up.astype(jnp.int32) + has_down.astype(jnp.int32))

    events = []
    for p, (route, n) in enumerate(pieces):
        q1, q2 = (x, y) if route == 1 else (y, x)
        to_q1, to_q2 = (across["x"], across["y"]) if route == 1 else (across["y"], across["x"])
        buf = bufs[p]

        def region(core_, z_, a=None, b=None, buf=buf):
            first = (core_ * nz + z_) * 4 * slot
            size = 4 * slot
            if a is not None:
                first, size = first + a * 2 * slot, 2 * slot
            if b is not None:
                first, size = first + b * slot, slot
            return buf.at[pl.ds(first, size)]

        def link(stage, zs, number, where, to, p=p):
            return pltpu.make_async_remote_copy(
                src_ref=where,
                dst_ref=where,
                send_sem=send_sem.at[p],
                recv_sem=recv_sem.at[p, stage, zs],
                device_id=to,
                device_id_type=MESH,
            )

        def pair(stage, zs, where, p=p):
            return pltpu.make_async_remote_copy(
                src_ref=where,
                dst_ref=where,
                send_sem=pair_send.at[p],
                recv_sem=pair_recv.at[p],
                device_id=partner,
                device_id_type=MESH,
            )

        reach = [(z, None, 0, None)]
        for t in range(1, nz):
            reach.append((z - t, z >= t, t, -1))
            reach.append((z + t, z + t < nz, t, 1))

        if route == 0:
            one = region(core, z, q1, q2)
            other = region(core, z, q1, 1 - q2)
            mine = region(core, z, q1)
            events.append(((p, "o", 0), p, [], [], [(None, link(0, z, 0, one, to_q2))], None))
            events.append(((p, "x", 0), p, [], [link(0, z, 0, other, to_q2)], [(None, link(1, z, 0, mine, to_q1))], None))
            for k, (zs, ok, t, way) in enumerate(reach):
                block = region(core, zs)
                sends = []
                if way in (None, -1):
                    sends.append((has_up, link(2, zs, 2 * k, block, up)))
                if way in (None, 1):
                    sends.append((has_down, link(2, zs, 2 * k + 1, block, down)))
                arrival = link(1, z, 0, region(core, z, 1 - q1), to_q1) if way is None else link(2, zs, 0, block, up)
                twin = region(1 - core, zs)
                name = (p, "z" if t else "y", t)
                events.append((name, p, [ok], [arrival], sends, (pair(0, zs, block), pair(0, zs, twin))))
        else:
            for k, (zs, ok, t, way) in enumerate(reach):
                one = region(core, zs, q1, q2)
                sends = []
                if way in (None, -1):
                    sends.append((has_up, link(0, zs, 2 * k, one, up)))
                if way in (None, 1):
                    sends.append((has_down, link(0, zs, 2 * k + 1, one, down)))
                sends.append((None, link(1, zs, k, one, to_q2)))
                arrival = [] if way is None else [link(0, zs, 0, one, up)]
                events.append(((p, "z" if t else "o", t), p, [ok], arrival, sends, None))
                near, far = region(core, zs, q1), region(core, zs, 1 - q1)
                events.append(
                    (
                        (p, "a", t),
                        p,
                        [ok],
                        [link(1, zs, 0, region(core, zs, q1, 1 - q2), to_q2)],
                        [(None, link(2, zs, k, near, to_q1))],
                        (pair(0, zs, near), pair(0, zs, region(1 - core, zs, q1))),
                    )
                )
                events.append(
                    (
                        (p, "b", t),
                        p,
                        [ok],
                        [link(2, zs, 0, far, to_q1)],
                        [],
                        (pair(1, zs, far), pair(1, zs, region(1 - core, zs, 1 - q1))),
                    )
                )

    def make_sine(i, carry):
        turns = defocus_ref[i].astype(jnp.float32) * slope_ref[...] + offset_ref[...]
        v = turns - ((turns + ROUND) - ROUND)
        w = v * v
        s = jnp.full_like(w, SINE[-1])
        for value in SINE[-2::-1]:
            s = s * w + value
        s = s * v
        base = pl.multiple_of(i * rows, 8)
        sine[pl.ds(base, half, stride=2), :] = s
        sine[pl.ds(base + 1, half, stride=2), :] = s
        return carry

    def sine_unit(j):
        def run():
            if j == 0:
                for c in small_copies[:3]:
                    c.wait()
            lax.fori_loop(j * UNIT, (j + 1) * UNIT, make_sine, 0, unroll=2)

        return run

    def make_table(a, carry):
        b = lax.broadcasted_iota(jnp.int32, (side, shells), 0)
        s = lax.broadcasted_iota(jnp.int32, (side, shells), 1)
        low = TILE * (rim + 1)
        row = jnp.where(a < low, a, a + 2 * TILE)
        far = jnp.where(a < low, side // 2 - 1 + TILE * rim - a, side // 2 + TILE + low - a)
        fb = jnp.where(b < side // 2, b, b - side)
        gb = b - side // 2
        fa = jnp.where(row < side // 2, row, row - side)
        ga = jnp.where(far < side // 2, far, far - side)
        r = fa * fa + fb * fb
        folds = (a >= TILE * rim) & (a < TILE * (rim + 2)) & (a != low)
        r = jnp.where(folds & (r >= (side // 2) * (side // 2)), ga * ga + gb * gb, r)
        inside = (s * s <= r) & (r < (s + 1) * (s + 1))
        table[a] = jnp.where(inside, 1.0, 0.0).astype(jnp.bfloat16)
        return carry

    def table_unit(j, n):
        return lambda: lax.fori_loop(j * n, (j + 1) * n, make_table, 0)

    def fold_image(i, carry):
        for k in range(2):
            images[i, pl.ds(line * (rim + k), line), :] = folded(image_rim, i, k)
        return carry

    def fold_unit(j):
        def run():
            if j == 0:
                image_copies[0].wait()
            lax.fori_loop(j * 4 * UNIT, (j + 1) * 4 * UNIT, fold_image, 0, unroll=4)

        return run

    fillers = [table_unit(j, half // 8) for j in range(8)] + [sine_unit(j) for j in range(count // UNIT)]
    fillers += [fold_unit(j) for j in range(count // (4 * UNIT))]
    fillers.reverse()
    calculated = []
    acc[...] = jnp.zeros_like(acc)

    def twins(p):
        where = bufs[p].at[pl.ds((1 - core) * (4 * nz * slot), 4 * nz * slot)]
        return pltpu.make_async_remote_copy(
            src_ref=where,
            dst_ref=where,
            send_sem=pair_send.at[p],
            recv_sem=pair_recv.at[p],
            device_id=partner,
            device_id_type=MESH,
        )

    def calc(p):
        route, held_tiles = pieces[p]
        if not calculated:
            for c in image_copies[1:] + small_copies[3:]:
                c.wait()
        calculated.append(p)
        twins(p).wait_recv()
        pitch = line * len(held_tiles) + TILE

        def one(i, carry, p=p, route=route, held_tiles=held_tiles, pitch=pitch):
            c = classes_ref[i]
            owner, sub = (c, 0) if classes_here == 1 else (c // classes_here, c % classes_here)
            place = owner >> 1
            if route == 1:
                place = (place & ~3) | ((place & 1) << 1) | ((place >> 1) & 1)
            at = ((owner & 1) * (nz * 4) + place) * slot + sub * rot_count + rotations_ref[i]
            for k, t, n in runs_of(held_tiles):
                f = bufs[p][at, pl.ds(line * k, line * n), :].astype(jnp.float32)
                s = sine[pl.ds(pl.multiple_of(i * rows + line * t, 8), line * n), :]
                d = images[i, pl.ds(line * t, line * n), :].astype(jnp.float32) + s * f
                power[pl.ds(pl.multiple_of(i * pitch + line * k, 8), line * n), :] = d * d
            return carry

        lax.fori_loop(0, count, one, 0, unroll=16)
        total = acc[...]
        for j, places in row_groups(held_tiles, side):
            v = None
            for k in places:
                for part in range(2):
                    w = power[pl.ds(2 * k + part, count, stride=pitch), :]
                    v = w if v is None else v + w
            high = v.astype(jnp.bfloat16)
            low = (v - high.astype(jnp.float32)).astype(jnp.bfloat16)
            t = table[j]
            total = total + jnp.dot(
                jnp.concatenate([high, low], axis=1),
                jnp.concatenate([t, t], axis=0),
                preferred_element_type=jnp.float32,
            )
        acc[...] = total

    def amount(p, slots):
        where = bufs[p].at[pl.ds(0, slots * slot)]
        return pltpu.make_async_remote_copy(
            src_ref=where,
            dst_ref=where,
            send_sem=send_sem.at[p],
            recv_sem=pair_recv.at[p],
            device_id=partner,
            device_id_type=MESH,
        )

    def handle(event):
        _, _, exists, arrivals, sends, twin = event

        def arrive():
            for c in arrivals:
                c.wait_recv()
            for ok, c in sends:
                when([ok], c.start)
            if twin is not None:
                twin[0].start()

        when(exists, arrive)

    for step in SCHEDULE:
        if step[0] == "fill":
            for _ in range(step[1]):
                fillers.pop()()
        elif step[0] == "calc":
            calc(step[1])
        else:
            for event in events:
                if event[0] == step:
                    handle(event)
    assert not fillers and len(calculated) == len(pieces)

    owners, groups_here = parts.shape[:2]
    ids = lax.broadcasted_iota(jnp.int32, (owners * groups_here, count), 0)
    member = jnp.where(ids == groups_ref[...], 1.0, 0.0).astype(jnp.bfloat16)
    rest = jnp.concatenate([acc[...], jnp.ones((count, parts.shape[2] - shells), jnp.float32)], axis=1)
    terms = []
    for _ in range(3):
        terms.append(rest.astype(jnp.bfloat16))
        rest = rest - terms[-1].astype(jnp.float32)
    parts[...] = jnp.dot(
        jnp.concatenate([member] * 3, axis=1), jnp.concatenate(terms, axis=0), preferred_element_type=jnp.float32
    ).reshape(parts.shape)

    me = dom * 4 + cls
    everyone = pl.ds(1, owners - 1)

    def part_copy(k):
        peer = me + k
        peer = jnp.where(peer >= owners, peer - owners, peer)
        return pltpu.make_async_remote_copy(
            src_ref=parts.at[peer],
            dst_ref=held.at[k],
            send_sem=part_send,
            recv_sem=part_recv,
            device_id=(peer >> 2, peer & 3),
            device_id_type=MESH,
        )

    for k in range(1, owners):
        part_copy(k).start()
    for p, (route, held_tiles) in enumerate(pieces):
        twins(p).wait_send()
        inner = (3 + 4 * (nz + 1)) if route == 0 else 3 * nz + nz + 1
        outer = (3 + 4) if route == 0 else 3 * nz + 1
        inside = has_up & has_down
        when([inside], amount(p, inner).wait_send)
        when([jnp.logical_not(inside)], amount(p, outer).wait_send)

    all_parts = pltpu.make_async_remote_copy(
        src_ref=held.at[everyone],
        dst_ref=held.at[everyone],
        send_sem=part_send,
        recv_sem=part_recv,
        device_id=partner,
        device_id_type=MESH,
    )
    all_parts.wait_recv()
    total = parts[me] + jnp.sum(held[everyone], axis=0)
    all_parts.wait_send()
    counts = total[:, shells : shells + 1]
    out_ref[...] = total[:, :shells] / (2.0 * counts * weight_ref[...])


def pixel_tables(side):
    offsets = np.arange(side)
    signed = np.where(offsets < side // 2, offsets, offsets - side)
    radius = (signed[:, None] ** 2 + signed[None, :] ** 2).astype(np.float64)
    spatial = folded_radius(side).astype(np.float64) / (side * PIXEL_SIZE) ** 2
    slope = (0.5 * WAVELENGTH * spatial).astype(np.float32)
    offset = -0.25 * SPHERICAL * WAVELENGTH**3 * spatial**2 + math.asin(AMPLITUDE) / (2 * math.pi)
    offset = (offset - np.round(offset)).astype(np.float32)
    s = np.arange(side // 2)[:, None, None]
    weight = ((s * s <= radius) & (radius < (s + 1) ** 2)).sum(axis=(1, 2)).astype(np.float32)
    return slope, offset, weight.reshape(1, -1)


def fused(nz, images, own, classes, rotations, defocus, groups, classes_here, rot_count, owners):
    count, rows, side = images.shape
    shells = side // 2
    pieces = PIECES
    tiles = sum(len(held) for _, held in pieces)
    slots = owners * classes_here * rot_count
    slope, offset, weight = pixel_tables(side)
    vmem = pl.BlockSpec(memory_space=pltpu.VMEM)
    hbm = pl.BlockSpec(memory_space=pltpu.HBM)
    dma = pltpu.SemaphoreType.DMA
    widest = max(len(held) for _, held in pieces)
    return pl.pallas_call(
        functools.partial(fused_kernel, nz, side, classes_here, rot_count, (pieces, tiles)),
        out_shape=jax.ShapeDtypeStruct((GROUPS_DEV, shells), jnp.float32),
        in_specs=[hbm] * 9,
        out_specs=vmem,
        scratch_shapes=[pltpu.VMEM((slots, 16 * len(held), side), jnp.bfloat16) for _, held in pieces]
        + [pltpu.SMEM((count,), jnp.int32)] * 3
        + [
            pltpu.VMEM(slope.shape, jnp.float32),
            pltpu.VMEM(slope.shape, jnp.float32),
            pltpu.VMEM((1, count), jnp.int32),
            pltpu.VMEM(weight.shape, jnp.float32),
            pltpu.VMEM((count, 16 * tiles, side), jnp.bfloat16),
            pltpu.VMEM((count, 8 * TILE, side), jnp.bfloat16),
            pltpu.VMEM((classes_here * rot_count, 8 * TILE, side), jnp.bfloat16),
            pltpu.VMEM((count * 16 * tiles, side), jnp.float32),
            pltpu.VMEM((count * (16 * widest + 8), side), jnp.float32),
            pltpu.VMEM((8 * tiles, side, shells), jnp.bfloat16),
            pltpu.VMEM((count, shells), jnp.float32),
            pltpu.VMEM((owners, GROUPS_DEV, 128), jnp.float32),
            pltpu.VMEM((owners, GROUPS_DEV, 128), jnp.float32),
            dma((sum(len(runs_of(held)) for _, held in pieces) + 3,)),
            dma((3,)),
            dma((7,)),
            dma((len(pieces),)),
            dma((len(pieces), 3, nz)),
            dma((len(pieces),)),
            dma((len(pieces),)),
            dma,
            dma,
        ],
        compiler_params=pltpu.CompilerParams(
            collective_id=0, has_side_effects=True, vmem_limit_bytes=50 * 1024 * 1024
        ),
        name="fused_spectrum",
    )(
        *(
            pltpu.with_memory_space_constraint(operand, pltpu.HBM)
            for operand in (
                classes,
                rotations,
                defocus,
                jnp.asarray(slope),
                jnp.asarray(offset),
                groups.reshape(1, count),
                jnp.asarray(weight),
                own,
                images,
            )
        )
    )


def body(sizes, images, slices, classes, rotations, defocus, groups):
    doms, clss = sizes
    n = doms * clss
    count, _, pixels = images.shape
    side = math.isqrt(pixels)
    classes_here, rot_count = slices.shape[:2]

    def rows_of(array):
        lead = array.shape[:-2]
        split = array.reshape(lead + (2, side, side))
        return jnp.swapaxes(split, -3, -2).reshape(lead + (2 * side, side))

    own = rows_of(slices).reshape(classes_here * rot_count, 2 * side, side)
    if clss == 4 and doms == 8 and side == 16 * TILE:
        return fused(
            doms // 2, rows_of(images), own, classes, rotations, defocus, groups, classes_here, rot_count, n
        )
    ny = clss // 2
    if clss % 2 == 0 and doms % ny == 0 and n <= 32:
        every = gather((ny, ny, doms // ny), own)
    else:
        every = lax.all_gather(own, AXES, axis=0)
    every = every.reshape(n * own.shape[0], 2 * side, side)
    parts = shell_power(rows_of(images), every, classes, rotations, rot_count, defocus, groups, GROUPS_DEV * n)
    offsets = np.arange(side)
    signed = np.where(offsets < side // 2, offsets, offsets - side)
    radius = signed[:, None] ** 2 + signed[None, :] ** 2
    s = np.arange(side // 2)[:, None, None]
    weight = ((s * s <= radius) & (radius < (s + 1) ** 2)).sum(axis=(1, 2)).astype(np.float32)
    return exchange(sizes, parts, jnp.asarray(weight).reshape(1, -1))


def solution(mesh):
    sizes = (mesh.shape["dom"], mesh.shape["cls"])
    return jax.shard_map(
        functools.partial(body, sizes),
        mesh=mesh,
        in_specs=(
            P(AXES, None, None),
            P(AXES, None, None, None),
            P(AXES),
            P(AXES),
            P(AXES),
            P(AXES),
        ),
        out_specs=P(AXES, None),
        check_vma=False,
    )
```

```python
import functools
import math

import jax
import jax.numpy as jnp
import numpy as np
from jax import lax
from jax.experimental import pallas as pl
from jax.experimental.pallas import tpu as pltpu
from jax.sharding import PartitionSpec as P

GROUPS_DEV = 8
PIXEL_SIZE = 1.5
WAVELENGTH = 0.0197
SPHERICAL = 27000000.0
AMPLITUDE = 0.1
ROUND = 12582912.0
MESH = pl.DeviceIdType.MESH
AXES = ("dom", "cls")
ROUTES = (("x", "y", "z"), ("z", "y", "x"), ("z", "x", "y"))
SHARE = (8, 12, 12)


def sine_coefficients(terms):
    nodes = 0.5 * np.cos((np.arange(400) + 0.5) * math.pi / 400)
    nodes = nodes[np.abs(nodes) > 1e-3]
    basis = np.stack([nodes ** (2 * k + 1) for k in range(terms)], 1)
    return np.linalg.lstsq(basis, np.sin(2 * math.pi * nodes), rcond=None)[0]


SINE = [float(v) for v in sine_coefficients(5)]


def gather_kernel(shape, own_ref, out_ref, local_sem, send_sem, recv_sem, pair_send, pair_recv):
    size = dict(x=shape[0], y=shape[1], z=shape[2])
    dom, cls = lax.axis_index("dom"), lax.axis_index("cls")
    here = dict(x=cls // 2, y=dom % size["y"], z=dom // size["y"])
    core = cls % 2
    rows = out_ref.shape[2]
    starts = [0]
    for share in SHARE:
        starts.append(starts[-1] + rows * share // 32)

    def device(at, which):
        return (at["z"] * size["y"] + at["y"], at["x"] * 2 + which)

    def slot(at, which):
        d = device(at, which)
        return d[0] * (size["x"] * 2) + d[1]

    def moved(at, dim, step):
        new = dict(at)
        new[dim] = at[dim] + step
        return new

    ways = []
    for dim in "xyz":
        if size[dim] == 1:
            continue
        if size[dim] == 2:
            other = dict(here)
            other[dim] = 1 - here[dim]
            ways.append((dim, 0, other, None))
        else:
            ways.append((dim, 1, moved(here, dim, 1), here[dim] < size[dim] - 1))
            ways.append((dim, -1, moved(here, dim, -1), here[dim] > 0))

    def when(conds, fn):
        conds = [c for c in conds if c is not None]
        if not conds:
            fn()
        else:
            pl.when(functools.reduce(jnp.logical_and, conds))(fn)

    barrier = pltpu.get_barrier_semaphore()
    partner = device(here, 1 - core)
    pl.semaphore_signal(barrier, inc=1, device_id=partner, device_id_type=MESH)
    for dim, sign, other, ok in ways:

        def greet(other=other):
            pl.semaphore_signal(barrier, inc=1, device_id=device(other, core), device_id_type=MESH)

        when([ok], greet)
    peers = 1
    for dim, sign, other, ok in ways:
        peers = peers + (1 if ok is None else ok.astype(jnp.int32))
    pl.semaphore_wait(barrier, peers)

    mine = slot(here, core)
    local = pltpu.make_async_copy(own_ref, out_ref.at[mine], local_sem)
    local.start()

    def part(ref, index):
        return ref.at[:, pl.ds(starts[index], starts[index + 1] - starts[index]), :]

    def copy(index, source, src_slot, to, way, own):
        src = part(own_ref, index) if own else part(out_ref.at[src_slot], index)
        return pltpu.make_async_remote_copy(
            src_ref=src,
            dst_ref=part(out_ref.at[src_slot], index),
            send_sem=send_sem.at[index, source, way],
            recv_sem=recv_sem.at[index, src_slot],
            device_id=to,
            device_id_type=MESH,
        )

    def pair_copy(index, source, src_slot, own):
        src = part(own_ref, index) if own else part(out_ref.at[src_slot], index)
        return pltpu.make_async_remote_copy(
            src_ref=src,
            dst_ref=part(out_ref.at[src_slot], index),
            send_sem=pair_send.at[index, source],
            recv_sem=pair_recv.at[index, src_slot],
            device_id=partner,
            device_id_type=MESH,
        )

    choices = {}
    for dim in "xyz":
        n = size[dim]
        if n == 1:
            choices[dim] = [(0, here[dim], None, 0)]
        elif n == 2:
            choices[dim] = [(0, here[dim], None, 0), (0, 1 - here[dim], None, 1)]
        else:
            listed = [(0, here[dim], None, 0)]
            for t in range(1, n):
                listed.append((1, here[dim] - t, here[dim] >= t, t))
                listed.append((-1, here[dim] + t, here[dim] + t < n, t))
            choices[dim] = listed
    events = []
    for ix, cx in enumerate(choices["x"]):
        for iy, cy in enumerate(choices["y"]):
            for iz, cz in enumerate(choices["z"]):
                pick = dict(x=cx, y=cy, z=cz)
                depth = cx[3] + cy[3] + cz[3]
                number = (ix * len(choices["y"]) + iy) * len(choices["z"]) + iz
                for index in range(3):
                    events.append((depth, index, number, pick))
    events.sort(key=lambda e: e[:3])
    finish = []
    for depth, index, number, pick in events:
        at = {dim: pick[dim][1] for dim in "xyz"}
        exists = [pick[dim][2] for dim in "xyz"]
        src_slot = slot(at, core)
        order = ROUTES[index]
        last = max([k for k, dim in enumerate(order) if pick[dim][3] > 0], default=-1)
        sends = []
        for number_way, (dim, sign, other, ok) in enumerate(ways):
            k = order.index(dim)
            if k < last:
                continue
            if k == last and (size[dim] == 2 or sign != pick[dim][0]):
                continue
            sends.append((number_way, device(other, core), ok))

        def arrive(index=index, number=number, src_slot=src_slot, depth=depth, sends=sends):
            own = depth == 0
            if not own:
                copy(index, number, src_slot, partner, 0, False).wait_recv()
            for way, to, ok in sends:
                when([ok], copy(index, number, src_slot, to, way, own).start)
            pair_copy(index, number, src_slot, own).start()

        def done(index=index, number=number, src_slot=src_slot, depth=depth, sends=sends, at=at):
            own = depth == 0
            for way, to, ok in sends:
                when([ok], copy(index, number, src_slot, to, way, own).wait_send)
            pair_copy(index, number, src_slot, own).wait_send()
            pair_copy(index, number, slot(at, 1 - core), False).wait_recv()

        when(exists, arrive)
        finish.append((exists, done))
    for exists, done in finish:
        when(exists, done)
    local.wait()


def gather(shape, own):
    devices = 2 * shape[0] * shape[1] * shape[2]
    total = 1
    for n in shape:
        total *= n if n <= 2 else 2 * n - 1
    return pl.pallas_call(
        functools.partial(gather_kernel, shape),
        out_shape=jax.ShapeDtypeStruct((devices,) + own.shape, own.dtype),
        in_specs=[pl.BlockSpec(memory_space=pltpu.VMEM)],
        out_specs=pl.BlockSpec(memory_space=pltpu.VMEM),
        scratch_shapes=[
            pltpu.SemaphoreType.DMA,
            pltpu.SemaphoreType.DMA((3, total, 4)),
            pltpu.SemaphoreType.DMA((3, devices)),
            pltpu.SemaphoreType.DMA((3, total)),
            pltpu.SemaphoreType.DMA((3, devices)),
        ],
        compiler_params=pltpu.CompilerParams(
            collective_id=0, has_side_effects=True, vmem_limit_bytes=12 * 1024 * 1024
        ),
        name="gather_slices",
    )(own)


def power_kernel(
    side, rot_count, classes_ref, rotations_ref, defocus_ref, images_ref, slices_ref, slope_ref, offset_ref, groups_ref, out_ref, power, acc
):
    step = pl.program_id(0)
    count, chunk, lanes = images_ref.shape
    shells = side // 2
    pitch = power.shape[0] // count

    @pl.when(step == 0)
    def _():
        acc[...] = jnp.zeros_like(acc)

    slope = slope_ref[...]
    offset = offset_ref[...]

    def one(i, carry):
        turns = defocus_ref[i].astype(jnp.float32) * slope + offset
        x = turns - ((turns + ROUND) - ROUND)
        y = x * x
        s = jnp.full_like(y, SINE[-1])
        for value in SINE[-2::-1]:
            s = s * y + value
        s = s * x
        d = images_ref[i].astype(jnp.float32) + s * slices_ref[classes_ref[i] * rot_count + rotations_ref[i]].astype(jnp.float32)
        power[pl.ds(pl.multiple_of(i * pitch, 8), chunk), :] = d * d
        return carry

    lax.fori_loop(0, count, one, 0, unroll=8)

    b = lax.broadcasted_iota(jnp.int32, (lanes, shells), 0)
    s = lax.broadcasted_iota(jnp.int32, (lanes, shells), 1)
    fb = jnp.where(b < side // 2, b, b - side)
    total = acc[...]
    for k in range(chunk // 2):
        a = step * (chunk // 2) + k
        fa = jnp.where(a < side // 2, a, a - side)
        r = fa * fa + fb * fb
        table = jnp.where((s * s <= r) & (r < (s + 1) * (s + 1)), 1.0, 0.0).astype(jnp.bfloat16)
        p = power[pl.ds(2 * k, count, stride=pitch), :] + power[pl.ds(2 * k + 1, count, stride=pitch), :]
        high = p.astype(jnp.bfloat16)
        low = (p - high.astype(jnp.float32)).astype(jnp.bfloat16)
        total = total + jnp.dot(
            jnp.concatenate([high, low], axis=1),
            jnp.concatenate([table, table], axis=0),
            preferred_element_type=jnp.float32,
        )
    acc[...] = total

    @pl.when(step == pl.num_programs(0) - 1)
    def _():
        groups = out_ref.shape[0]
        ids = lax.broadcasted_iota(jnp.int32, (groups, count), 0)
        member = jnp.where(ids == groups_ref[...], 1.0, 0.0)
        both = jnp.concatenate([acc[...], jnp.ones((count, out_ref.shape[1] - shells), jnp.float32)], axis=1)
        out_ref[...] = jnp.dot(
            member, both, precision=lax.Precision.HIGHEST, preferred_element_type=jnp.float32
        )


def shell_power(images, slices, classes, rotations, rot_count, defocus, groups, group_total):
    count, rows, side = images.shape
    chunk = 32
    offsets = np.arange(side)
    signed = np.where(offsets < side // 2, offsets, offsets - side)
    radius = (signed[:, None] ** 2 + signed[None, :] ** 2).astype(np.float64)
    spatial = np.repeat(radius / (side * PIXEL_SIZE) ** 2, 2, axis=0)
    slope = (0.5 * WAVELENGTH * spatial).astype(np.float32)
    offset = -0.25 * SPHERICAL * WAVELENGTH**3 * spatial**2 + math.asin(AMPLITUDE) / (2 * math.pi)
    offset = (offset - np.round(offset)).astype(np.float32)
    smem = pl.BlockSpec(memory_space=pltpu.SMEM)
    return pl.pallas_call(
        functools.partial(power_kernel, side, rot_count),
        grid=(rows // chunk,),
        out_shape=jax.ShapeDtypeStruct((group_total, 128), jnp.float32),
        in_specs=[
            smem,
            smem,
            smem,
            pl.BlockSpec((count, chunk, side), lambda i: (0, i, 0)),
            pl.BlockSpec((slices.shape[0], chunk, side), lambda i: (0, i, 0)),
            pl.BlockSpec((chunk, side), lambda i: (i, 0)),
            pl.BlockSpec((chunk, side), lambda i: (i, 0)),
            pl.BlockSpec((1, count), lambda i: (0, 0)),
        ],
        out_specs=pl.BlockSpec((group_total, 128), lambda i: (0, 0)),
        scratch_shapes=[
            pltpu.VMEM((count * (chunk + 8), side), jnp.float32),
            pltpu.VMEM((count, side // 2), jnp.float32),
        ],
        compiler_params=pltpu.CompilerParams(vmem_limit_bytes=20 * 1024 * 1024),
        name="shell_power",
    )(classes, rotations, defocus, images, slices, jnp.asarray(slope), jnp.asarray(offset), groups.reshape(1, count))


def exchange_kernel(sizes, shells, parts_ref, weight_ref, out_ref, held, send_sem, recv_sem):
    doms, clss = sizes
    n = doms * clss
    me = lax.axis_index("dom") * clss + lax.axis_index("cls")
    barrier = pltpu.get_barrier_semaphore()

    def device(k):
        peer = lax.rem(me + k, n)
        return peer, (peer // clss, lax.rem(peer, clss))

    def greet(k, carry):
        pl.semaphore_signal(barrier, inc=1, device_id=device(k)[1], device_id_type=MESH)
        return carry

    lax.fori_loop(1, n, greet, 0)
    pl.semaphore_wait(barrier, n - 1)

    def copy(k):
        peer, to = device(k)
        return pltpu.make_async_remote_copy(
            src_ref=parts_ref.at[peer],
            dst_ref=held.at[k],
            send_sem=send_sem.at[k],
            recv_sem=recv_sem.at[k],
            device_id=to,
            device_id_type=MESH,
        )

    def send(k, carry):
        copy(k).start()
        return carry

    lax.fori_loop(1, n, send, 0)

    def take(k, total):
        copy(k).wait_recv()
        return total + held[k]

    total = lax.fori_loop(1, n, take, parts_ref[me])

    def sent(k, carry):
        copy(k).wait_send()
        return carry

    lax.fori_loop(1, n, sent, 0)
    counts = total[:, shells : shells + 1]
    out_ref[...] = total[:, :shells] / (2.0 * counts * weight_ref[...])


def exchange(sizes, parts, weight):
    n = sizes[0] * sizes[1]
    shells = weight.shape[1]
    vmem = pl.BlockSpec(memory_space=pltpu.VMEM)
    return pl.pallas_call(
        functools.partial(exchange_kernel, sizes, shells),
        out_shape=jax.ShapeDtypeStruct((GROUPS_DEV, shells), jnp.float32),
        in_specs=[vmem, vmem],
        out_specs=vmem,
        scratch_shapes=[
            pltpu.VMEM((n, GROUPS_DEV, parts.shape[-1]), jnp.float32),
            pltpu.SemaphoreType.DMA((n,)),
            pltpu.SemaphoreType.DMA((n,)),
        ],
        compiler_params=pltpu.CompilerParams(
            collective_id=1, has_side_effects=True, vmem_limit_bytes=4 * 1024 * 1024
        ),
        name="exchange_groups",
    )(parts.reshape(n, GROUPS_DEV, parts.shape[-1]), weight)


PIECES = ((0, (0, 6, 13)), (1, (1, 2, 3, 10, 11, 12)), (2, (4, 5, 7, 8, 9)))
SCHEDULE = (
    (0, "o", 0), (1, "o", 0), (2, "o", 0), ("fill", 6), (0, "x", 0), (1, "a", 0), (1, "z", 1), (2, "a", 0),
    ("fill", 2), (2, "z", 1), (0, "y", 0), ("fill", 4), (1, "z", 2), (1, "a", 1), ("fill", 2), (2, "z", 2),
    (2, "a", 1), ("fill", 4), (1, "z", 3), (1, "a", 2), (0, "z", 1), ("fill", 4), (2, "z", 3), (2, "a", 2),
    ("fill", 4), (1, "a", 3), (2, "a", 3), (0, "z", 2), (2, "b", 0), (1, "b", 0), (2, "b", 1), (1, "b", 1),
    ("fill", 2), (2, "b", 2), (1, "b", 2), (2, "b", 3), (1, "b", 3), ("calc", 2), (0, "z", 3), ("calc", 1),
    ("calc", 0),
)
UNIT = 8
TILE = 8


def folded_rows(side):
    half = side // 2
    low, high = half - TILE, half + TILE
    kept = np.concatenate([np.arange(low), np.arange(high, side)])
    other = kept.copy()
    other[low - TILE : low] = half - 1 - np.arange(TILE)
    other[low : low + TILE] = high - np.arange(TILE)
    return kept, other


def folded_radius(side):
    half = side // 2
    offsets = np.arange(side)
    signed = np.where(offsets < half, offsets, offsets - side)
    radius = signed[:, None] ** 2 + signed[None, :] ** 2
    kept, other = folded_rows(side)
    own, far = radius[kept], np.roll(radius[other], half, axis=1)
    inside = own < half * half
    fold = (other != kept)[:, None] & ~inside
    assert not np.any((other != kept)[:, None] & inside & (far < half * half))
    packed = np.where(fold, far, own)
    assert np.sum(packed < half * half) == np.sum(radius < half * half)
    return packed


def runs_of(tiles):
    runs = []
    for k, t in enumerate(tiles):
        if runs and runs[-1][1] + runs[-1][2] == t:
            runs[-1][2] += 1
        else:
            runs.append([k, t, 1])
    return runs


def row_groups(tiles, side):
    place = {TILE * t + r: TILE * k + r for k, t in enumerate(tiles) for r in range(TILE)}
    kept, other = folded_rows(side)
    plain = {int(a): j for j, a in enumerate(kept) if other[j] == a and (a == 0 or other[j - 1] == kept[j - 1])}
    groups, used = [], set()
    for j in sorted(place):
        if j in used:
            continue
        a = int(kept[j])
        mate = plain.get(side - a) if plain.get(a) == j else None
        if mate is not None and mate != j and mate in place:
            used.add(mate)
            groups.append((j, (place[j], place[mate])))
        else:
            groups.append((j, (place[j],)))
    return groups


def fold(keep, far, shifted, first_row, side):
    lines = 2 * TILE
    order = [(-i if shifted else TILE - 1 - i) % TILE for i in range(TILE)]
    far = far.astype(jnp.float32)
    far = jnp.concatenate([far[2 * k : 2 * k + 2] for k in order], axis=0)
    far = pltpu.roll(far, side // 2, axis=1)
    a = first_row + lax.broadcasted_iota(jnp.int32, (lines, side), 0) // 2
    b = lax.broadcasted_iota(jnp.int32, (lines, side), 1)
    fa = jnp.where(a < side // 2, a, a - side)
    fb = jnp.where(b < side // 2, b, b - side)
    inside = fa * fa + fb * fb < (side // 2) * (side // 2)
    return jnp.where(inside, keep.astype(jnp.float32), far).astype(keep.dtype)


def arrival_slot(pieces, nz, p, stage, zs):
    if p < len(pieces) and pieces[p][0] == 0:
        place = stage if stage < 2 else 2 + zs
    else:
        place = stage * nz + zs
    return sum(2 + nz if route == 0 else 3 * nz for route, _ in pieces[:p]) + place


def fused_kernel(
    nz,
    side,
    classes_here,
    rot_count,
    layout,
    classes_hbm,
    rotations_hbm,
    defocus_hbm,
    slope_hbm,
    offset_hbm,
    groups_hbm,
    weight_hbm,
    own_hbm,
    images_hbm,
    out_ref,
    *scratch,
):
    pieces, tiles = layout
    count = images_hbm.shape[0]
    shells = side // 2
    rows = 16 * tiles
    half = rows // 2
    bufs = scratch[: len(pieces)]
    (
        classes_ref,
        rotations_ref,
        defocus_ref,
        slope_ref,
        offset_ref,
        groups_ref,
        weight_ref,
        images,
        image_rim,
        own_rim,
        sine,
        power,
        table,
        acc,
        parts,
        held,
        local_sem,
        image_sem,
        small_sem,
        send_sem,
        recv_sem,
        pair_send,
        pair_recv,
        part_send,
        part_recv,
    ) = scratch[len(pieces) :]
    dom, cls = lax.axis_index("dom"), lax.axis_index("cls")
    x, core, y, z = cls // 2, cls % 2, dom % 2, dom // 2
    slot = classes_here * rot_count

    def device(x_, y_, z_, core_):
        return (z_ * 2 + y_, x_ * 2 + core_)

    partner = device(x, y, z, 1 - core)
    up, down = device(x, y, z + 1, core), device(x, y, z - 1, core)
    across = {"x": device(1 - x, y, z, core), "y": device(x, 1 - y, z, core)}

    def when(conds, fn):
        conds = [c for c in conds if c is not None]
        if not conds:
            fn()
        else:
            pl.when(functools.reduce(jnp.logical_and, conds))(fn)

    barrier = pltpu.get_barrier_semaphore()
    for to in (partner, across["x"], across["y"]):
        pl.semaphore_signal(barrier, inc=1, device_id=to, device_id_type=MESH)
    has_up, has_down = z < nz - 1, z > 0
    when([has_up], lambda: pl.semaphore_signal(barrier, inc=1, device_id=up, device_id_type=MESH))
    when([has_down], lambda: pl.semaphore_signal(barrier, inc=1, device_id=down, device_id_type=MESH))

    line = 2 * TILE
    rim = tiles // 2 - 1
    own_copies = [
        pltpu.make_async_copy(own_hbm.at[:, pl.ds(line * rim, 4 * line), :], own_rim, local_sem.at[0])
    ]
    rim_stores = []
    for p, (route, held_tiles) in enumerate(pieces):
        q1, q2 = (x, y) if route == 1 else (y, x)
        at = (((core * nz + z) * 2 + q1) * 2 + q2) * slot
        for k, t in enumerate(held_tiles):
            if rim <= t < rim + 2:
                rim_stores.append((p, at, line * k, t - rim))
        for k, t, n in runs_of([t if not rim <= t < rim + 2 else -line * t for t in held_tiles]):
            if t >= 0:
                own_copies.append(
                    pltpu.make_async_copy(
                        own_hbm.at[:, pl.ds(line * (t + 2 * (t > rim)), line * n), :],
                        bufs[p].at[pl.ds(at, slot), pl.ds(line * k, line * n), :],
                        local_sem.at[len(own_copies)],
                    )
                )
    for c in own_copies:
        c.start()
    edge = line * rim
    image_copies = [
        pltpu.make_async_copy(images_hbm.at[:, pl.ds(edge, 4 * line), :], image_rim, image_sem.at[0]),
        pltpu.make_async_copy(images_hbm.at[:, pl.ds(0, edge), :], images.at[:, pl.ds(0, edge), :], image_sem.at[1]),
        pltpu.make_async_copy(
            images_hbm.at[:, pl.ds(edge + 4 * line, edge), :],
            images.at[:, pl.ds(edge + 2 * line, edge), :],
            image_sem.at[2],
        ),
    ]
    small = (
        (slope_hbm, slope_ref),
        (offset_hbm, offset_ref),
        (defocus_hbm, defocus_ref),
        (classes_hbm, classes_ref),
        (rotations_hbm, rotations_ref),
        (groups_hbm, groups_ref),
        (weight_hbm, weight_ref),
    )
    small_copies = [pltpu.make_async_copy(src, dst, small_sem.at[k]) for k, (src, dst) in enumerate(small)]
    for c in small_copies:
        c.start()

    def folded(ref, i, k):
        keep = ref[i, pl.ds(3 * line * k, line), :]
        far = ref[i, pl.ds(line * (1 + k), line), :]
        return fold(keep, far, k == 1, TILE * (rim + 3 * k), side)

    for c in own_copies:
        c.wait()
    for c in image_copies:
        c.start()
    for p, at, row, k in rim_stores:
        for j in range(slot):
            bufs[p][at + j, pl.ds(row, line), :] = folded(own_rim, j, k)
    pl.semaphore_wait(barrier, 3 + has_up.astype(jnp.int32) + has_down.astype(jnp.int32))

    events = []
    for p, (route, n) in enumerate(pieces):
        q1, q2 = (x, y) if route == 1 else (y, x)
        to_q1, to_q2 = (across["x"], across["y"]) if route == 1 else (across["y"], across["x"])
        buf = bufs[p]

        def region(core_, z_, a=None, b=None, buf=buf):
            first = (core_ * nz + z_) * 4 * slot
            size = 4 * slot
            if a is not None:
                first, size = first + a * 2 * slot, 2 * slot
            if b is not None:
                first, size = first + b * slot, slot
            return buf.at[pl.ds(first, size)]

        def link(stage, zs, number, where, to, p=p):
            return pltpu.make_async_remote_copy(
                src_ref=where,
                dst_ref=where,
                send_sem=send_sem.at[p],
                recv_sem=recv_sem.at[arrival_slot(pieces, nz, p, stage, zs)],
                device_id=to,
                device_id_type=MESH,
            )

        def pair(stage, zs, where, p=p):
            return pltpu.make_async_remote_copy(
                src_ref=where,
                dst_ref=where,
                send_sem=pair_send.at[p],
                recv_sem=pair_recv.at[p],
                device_id=partner,
                device_id_type=MESH,
            )

        reach = [(z, None, 0, None)]
        for t in range(1, nz):
            reach.append((z - t, z >= t, t, -1))
            reach.append((z + t, z + t < nz, t, 1))

        if route == 0:
            one = region(core, z, q1, q2)
            other = region(core, z, q1, 1 - q2)
            mine = region(core, z, q1)
            events.append(((p, "o", 0), p, [], [], [(None, link(0, z, 0, one, to_q2))], None))
            events.append(((p, "x", 0), p, [], [link(0, z, 0, other, to_q2)], [(None, link(1, z, 0, mine, to_q1))], None))
            for k, (zs, ok, t, way) in enumerate(reach):
                block = region(core, zs)
                sends = []
                if way in (None, -1):
                    sends.append((has_up, link(2, zs, 2 * k, block, up)))
                if way in (None, 1):
                    sends.append((has_down, link(2, zs, 2 * k + 1, block, down)))
                arrival = link(1, z, 0, region(core, z, 1 - q1), to_q1) if way is None else link(2, zs, 0, block, up)
                twin = region(1 - core, zs)
                name = (p, "z" if t else "y", t)
                events.append((name, p, [ok], [arrival], sends, (pair(0, zs, block), pair(0, zs, twin))))
        else:
            for k, (zs, ok, t, way) in enumerate(reach):
                one = region(core, zs, q1, q2)
                sends = []
                if way in (None, -1):
                    sends.append((has_up, link(0, zs, 2 * k, one, up)))
                if way in (None, 1):
                    sends.append((has_down, link(0, zs, 2 * k + 1, one, down)))
                sends.append((None, link(1, zs, k, one, to_q2)))
                arrival = [] if way is None else [link(0, zs, 0, one, up)]
                events.append(((p, "z" if t else "o", t), p, [ok], arrival, sends, None))
                near, far = region(core, zs, q1), region(core, zs, 1 - q1)
                events.append(
                    (
                        (p, "a", t),
                        p,
                        [ok],
                        [link(1, zs, 0, region(core, zs, q1, 1 - q2), to_q2)],
                        [(None, link(2, zs, k, near, to_q1))],
                        (pair(0, zs, near), pair(0, zs, region(1 - core, zs, q1))),
                    )
                )
                events.append(
                    (
                        (p, "b", t),
                        p,
                        [ok],
                        [link(2, zs, 0, far, to_q1)],
                        [],
                        (pair(1, zs, far), pair(1, zs, region(1 - core, zs, 1 - q1))),
                    )
                )

    def make_sine(i, carry):
        turns = defocus_ref[i].astype(jnp.float32) * slope_ref[...] + offset_ref[...]
        v = turns - ((turns + ROUND) - ROUND)
        w = v * v
        s = jnp.full_like(w, SINE[-1])
        for value in SINE[-2::-1]:
            s = s * w + value
        s = s * v
        base = pl.multiple_of(i * rows, 8)
        sine[pl.ds(base, half, stride=2), :] = s
        sine[pl.ds(base + 1, half, stride=2), :] = s
        return carry

    def sine_unit(j):
        def run():
            if j == 0:
                for c in small_copies[:3]:
                    c.wait()
            lax.fori_loop(j * UNIT, (j + 1) * UNIT, make_sine, 0, unroll=2)

        return run

    def make_table(a, carry):
        b = lax.broadcasted_iota(jnp.int32, (side, shells), 0)
        s = lax.broadcasted_iota(jnp.int32, (side, shells), 1)
        low = TILE * (rim + 1)
        row = jnp.where(a < low, a, a + 2 * TILE)
        far = jnp.where(a < low, side // 2 - 1 + TILE * rim - a, side // 2 + TILE + low - a)
        fb = jnp.where(b < side // 2, b, b - side)
        gb = b - side // 2
        fa = jnp.where(row < side // 2, row, row - side)
        ga = jnp.where(far < side // 2, far, far - side)
        r = fa * fa + fb * fb
        folds = (a >= TILE * rim) & (a < TILE * (rim + 2)) & (a != low)
        r = jnp.where(folds & (r >= (side // 2) * (side // 2)), ga * ga + gb * gb, r)
        inside = (s * s <= r) & (r < (s + 1) * (s + 1))
        table[a] = jnp.where(inside, 1.0, 0.0).astype(jnp.bfloat16)
        return carry

    def table_unit(j, n):
        return lambda: lax.fori_loop(j * n, (j + 1) * n, make_table, 0)

    def fold_image(i, carry):
        for k in range(2):
            images[i, pl.ds(line * (rim + k), line), :] = folded(image_rim, i, k)
        return carry

    def fold_unit(j):
        def run():
            if j == 0:
                image_copies[0].wait()
            lax.fori_loop(j * 4 * UNIT, (j + 1) * 4 * UNIT, fold_image, 0, unroll=4)

        return run

    fillers = [table_unit(j, half // 8) for j in range(8)] + [sine_unit(j) for j in range(count // UNIT)]
    fillers += [fold_unit(j) for j in range(count // (4 * UNIT))]
    fillers.reverse()
    calculated = []
    acc[...] = jnp.zeros_like(acc)

    def twins(p):
        where = bufs[p].at[pl.ds((1 - core) * (4 * nz * slot), 4 * nz * slot)]
        return pltpu.make_async_remote_copy(
            src_ref=where,
            dst_ref=where,
            send_sem=pair_send.at[p],
            recv_sem=pair_recv.at[p],
            device_id=partner,
            device_id_type=MESH,
        )

    def calc(p):
        route, held_tiles = pieces[p]
        if not calculated:
            for c in image_copies[1:] + small_copies[3:]:
                c.wait()
        calculated.append(p)
        twins(p).wait_recv()
        pitch = line * len(held_tiles) + TILE

        def one(i, carry, p=p, route=route, held_tiles=held_tiles, pitch=pitch):
            c = classes_ref[i]
            owner, sub = (c, 0) if classes_here == 1 else (c // classes_here, c % classes_here)
            place = owner >> 1
            if route == 1:
                place = (place & ~3) | ((place & 1) << 1) | ((place >> 1) & 1)
            at = ((owner & 1) * (nz * 4) + place) * slot + sub * rot_count + rotations_ref[i]
            for k, t, n in runs_of(held_tiles):
                f = bufs[p][at, pl.ds(line * k, line * n), :].astype(jnp.float32)
                s = sine[pl.ds(pl.multiple_of(i * rows + line * t, 8), line * n), :]
                d = images[i, pl.ds(line * t, line * n), :].astype(jnp.float32) + s * f
                power[pl.ds(pl.multiple_of(i * pitch + line * k, 8), line * n), :] = d * d
            return carry

        lax.fori_loop(0, count, one, 0, unroll=16)
        total = acc[...]
        for j, places in row_groups(held_tiles, side):
            v = None
            for k in places:
                for part in range(2):
                    w = power[pl.ds(2 * k + part, count, stride=pitch), :]
                    v = w if v is None else v + w
            high = v.astype(jnp.bfloat16)
            low = (v - high.astype(jnp.float32)).astype(jnp.bfloat16)
            t = table[j]
            total = total + jnp.dot(
                jnp.concatenate([high, low], axis=1),
                jnp.concatenate([t, t], axis=0),
                preferred_element_type=jnp.float32,
            )
        acc[...] = total

    def amount(p, slots):
        where = bufs[p].at[pl.ds(0, slots * slot)]
        return pltpu.make_async_remote_copy(
            src_ref=where,
            dst_ref=where,
            send_sem=send_sem.at[p],
            recv_sem=pair_recv.at[p],
            device_id=partner,
            device_id_type=MESH,
        )

    def handle(event):
        _, _, exists, arrivals, sends, twin = event

        def arrive():
            for c in arrivals:
                c.wait_recv()
            for ok, c in sends:
                when([ok], c.start)
            if twin is not None:
                twin[0].start()

        when(exists, arrive)

    for step in SCHEDULE:
        if step[0] == "fill":
            for _ in range(step[1]):
                fillers.pop()()
        elif step[0] == "calc":
            calc(step[1])
        else:
            for event in events:
                if event[0] == step:
                    handle(event)
    assert not fillers and len(calculated) == len(pieces)

    owners, groups_here = parts.shape[:2]
    ids = lax.broadcasted_iota(jnp.int32, (owners * groups_here, count), 0)
    member = jnp.where(ids == groups_ref[...], 1.0, 0.0).astype(jnp.bfloat16)
    rest = jnp.concatenate([acc[...], jnp.ones((count, parts.shape[2] - shells), jnp.float32)], axis=1)
    terms = []
    for _ in range(3):
        terms.append(rest.astype(jnp.bfloat16))
        rest = rest - terms[-1].astype(jnp.float32)
    parts[...] = jnp.dot(
        jnp.concatenate([member] * 3, axis=1), jnp.concatenate(terms, axis=0), preferred_element_type=jnp.float32
    ).reshape(parts.shape)

    me = dom * 4 + cls
    everyone = pl.ds(1, owners - 1)

    def part_copy(k):
        peer = me + k
        peer = jnp.where(peer >= owners, peer - owners, peer)
        return pltpu.make_async_remote_copy(
            src_ref=parts.at[peer],
            dst_ref=held.at[k],
            send_sem=part_send,
            recv_sem=part_recv,
            device_id=(peer >> 2, peer & 3),
            device_id_type=MESH,
        )

    for k in sorted(range(1, owners), key=lambda k: -abs(k - owners // 2)):
        part_copy(k).start()
    for p, (route, held_tiles) in enumerate(pieces):
        twins(p).wait_send()
        inner = (3 + 4 * (nz + 1)) if route == 0 else 3 * nz + nz + 1
        outer = (3 + 4) if route == 0 else 3 * nz + 1
        inside = has_up & has_down
        when([inside], amount(p, inner).wait_send)
        when([jnp.logical_not(inside)], amount(p, outer).wait_send)

    all_parts = pltpu.make_async_remote_copy(
        src_ref=held.at[everyone],
        dst_ref=held.at[everyone],
        send_sem=part_send,
        recv_sem=part_recv,
        device_id=partner,
        device_id_type=MESH,
    )
    all_parts.wait_recv()
    total = parts[me] + jnp.sum(held[everyone], axis=0)
    all_parts.wait_send()
    counts = total[:, shells : shells + 1]
    out_ref[...] = total[:, :shells] / (2.0 * counts * weight_ref[...])


def pixel_tables(side):
    offsets = np.arange(side)
    signed = np.where(offsets < side // 2, offsets, offsets - side)
    radius = (signed[:, None] ** 2 + signed[None, :] ** 2).astype(np.float64)
    spatial = folded_radius(side).astype(np.float64) / (side * PIXEL_SIZE) ** 2
    slope = (0.5 * WAVELENGTH * spatial).astype(np.float32)
    offset = -0.25 * SPHERICAL * WAVELENGTH**3 * spatial**2 + math.asin(AMPLITUDE) / (2 * math.pi)
    offset = (offset - np.round(offset)).astype(np.float32)
    s = np.arange(side // 2)[:, None, None]
    weight = ((s * s <= radius) & (radius < (s + 1) ** 2)).sum(axis=(1, 2)).astype(np.float32)
    return slope, offset, weight.reshape(1, -1)


def fused(nz, images, own, classes, rotations, defocus, groups, classes_here, rot_count, owners):
    count, rows, side = images.shape
    shells = side // 2
    pieces = PIECES
    tiles = sum(len(held) for _, held in pieces)
    slots = owners * classes_here * rot_count
    slope, offset, weight = pixel_tables(side)
    vmem = pl.BlockSpec(memory_space=pltpu.VMEM)
    hbm = pl.BlockSpec(memory_space=pltpu.HBM)
    dma = pltpu.SemaphoreType.DMA
    widest = max(len(held) for _, held in pieces)
    return pl.pallas_call(
        functools.partial(fused_kernel, nz, side, classes_here, rot_count, (pieces, tiles)),
        out_shape=jax.ShapeDtypeStruct((GROUPS_DEV, shells), jnp.float32),
        in_specs=[hbm] * 9,
        out_specs=vmem,
        scratch_shapes=[pltpu.VMEM((slots, 16 * len(held), side), jnp.bfloat16) for _, held in pieces]
        + [pltpu.SMEM((count,), jnp.int32)] * 3
        + [
            pltpu.VMEM(slope.shape, jnp.float32),
            pltpu.VMEM(slope.shape, jnp.float32),
            pltpu.VMEM((1, count), jnp.int32),
            pltpu.VMEM(weight.shape, jnp.float32),
            pltpu.VMEM((count, 16 * tiles, side), jnp.bfloat16),
            pltpu.VMEM((count, 8 * TILE, side), jnp.bfloat16),
            pltpu.VMEM((classes_here * rot_count, 8 * TILE, side), jnp.bfloat16),
            pltpu.VMEM((count * 16 * tiles, side), jnp.float32),
            pltpu.VMEM((count * (16 * widest + 8), side), jnp.float32),
            pltpu.VMEM((8 * tiles, side, shells), jnp.bfloat16),
            pltpu.VMEM((count, shells), jnp.float32),
            pltpu.VMEM((owners, GROUPS_DEV, 128), jnp.float32),
            pltpu.VMEM((owners, GROUPS_DEV, 128), jnp.float32),
            dma((sum(len(runs_of(held)) for _, held in pieces),)),
            dma((3,)),
            dma((7,)),
            dma((len(pieces),)),
            dma((arrival_slot(pieces, nz, len(pieces), 0, 0),)),
            dma((len(pieces),)),
            dma((len(pieces),)),
            dma,
            dma,
        ],
        compiler_params=pltpu.CompilerParams(
            collective_id=0, has_side_effects=True, vmem_limit_bytes=50 * 1024 * 1024
        ),
        name="fused_spectrum",
    )(
        *(
            pltpu.with_memory_space_constraint(operand, pltpu.HBM)
            for operand in (
                classes,
                rotations,
                defocus,
                jnp.asarray(slope),
                jnp.asarray(offset),
                groups.reshape(1, count),
                jnp.asarray(weight),
                own,
                images,
            )
        )
    )


def body(sizes, images, slices, classes, rotations, defocus, groups):
    doms, clss = sizes
    n = doms * clss
    count, _, pixels = images.shape
    side = math.isqrt(pixels)
    classes_here, rot_count = slices.shape[:2]

    def rows_of(array):
        lead = array.shape[:-2]
        split = array.reshape(lead + (2, side, side))
        return jnp.swapaxes(split, -3, -2).reshape(lead + (2 * side, side))

    own = rows_of(slices).reshape(classes_here * rot_count, 2 * side, side)
    if clss == 4 and doms == 8 and side == 16 * TILE:
        return fused(
            doms // 2, rows_of(images), own, classes, rotations, defocus, groups, classes_here, rot_count, n
        )
    ny = clss // 2
    if clss % 2 == 0 and doms % ny == 0 and n <= 32:
        every = gather((ny, ny, doms // ny), own)
    else:
        every = lax.all_gather(own, AXES, axis=0)
    every = every.reshape(n * own.shape[0], 2 * side, side)
    parts = shell_power(rows_of(images), every, classes, rotations, rot_count, defocus, groups, GROUPS_DEV * n)
    offsets = np.arange(side)
    signed = np.where(offsets < side // 2, offsets, offsets - side)
    radius = signed[:, None] ** 2 + signed[None, :] ** 2
    s = np.arange(side // 2)[:, None, None]
    weight = ((s * s <= radius) & (radius < (s + 1) ** 2)).sum(axis=(1, 2)).astype(np.float32)
    return exchange(sizes, parts, jnp.asarray(weight).reshape(1, -1))


def solution(mesh):
    sizes = (mesh.shape["dom"], mesh.shape["cls"])
    return jax.shard_map(
        functools.partial(body, sizes),
        mesh=mesh,
        in_specs=(
            P(AXES, None, None),
            P(AXES, None, None, None),
            P(AXES),
            P(AXES),
            P(AXES),
            P(AXES),
        ),
        out_specs=P(AXES, None),
        check_vma=False,
    )
```
